32 devices in a mesh: wide: 8 (over y, x, core), narrow: 4 (over z).
Axes of the slice: x: 2, y: 2, z: 4, core: 2. Of those that a mesh axis runs over, the one named last changes fastest.
Arguments:
- tokens: bfloat16 [65536, 768], P(('wide', 'narrow')), may hold values from -6 to 6
- cotangent: bfloat16 [65536, 768], P(('wide', 'narrow')), may hold values from -6 to 6
- segment_ids: int32 [128, 512], P(('wide', 'narrow')), may hold values from 0 to 3, never falling along the last dimension, each value on 1 to 256 neighbouring positions
- feature_ids: int32 [128, 512], P(('wide', 'narrow')), may hold values from 0 to 15
- attention_master: float32 [3072, 768], P(('wide', 'narrow')), may hold values from -1.1547005 to 1.1547005
- attention_first: float32 [3072, 768], P(('wide', 'narrow')), may hold values from -1024 to 1024
- attention_second: float32 [3072, 768], P(('wide', 'narrow')), may hold values from 327.68 to 262144
- feedforward_master: float32 [6144, 768], P(('wide', 'narrow')), may hold values from -0.14433757 to 0.14433757
- feedforward_first: float32 [6144, 768], P(('wide', 'narrow')), may hold values from -1024 to 1024
- feedforward_second: float32 [6144, 768], P(('wide', 'narrow')), may hold values from 327.68 to 262144
- vector_master: float32 [13, 768], P(None, ('wide', 'narrow')), may hold values from -0.8 to 1.5
- vector_first: float32 [13, 768], P(None, ('wide', 'narrow')), may hold values from -1024 to 1024
- vector_second: float32 [13, 768], P(None, ('wide', 'narrow')), may hold values from 327.68 to 262144
Outputs:
- block_out: bfloat16 [65536, 768], P(('wide', 'narrow'))
- tokens_grad: bfloat16 [65536, 768], P(('wide', 'narrow'))
- attention_master_new: float32 [3072, 768], P(('wide', 'narrow'))
- attention_first_new: float32 [3072, 768], P(('wide', 'narrow'))
- attention_second_new: float32 [3072, 768], P(('wide', 'narrow'))
- attention_copy: bfloat16 [3072, 768], P(('wide', 'narrow'))
- feedforward_master_new: float32 [6144, 768], P(('wide', 'narrow'))
- feedforward_first_new: float32 [6144, 768], P(('wide', 'narrow'))
- feedforward_second_new: float32 [6144, 768], P(('wide', 'narrow'))
- feedforward_copy: bfloat16 [6144, 768], P(('wide', 'narrow'))
- vector_master_new: float32 [13, 768], P(None, ('wide', 'narrow'))
- vector_first_new: float32 [13, 768], P(None, ('wide', 'narrow'))
- vector_second_new: float32 [13, 768], P(None, ('wide', 'narrow'))
- vector_copy: bfloat16 [13, 768], P(None, ('wide', 'narrow'))
The draws below stay inside these ranges and needn't reach their ends.
All inputs are finite; a program needn't handle non-finite values.
Results may differ from the reference program's by a relative error of at most 0.015.
The reference program's roundings to bfloat16 on the way count: a program that leaves them out, or rounds other values in their place, can miss the bound.
Values may be sent and summed in bfloat16 or wider, within the bound.
A program may use at most 256 MiB of HBM per device.

```python
import math
import jax
import jax.numpy as jnp
import numpy as np
from jax import lax

D = 768
FF = 3072
HEADS = 12
HEAD_DIM = 64
L = 512
SEGMENTS = 4
FEATURES = 16
ADAM_STEP = 3
SMALL = 13
SEQS = 128
TOKENS = 65536


def unit_normal(key, shape):
    return jax.random.truncated_normal(key, -4.0, 4.0, shape, jnp.float32)


def second_factor(key, shape):
    return jnp.exp(jax.random.uniform(key, shape, jnp.float32, jnp.log(0.7), jnp.log(4.0)))


def attention_scale(row_index):
    return jnp.where(row_index < 2 * D, 0.42, jnp.where(row_index < 3 * D, 0.7, 0.09))


def feedforward_scale(row_index):
    return jnp.where(row_index < FF, 0.25, 0.5)


def vector_scale():
    expand = FF // D
    table = [0.35, 0.42, 0.7, 0.6, 1.0, 1.0] + [0.25] * expand + [0.85, 1.0, 1.0]
    return jnp.array(table, jnp.float32)[:, None]


def draw_attention_master(key, part):
    row_index = jnp.arange(4 * D)[:, None]
    spread = jnp.where(row_index < 3 * D, D ** (-0.5), (D // 64) ** (-0.5))
    return unit_normal(key, (4 * D, D)) * spread


def draw_attention_first(key, part):
    row_index = jnp.arange(4 * D)[:, None]
    return unit_normal(key, (4 * D, D)) * attention_scale(row_index) * TOKENS ** 0.5


def draw_attention_second(key, part):
    row_index = jnp.arange(4 * D)[:, None]
    scale_rows = attention_scale(row_index)
    return second_factor(key, (4 * D, D)) * scale_rows * scale_rows * TOKENS


def draw_feedforward_master(key, part):
    row_index = jnp.arange(2 * FF)[:, None]
    spread = jnp.where(row_index < FF, D ** (-0.5), FF ** (-0.5))
    return unit_normal(key, (2 * FF, D)) * spread


def draw_feedforward_first(key, part):
    row_index = jnp.arange(2 * FF)[:, None]
    return unit_normal(key, (2 * FF, D)) * feedforward_scale(row_index) * TOKENS ** 0.5


def draw_feedforward_second(key, part):
    row_index = jnp.arange(2 * FF)[:, None]
    scale_rows = feedforward_scale(row_index)
    return second_factor(key, (2 * FF, D)) * scale_rows * scale_rows * TOKENS


def draw_vector_master(key, part):
    row_index = jnp.arange(SMALL)[:, None]
    gains = jax.random.uniform(jax.random.fold_in(key, 1), (SMALL, D), jnp.float32, 0.5, 1.5)
    biases = jax.random.truncated_normal(jax.random.fold_in(key, 2), -4.0, 4.0, (SMALL, D), jnp.float32) * 0.2
    is_gain = (row_index == 0) | (row_index == 4) | (row_index == SMALL - 2)
    return jnp.where(is_gain, gains, biases)


def draw_vector_first(key, part):
    return unit_normal(key, (SMALL, D)) * vector_scale() * TOKENS ** 0.5


def draw_vector_second(key, part):
    scale_rows = vector_scale()
    return second_factor(key, (SMALL, D)) * scale_rows * scale_rows * TOKENS


def set_ends(values, key, smallest, largest):
    dims = values.shape
    index_at = [jax.random.randint(jax.random.fold_in(key, axis), (), 0, dims[axis]) for axis in range(len(dims))]
    values = values.at[tuple(index_at)].set(smallest)
    longest = dims.index(max(dims))
    index_at[longest] = (index_at[longest] + 1) % dims[longest]
    return values.at[tuple(index_at)].set(largest)


def level_of(stream_key, shape, shards, least, high):
    gain = 1.0
    for axis_at, shards_of in shards:
        steps = jax.random.uniform(jax.random.fold_in(jax.random.fold_in(stream_key, 6), axis_at), (shards_of,), jnp.float32, least / len(shards), high / len(shards))
        gain = gain * jnp.repeat(jnp.exp(steps), shape[axis_at] // shards_of).reshape((-1,) + (1,) * (len(shape) - 1 - axis_at))
    return gain


def split_up(amount, total, most, slope):
    weights = [(1 << 20) // math.isqrt(standing ** slope) + 1 for standing in range(2, amount + 1)]
    spare, holding = total - most - (amount - 1), [1] * (amount - 1)
    while spare > 0:
        candidates = [i for i in range(amount - 1) if holding[i] < most]
        pool, left = sum([weights[i] for i in candidates]), spare
        for i in candidates:
            addition = min(most - holding[i], max(1, left * weights[i] // pool), spare)
            holding[i] = holding[i] + addition
            spare = spare - addition
    return np.array([most] + holding)


def uneven_parts(stream_key, count, total, reach, slope):
    if count == 2:
        one = jax.random.randint(stream_key, (), max(1, total - reach), min(reach, total - 1) + 1)
        return jnp.stack([one, total - one])
    tallies = jnp.asarray(split_up(count, total, reach, slope), jnp.int32)
    couples = (count - 1) // 2
    source_of, taker = tallies[1:1 + 2 * couples:2], tallies[2:2 + 2 * couples:2]
    room = jnp.minimum(source_of - 1, reach - taker)
    passed = jax.random.randint(jax.random.fold_in(stream_key, 1), (couples,), 0, 1 << 20) % (room + 1)
    tallies = tallies.at[1:1 + 2 * couples:2].set(source_of - passed).at[2:2 + 2 * couples:2].set(taker + passed)
    return tallies[jax.random.permutation(jax.random.fold_in(stream_key, 2), count)]


def bell_draw(own_key, dims, scale, most, shards=(), dtype=jnp.bfloat16):
    drawn = jax.random.normal(own_key, dims, jnp.float32) * scale
    if len(shards) > 0:
        drawn = level_of(own_key, dims, shards, -0.22, 0.18) * drawn
    return jnp.clip(drawn, min=-most, max=most).astype(dtype)


def setup_inputs(seed: int = 0) -> dict:
    streams_of = jax.random.split(jax.random.key(seed), 14)
    return {
        "tokens": bell_draw(streams_of[0], (TOKENS, D), 1.0, 6.0, ((0, 32),)),
        "cotangent": bell_draw(streams_of[1], (TOKENS, D), 1.0, 6.0, ((0, 32),)),
        "segment_ids": jax.vmap(lambda own: jnp.searchsorted(jnp.cumsum(uneven_parts(own, SEGMENTS, L, L // 2, 0)), jnp.arange(L), side="right"))(jax.random.split(streams_of[2], SEQS)).reshape((SEQS, L)).astype(jnp.int32),
        "feature_ids": set_ends(jax.random.randint(streams_of[3], (SEQS, L), 0, FEATURES), jax.random.fold_in(streams_of[3], 1), 0, FEATURES - 1).astype(jnp.int32),
        "attention_master": draw_attention_master(jax.random.fold_in(streams_of[13], 71), 0),
        "attention_first": draw_attention_first(jax.random.fold_in(streams_of[13], 71), 0),
        "attention_second": draw_attention_second(jax.random.fold_in(streams_of[13], 71), 0),
        "feedforward_master": draw_feedforward_master(jax.random.fold_in(streams_of[13], 71), 0),
        "feedforward_first": draw_feedforward_first(jax.random.fold_in(streams_of[13], 71), 0),
        "feedforward_second": draw_feedforward_second(jax.random.fold_in(streams_of[13], 71), 0),
        "vector_master": draw_vector_master(jax.random.fold_in(streams_of[13], 71), 0),
        "vector_first": draw_vector_first(jax.random.fold_in(streams_of[13], 71), 0),
        "vector_second": draw_vector_second(jax.random.fold_in(streams_of[13], 71), 0),
    }


@jax.custom_vjp
def low(v):
    return lax.optimization_barrier(v.astype(jnp.bfloat16)).astype(jnp.float32)

@jax.custom_vjp
def low_back(v):
    return v

def low_keep(v):
    return (low(v), None)

def low_pass(kept, grad):
    return (grad,)

def back_keep(v):
    return (v, None)

def back_low(kept, grad):
    return (low(grad),)
low.defvjp(low_keep, low_pass)
low_back.defvjp(back_keep, back_low)
NORM_EPS = 1e-05
BETA = 0.5
ADAM_EPS = 1e-08
DECAY = 0.01
VECTOR_RATE = 0.1
MASKED = -1000000000.0

def precise_dot(left, right):
    return jnp.dot(left, right, precision=lax.Precision.HIGHEST, preferred_element_type=jnp.float32)

def layer_norm(summed, gain_row, shift_row):
    average = lax.optimization_barrier(jnp.mean(summed, axis=-1, keepdims=True))
    centred = summed - average
    variance = lax.optimization_barrier(jnp.mean(centred * centred, axis=-1, keepdims=True))
    return centred * lax.rsqrt(variance + NORM_EPS) * gain_row + shift_row

def sequence_forward(token_rows, segment_row, feature_row, attention_low, feedforward_low, vector_low):
    expand = FF // D
    same_segment = segment_row[:, None] == segment_row[None, :]
    same_group = (same_segment & (feature_row[:, None] == feature_row[None, :])).astype(jnp.float32)
    members = lax.optimization_barrier(jnp.sum(same_group, axis=1, keepdims=True))
    merging = low_back(precise_dot(same_group, token_rows)) / members
    mixed = token_rows + vector_low[0] * merging
    rounded_in = low(mixed)
    queries = low(low_back((precise_dot(rounded_in, attention_low[0:D]) + vector_low[1]) * 0.125))
    key_rows = low(low_back(precise_dot(rounded_in, attention_low[D:2 * D])))
    values = low(low_back(precise_dot(rounded_in, attention_low[2 * D:3 * D]) + vector_low[2]))
    query_heads = queries.reshape(L, HEADS, HEAD_DIM)
    key_heads = key_rows.reshape(L, HEADS, HEAD_DIM)
    value_heads = values.reshape(L, HEADS, HEAD_DIM)
    scores = low_back(jnp.einsum('qhd,khd->hqk', query_heads, key_heads, precision=lax.Precision.HIGHEST))
    scores = jnp.where(same_segment[None], scores, MASKED)
    highest = lax.optimization_barrier(jnp.max(scores, axis=-1, keepdims=True))
    exponent = jnp.exp(scores - highest)
    attention = exponent / lax.optimization_barrier(jnp.sum(exponent, axis=-1, keepdims=True))
    context = jnp.einsum('hqk,khd->qhd', low(attention), value_heads, precision=lax.Precision.HIGHEST)
    context = low(low_back(context.reshape(L, D)))
    first_sum = mixed + low_back(precise_dot(context, attention_low[3 * D:4 * D])) + vector_low[3]
    normed = layer_norm(first_sum, vector_low[4], vector_low[5])
    up_rows = feedforward_low[0:FF]
    down_rows = feedforward_low[FF:2 * FF]
    hidden_pre = lax.dot_general(low(normed), up_rows, (((1,), (1,)), ((), ())), precision=lax.Precision.HIGHEST, preferred_element_type=jnp.float32)
    hidden_pre = low_back(hidden_pre + vector_low[6:6 + expand].reshape(FF))
    activated = low(jax.nn.gelu(hidden_pre, approximate=False))
    second_sum = normed + low_back(precise_dot(activated, down_rows)) + vector_low[6 + expand]
    return layer_norm(second_sum, vector_low[7 + expand], vector_low[8 + expand])

def adam_step(master, first, second, gradient, rate):
    first_new = BETA * first + (1.0 - BETA) * gradient
    second_new = BETA * second + (1.0 - BETA) * gradient * gradient
    correction = 1.0 - BETA ** ADAM_STEP
    master_new = master - rate * (first_new / correction / (jnp.sqrt(second_new / correction) + ADAM_EPS) + DECAY * master)
    return (master_new, first_new, second_new)

def reference(tokens, cotangent, segment_ids, feature_ids, attention_master, attention_first, attention_second, feedforward_master, feedforward_first, feedforward_second, vector_master, vector_first, vector_second):
    per_block = 8 if SEQS % 8 == 0 else 1
    block_count = SEQS // per_block
    segment_blocks = segment_ids.reshape(block_count, per_block, L)
    feature_blocks = feature_ids.reshape(block_count, per_block, L)

    def whole_layer(tokens_float, attention_float, feedforward_float, vector_float):
        weights = (low(attention_float), low(feedforward_float), low(vector_float))

        def one_block(running, inputs):
            token_block, segment_block, feature_block = inputs
            outputs = jax.vmap(sequence_forward, in_axes=(0, 0, 0, None, None, None))(token_block, segment_block, feature_block, running[0], running[1], running[2])
            return (running, outputs)
        token_blocks = tokens_float.reshape(block_count, per_block, L, D)
        _, stacked = lax.scan(jax.checkpoint(one_block), weights, (token_blocks, segment_blocks, feature_blocks))
        return stacked.reshape(TOKENS, D)
    tokens_float = tokens.astype(jnp.float32)
    output, pullback = jax.vjp(whole_layer, tokens_float, attention_master, feedforward_master, vector_master)
    tokens_grad, attention_grad, feedforward_grad, vector_grad = pullback(cotangent.astype(jnp.float32))
    attention_index = jnp.arange(4 * D)[:, None]
    attention_rate = jnp.where(attention_index < 3 * D, D ** (-0.5), (D // 64) ** (-0.5))
    feedforward_index = jnp.arange(2 * FF)[:, None]
    feedforward_rate = jnp.where(feedforward_index < FF, D ** (-0.5), FF ** (-0.5))
    attention_new, attention_first_new, attention_second_new = adam_step(attention_master, attention_first, attention_second, attention_grad, attention_rate)
    feedforward_new, feedforward_first_new, feedforward_second_new = adam_step(feedforward_master, feedforward_first, feedforward_second, feedforward_grad, feedforward_rate)
    vector_new, vector_first_new, vector_second_new = adam_step(vector_master, vector_first, vector_second, vector_grad, VECTOR_RATE)
    return (output.astype(jnp.bfloat16), tokens_grad.astype(jnp.bfloat16), attention_new, attention_first_new, attention_second_new, attention_new.astype(jnp.bfloat16), feedforward_new, feedforward_first_new, feedforward_second_new, feedforward_new.astype(jnp.bfloat16), vector_new, vector_first_new, vector_second_new, vector_new.astype(jnp.bfloat16))
```

```python
from functools import partial
import jax, jax.numpy as jnp
from jax import lax
from jax.experimental import pallas as pl
from jax.experimental.pallas import tpu as pltpu
from jax.sharding import PartitionSpec as P

D = 768
FF = 3072
HEADS = 12
HEAD_DIM = 64
NORM_EPS = 1e-05
AWAY = -1e30
F32, BF16 = jnp.float32, jnp.bfloat16
ERFC = (0.11841221385764535, 0.11979147087435008, 0.09737185909338779, 0.13434283549706147,
        -0.0652102059595758, 0.2202795624136942, -0.16009561537425632, 0.035107795064101)
VMEM = pltpu.VMEM


def nn(a, b):
    return lax.dot_general(a, b, (((1,), (0,)), ((), ())), preferred_element_type=F32)

def nt(a, b):
    return lax.dot_general(a, b, (((1,), (1,)), ((), ())), preferred_element_type=F32)

def tn(a, b):
    return lax.dot_general(a, b, (((0,), (0,)), ((), ())), preferred_element_type=F32)

def whole(shape):
    return pl.BlockSpec(shape, lambda i: (0,) * len(shape), pipeline_mode=pl.Buffered(1))

def gelu_pair(h):
    size = jnp.abs(h)
    t = 1.0 / (1.0 + (0.42 * 0.7071067811865476) * size)
    bell = jnp.exp(h * h * -0.5)
    poly = jnp.full_like(t, ERFC[-1])
    for coef in ERFC[-2::-1]:
        poly = poly * t + coef
    tail = poly * t * bell
    below = jnp.where(h < 0, tail, 1.0 - tail)
    return h * below, below + h * bell * 0.3989422804014327

def column_of(row):
    return jnp.transpose(jnp.broadcast_to(row, (8, row.shape[1])))[:, :1]

def group_of(seg, feat):
    both = seg * 16 + feat
    return column_of(both) == both

def k1_body(tok_ref, seg_ref, feat_ref, w_ref, vec_ref, mixed_ref, q_ref, k_ref, v_ref, ctx_ref, lse_ref, bias_scr):
    i = pl.program_id(0)
    seg = seg_ref[pl.ds(i, 1), :]
    feat = feat_ref[pl.ds(i, 1), :]
    length = seg.shape[1]
    bias_scr[...] = jnp.where(column_of(seg) == seg, 0.0, AWAY)
    group = group_of(seg, feat)
    members = jnp.sum(group.astype(F32), axis=1, keepdims=True)
    tok = tok_ref[...]
    merging = nn(group.astype(F32).astype(BF16), tok) / members
    mixed = tok.astype(F32) + vec_ref[0:1, :] * merging
    mixed_ref[...] = mixed
    mb = mixed.astype(BF16)
    q_ref[...] = ((nn(mb, w_ref[0:D, :]) + vec_ref[1:2, :]) * 0.125).astype(BF16)
    k_ref[...] = nn(mb, w_ref[D:2 * D, :]).astype(BF16)
    v_ref[...] = (nn(mb, w_ref[2 * D:3 * D, :]) + vec_ref[2:3, :]).astype(BF16)
    lane = lax.broadcasted_iota(jnp.int32, (length, 128), 1)
    low = lane < HEAD_DIM
    lse_ref[...] = jnp.zeros_like(lse_ref)

    def pair(p, carry):
        at = pl.ds(pl.multiple_of(p * 128, 128), 128)
        qp = q_ref[:, at]
        kp = k_ref[:, at]
        vp = v_ref[:, at]
        outs = []
        zero = jnp.zeros_like(qp)
        for half in range(2):
            mine = low if half == 0 else jnp.logical_not(low)
            s = nt(jnp.where(mine, qp, zero), kp) + bias_scr[...]
            top = jnp.max(s, axis=1, keepdims=True)
            e = jnp.exp(s - top)
            total = jnp.sum(e, axis=1, keepdims=True)
            o = nn(e.astype(BF16), vp) * (1.0 / total)
            outs.append(o)
            lse_ref[...] = jnp.where(lane == 2 * p + half, top + jnp.log(total), lse_ref[...])
        ctx_ref[:, at] = jnp.where(low, outs[0], outs[1]).astype(BF16)
        return carry
    lax.fori_loop(0, HEADS // 2, pair, 0)


def k1(tokens, seg, feat, att, vec):
    seqs, length = seg.shape
    blk = pl.BlockSpec((length, D), lambda i: (i, 0))
    n = seqs * length
    o = lambda dt: jax.ShapeDtypeStruct((n, D), dt)
    return pl.pallas_call(
        k1_body, grid=(seqs,),
        in_specs=[blk, whole((seqs, length)), whole((seqs, length)), pl.BlockSpec((3 * D, D), lambda i: (0, 0), pipeline_mode=pl.Buffered(1)), whole(vec.shape)],
        out_specs=[blk] * 5 + [pl.BlockSpec((length, 128), lambda i: (i, 0))],
        out_shape=[o(F32), o(BF16), o(BF16), o(BF16), o(BF16), jax.ShapeDtypeStruct((n, 128), F32)],
        scratch_shapes=[VMEM((length, length), F32)],
        name="mix_attend",
    )(tokens, seg, feat, att, vec)

def norm_parts(z):
    mean = jnp.mean(z, axis=1, keepdims=True)
    c = z - mean
    var = jnp.mean(c * c, axis=1, keepdims=True)
    inv = lax.rsqrt(var + NORM_EPS)
    return c * inv, inv

def norm_pull(g, xhat, inv):
    a = jnp.mean(g, axis=1, keepdims=True)
    b = jnp.mean(g * xhat, axis=1, keepdims=True)
    return (g - a - xhat * b) * inv

def colsum(x):
    return jnp.sum(x, axis=0, keepdims=True)

def k2_body(mixed_ref, ctx_ref, cot_ref, wo_ref, wf_ref, vec_ref,
            out_ref, first_ref, fb_ref, dctx_ref, act_ref, hg_ref, nb_ref, bg_ref, vg_ref, gp_scr, sum_scr):
    @pl.when(pl.program_id(0) == 0)
    def _():
        vg_ref[...] = jnp.zeros_like(vg_ref)
    ex = FF // D
    first_sum = mixed_ref[...] + nn(ctx_ref[...], wo_ref[...]) + vec_ref[3:4, :]
    xhat1, inv1 = norm_parts(first_sum)
    normed = xhat1 * vec_ref[4:5, :] + vec_ref[5:6, :]
    nb_ref[...] = normed.astype(BF16)
    sum_scr[...] = normed + vec_ref[6 + ex:7 + ex, :]
    for c in range(ex):
        at = pl.ds(c * D, D)
        h = nt(nb_ref[...], wf_ref[at, :]) + vec_ref[6 + c:7 + c, :]
        act, slope = gelu_pair(h)
        act_ref[:, at] = act.astype(BF16)
        gp_scr[:, at] = slope.astype(gp_scr.dtype)
        sum_scr[...] += nn(act_ref[:, at], wf_ref[pl.ds(FF + c * D, D), :])
    xhat2, inv2 = norm_parts(sum_scr[...])
    out_ref[...] = (xhat2 * vec_ref[7 + ex:8 + ex, :] + vec_ref[8 + ex:9 + ex, :]).astype(BF16)
    cot = cot_ref[...].astype(F32)
    vg_ref[4 + ex:5 + ex, :] += colsum(cot * xhat2)
    vg_ref[5 + ex:6 + ex, :] += colsum(cot)
    gs = norm_pull(cot * vec_ref[7 + ex:8 + ex, :], xhat2, inv2)
    vg_ref[3 + ex:4 + ex, :] += colsum(gs)
    bg_ref[...] = gs.astype(BF16)
    sum_scr[...] = gs
    for c in range(ex):
        at = pl.ds(c * D, D)
        hg = nt(bg_ref[...], wf_ref[pl.ds(FF + c * D, D), :]) * gp_scr[:, at].astype(F32)
        vg_ref[3 + c:4 + c, :] += colsum(hg)
        hg_ref[:, at] = hg.astype(BF16)
        sum_scr[...] += nn(hg_ref[:, at], wf_ref[at, :])
    ng = sum_scr[...]
    vg_ref[1:2, :] += colsum(ng * xhat1)
    vg_ref[2:3, :] += colsum(ng)
    fgr = norm_pull(ng * vec_ref[4:5, :], xhat1, inv1)
    vg_ref[0:1, :] += colsum(fgr)
    first_ref[...] = fgr
    fb_ref[...] = fgr.astype(BF16)
    dctx_ref[...] = nt(fb_ref[...], wo_ref[...]).astype(BF16)


def k2(mixed, ctx, cot, att, ff, vec, tile=256):
    n = mixed.shape[0]
    blk = pl.BlockSpec((tile, D), lambda i: (i, 0))
    wide = pl.BlockSpec((tile, FF), lambda i: (i, 0))
    o = lambda w, dt: jax.ShapeDtypeStruct((n, w), dt)
    return pl.pallas_call(
        k2_body, grid=(n // tile,),
        in_specs=[blk, blk, blk, pl.BlockSpec((D, D), lambda i: (3, 0), pipeline_mode=pl.Buffered(1)), whole(ff.shape), whole(vec.shape)],
        out_specs=[blk, blk, blk, blk, wide, wide, blk, blk, pl.BlockSpec((16, D), lambda i: (0, 0))],
        out_shape=[o(D, BF16), o(D, F32), o(D, BF16), o(D, BF16), o(FF, BF16), o(FF, BF16), o(D, BF16), o(D, BF16), jax.ShapeDtypeStruct((16, D), F32)],
        scratch_shapes=[VMEM((tile, FF), F32), VMEM((tile, D), F32)],
        name="feed_forward",
    )(mixed, ctx, cot, att, ff, vec)

def k3_body(q_ref, k_ref, v_ref, ctx_ref, dctx_ref, lse_ref, seg_ref, dq_ref, dk_ref, dv_ref, vg_ref, bias_scr, lse_scr, del_scr):
    i = pl.program_id(0)
    @pl.when(i == 0)
    def _():
        vg_ref[...] = jnp.zeros_like(vg_ref)
    seg = seg_ref[pl.ds(i, 1), :]
    length = seg.shape[1]
    bias_scr[...] = jnp.where(column_of(seg) == seg, 0.0, AWAY)
    lse_scr[...] = jnp.transpose(lse_ref[...])[:16, :]
    prod = dctx_ref[...].astype(F32) * ctx_ref[...].astype(F32)
    pick = (lax.broadcasted_iota(jnp.int32, (16, D), 1) // HEAD_DIM == lax.broadcasted_iota(jnp.int32, (16, D), 0)).astype(F32)
    del_scr[...] = lax.dot_general(pick, prod, (((1,), (1,)), ((), ())), precision=lax.Precision.HIGHEST, preferred_element_type=F32)
    low = lax.broadcasted_iota(jnp.int32, (length, 128), 1) < HEAD_DIM

    def pair(p, carry):
        at = pl.ds(pl.multiple_of(p * 128, 128), 128)
        qp, kp, vp, op = q_ref[:, at], k_ref[:, at], v_ref[:, at], dctx_ref[:, at]
        zero = jnp.zeros_like(qp)
        got = []
        for half in range(2):
            mine = low if half == 0 else jnp.logical_not(low)
            st = nt(jnp.where(mine, kp, zero), qp) + bias_scr[...]
            pt = jnp.exp(st - lse_scr[pl.ds(2 * p + half, 1), :])
            dv = nn(pt.astype(BF16), op)
            dpt = nt(jnp.where(mine, vp, zero), op)
            dst = (pt * (dpt - del_scr[pl.ds(2 * p + half, 1), :])).astype(BF16)
            dk = nn(dst, qp)
            dq = tn(dst, kp)
            got.append((dq, dk, dv))
        dq, dk, dv = (jnp.where(low, a, b) for a, b in zip(*got))
        dqb = dq.astype(BF16) * jnp.bfloat16(0.125)
        dvb = dv.astype(BF16)
        dq_ref[:, at] = dqb
        dk_ref[:, at] = dk.astype(BF16)
        dv_ref[:, at] = dvb
        vg_ref[0:1, at] += colsum(dqb.astype(F32))
        vg_ref[1:2, at] += colsum(dvb.astype(F32))
        return carry
    lax.fori_loop(0, HEADS // 2, pair, 0)


def k3(q, k, v, ctx, dctx, lse, seg):
    seqs, length = seg.shape
    n = seqs * length
    blk = pl.BlockSpec((length, D), lambda i: (i, 0))
    o = jax.ShapeDtypeStruct((n, D), BF16)
    return pl.pallas_call(
        k3_body, grid=(seqs,),
        in_specs=[blk] * 5 + [pl.BlockSpec((length, 128), lambda i: (i, 0)), whole((seqs, length))],
        out_specs=[blk] * 3 + [pl.BlockSpec((8, D), lambda i: (0, 0))],
        out_shape=[o, o, o, jax.ShapeDtypeStruct((8, D), F32)],
        scratch_shapes=[VMEM((length, length), F32), VMEM((16, length), F32), VMEM((16, length), F32)],
        name="attend_back",
    )(q, k, v, ctx, dctx, lse, seg)

def k4_body(first_ref, dq_ref, dk_ref, dv_ref, tok_ref, mixed_ref, seg_ref, feat_ref, w_ref, vec_ref, tg_ref, vg_ref):
    i = pl.program_id(0)
    @pl.when(i == 0)
    def _():
        vg_ref[...] = jnp.zeros_like(vg_ref)
    group = group_of(seg_ref[pl.ds(i, 1), :], feat_ref[pl.ds(i, 1), :])
    gf = group.astype(F32)
    members = jnp.sum(gf, axis=1, keepdims=True)
    gb = gf.astype(BF16)
    tok = tok_ref[...]
    merging = nn(gb, tok) / members
    mg = (first_ref[...] + nt(dq_ref[...], w_ref[0:D, :]) + nt(dk_ref[...], w_ref[D:2 * D, :])
          + nt(dv_ref[...], w_ref[2 * D:3 * D, :]))
    vg_ref[0:1, :] += colsum(mg * merging)
    spread = (vec_ref[0:1, :] * mg / members).astype(BF16)
    tg_ref[...] = (mg + nn(gb, spread)).astype(BF16)


def k4(first, dq, dk, dv, tokens, mixed, seg, feat, att, vec):
    seqs, length = seg.shape
    n = seqs * length
    blk = pl.BlockSpec((length, D), lambda i: (i, 0))
    return pl.pallas_call(
        k4_body, grid=(seqs,),
        in_specs=[blk] * 5 + [blk, whole((seqs, length)), whole((seqs, length)), pl.BlockSpec((3 * D, D), lambda i: (0, 0), pipeline_mode=pl.Buffered(1)), whole(vec.shape)],
        out_specs=[blk, pl.BlockSpec((8, D), lambda i: (0, 0))],
        out_shape=[jax.ShapeDtypeStruct((n, D), BF16), jax.ShapeDtypeStruct((8, D), F32)],
        name="token_grad",
    )(first, dq, dk, dv, tokens, mixed, seg, feat, att, vec)

def adam_step(master, first, second, gradient, rate):
    first_new = BETA * first + (1.0 - BETA) * gradient
    second_new = BETA * second + (1.0 - BETA) * gradient * gradient
    correction = 1.0 - BETA**ADAM_STEP
    master_new = master - rate * (
        first_new / correction / (jnp.sqrt(second_new / correction) + ADAM_EPS) + DECAY * master
    )
    return (master_new, first_new, second_new)


BETA = 0.5
ADAM_STEP = 3
ADAM_EPS = 1e-08
DECAY = 0.01
VECTOR_RATE = 0.1
BOTH = ("wide", "narrow")


def rates(rows, split, first_rate, second_rate):
    index = (lax.axis_index(BOTH) * rows + jnp.arange(rows))[:, None]
    return jnp.where(index < split, first_rate, second_rate)


def local(tokens, cotangent, segment_ids, feature_ids,
          attention_master, attention_first, attention_second,
          feedforward_master, feedforward_first, feedforward_second,
          vector_master, vector_first, vector_second):
    gather = partial(lax.all_gather, axis_name=BOTH, tiled=True)
    att = gather(attention_master.astype(BF16), axis=0)
    ff = gather(feedforward_master.astype(BF16), axis=0)
    vec = jnp.pad(gather(vector_master.astype(BF16), axis=1).astype(F32), ((0, 3), (0, 0)))
    seg, feat = segment_ids, feature_ids
    mixed, q, k, v, ctx, lse = k1(tokens, seg, feat, att, vec)
    out, first, fb, dctx, act, hg, nb, bg, vg2 = k2(mixed, ctx, cotangent, att, ff, vec)
    scatter = partial(lax.psum_scatter, axis_name=BOTH, tiled=True)
    ff_grad = jnp.concatenate([tn(hg, nb), tn(act, bg)], axis=0).astype(BF16)
    ff_owned = scatter(ff_grad, scatter_dimension=0).astype(F32)
    dq, dk, dv, vg3 = k3(q, k, v, ctx, dctx, lse, seg)
    mb = mixed.astype(BF16)
    att_grad = jnp.concatenate([tn(mb, dq), tn(mb, dk), tn(mb, dv), tn(ctx, fb)], axis=0).astype(BF16)
    att_owned = scatter(att_grad, scatter_dimension=0).astype(F32)
    token_grads, vg4 = k4(first, dq, dk, dv, tokens, mixed, seg, feat, att, vec)
    vec_grad = jnp.concatenate([vg4[0:1], vg3[0:2], vg2[:10]], axis=0)
    vec_owned = scatter(vec_grad, scatter_dimension=1)
    ff_rate = rates(feedforward_master.shape[0], FF, D ** (-0.5), FF ** (-0.5))
    att_rate = rates(attention_master.shape[0], 3 * D, D ** (-0.5), (D // 64) ** (-0.5))
    f_new = adam_step(feedforward_master, feedforward_first, feedforward_second, ff_owned, ff_rate)
    a_new = adam_step(attention_master, attention_first, attention_second, att_owned, att_rate)
    v_new = adam_step(vector_master, vector_first, vector_second, vec_owned, VECTOR_RATE)
    result = [out, token_grads]
    for new in (a_new, f_new, v_new):
        result += [*new, new[0].astype(BF16)]
    return tuple(result)


def solution(mesh):
    rows, cols = P(BOTH, None), P(None, BOTH)
    return jax.shard_map(
        local, mesh=mesh,
        in_specs=(rows,) * 10 + (cols,) * 3,
        out_specs=(rows,) * 10 + (cols,) * 4,
        check_vma=False,
    )
```

```python
from functools import partial
import jax, jax.numpy as jnp
from jax import lax
from jax.experimental import pallas as pl
from jax.experimental.pallas import tpu as pltpu
from jax.sharding import PartitionSpec as P

D = 768
FF = 3072
HEADS = 12
HEAD_DIM = 64
NORM_EPS = 1e-05
AWAY = -1e30
F32, BF16 = jnp.float32, jnp.bfloat16
ERFC = (0.11841221385764535, 0.11979147087435008, 0.09737185909338779, 0.13434283549706147,
        -0.0652102059595758, 0.2202795624136942, -0.16009561537425632, 0.035107795064101)
VMEM = pltpu.VMEM


def nn(a, b):
    return lax.dot_general(a, b, (((1,), (0,)), ((), ())), preferred_element_type=F32)

def nt(a, b):
    return lax.dot_general(a, b, (((1,), (1,)), ((), ())), preferred_element_type=F32)

def tn(a, b):
    return lax.dot_general(a, b, (((0,), (0,)), ((), ())), preferred_element_type=F32)

def whole(shape):
    return pl.BlockSpec(shape, lambda *_: (0,) * len(shape), pipeline_mode=pl.Buffered(1))

def gelu_pair(h):
    size = jnp.abs(h)
    t = 1.0 / (1.0 + (0.42 * 0.7071067811865476) * size)
    bell = jnp.exp(h * h * -0.5)
    poly = jnp.full_like(t, ERFC[-1])
    for coef in ERFC[-2::-1]:
        poly = poly * t + coef
    tail = poly * t * bell
    below = jnp.where(h < 0, tail, 1.0 - tail)
    return h * below, below + h * bell * 0.3989422804014327

def column_of(row):
    return jnp.transpose(jnp.broadcast_to(row, (8, row.shape[1])))[:, :1]

def group_of(seg, feat):
    both = seg * 16 + feat
    return column_of(both) == both

def cost(gigaflops, megabytes):
    return pl.CostEstimate(flops=int(gigaflops * 1e9), bytes_accessed=int(megabytes * 1e6), transcendentals=0)


def fetch_weights(me, offsets, pieces, w_ref, sem):
    rows = pieces[0].shape[1]
    half = D // 2
    copies = []
    for j, offset in enumerate(offsets):
        for side in range(2):
            for col in range(2):
                owner = (me ^ offset[col]) if side == 0 else (me ^ offset[col] ^ offset[2])
                at = pl.ds(pl.multiple_of(owner * rows, 8), rows)
                copies.append(pltpu.make_async_copy(pieces[2 * side + col].at[j], w_ref.at[at, pl.ds(col * half, half)], sem))
    for c in copies:
        c.start()
    for c in copies:
        c.wait()

def attend_forward(i, tok_ref, seg_ref, feat_ref, w_ref, vec_ref, mixed_ref, q_ref, k_ref, v_ref, ctx_ref, lse_ref, bias_scr, service):
    seg = seg_ref[pl.ds(i, 1), :]
    feat = feat_ref[pl.ds(i, 1), :]
    length = seg.shape[1]
    bias_scr[...] = jnp.where(column_of(seg) == seg, 0.0, AWAY)
    group = group_of(seg, feat)
    members = jnp.sum(group.astype(F32), axis=1, keepdims=True)
    tok = tok_ref[...]
    merging = nn(group.astype(F32).astype(BF16), tok) / members
    mixed = tok.astype(F32) + vec_ref[0:1, :] * merging
    mixed_ref[...] = mixed
    mb = mixed.astype(BF16)
    ctx_ref[0] = mb
    q_ref[...] = ((nn(mb, w_ref[0:D, :]) + vec_ref[1:2, :]) * 0.125).astype(BF16)
    k_ref[...] = nn(mb, w_ref[D:2 * D, :]).astype(BF16)
    v_ref[...] = (nn(mb, w_ref[2 * D:3 * D, :]) + vec_ref[2:3, :]).astype(BF16)
    lane = lax.broadcasted_iota(jnp.int32, (length, 128), 1)
    low = lane < HEAD_DIM
    lse_ref[...] = jnp.zeros_like(lse_ref)

    def pair(p, carry):
        at = pl.ds(pl.multiple_of(p * 128, 128), 128)
        qp = q_ref[:, at]
        kp = k_ref[:, at]
        vp = v_ref[:, at]
        outs = []
        zero = jnp.zeros_like(qp)
        for half in range(2):
            mine = low if half == 0 else jnp.logical_not(low)
            s = nt(jnp.where(mine, qp, zero), kp) + bias_scr[...]
            top = jnp.max(s, axis=1, keepdims=True)
            e = jnp.exp(s - top)
            total = jnp.sum(e, axis=1, keepdims=True)
            o = nn(e.astype(BF16), vp) * (1.0 / total)
            outs.append(o)
            lse_ref[...] = jnp.where(lane == 2 * p + half, top + jnp.log(total), lse_ref[...])
        ctx_ref[1, :, at] = jnp.where(low, outs[0], outs[1]).astype(BF16)
        return carry
    service(0)
    lax.fori_loop(0, HEADS // 4, pair, 0)
    service(1)
    lax.fori_loop(HEADS // 4, HEADS // 2, pair, 0)
    service(2)


def k1_body(first_seq, offsets, kept, self_ref, tok_ref, seg_ref, feat_ref, vec_ref, *rest):
    if kept:
        w_ref, rest = rest[0], rest[1 + kept:]
        mixed_ref, q_ref, k_ref, v_ref, ctx_ref, lse_ref, bias_scr = rest
    else:
        pieces, rest = rest[:4], rest[4:]
        mixed_ref, q_ref, k_ref, v_ref, ctx_ref, lse_ref, w_ref, bias_scr, sem = rest
    i = pl.program_id(0) + first_seq

    if not kept:
        @pl.when(pl.program_id(0) == 0)
        def _():
            fetch_weights(self_ref[0], offsets, pieces, w_ref, sem)

    attend_forward(i, tok_ref, seg_ref, feat_ref, w_ref, vec_ref, mixed_ref, q_ref, k_ref, v_ref, ctx_ref, lse_ref, bias_scr, lambda point: None)


def k1(first_seq, count, me, tokens, seg, feat, weights, offsets, vec, kept):
    seqs, length = seg.shape
    blk = pl.BlockSpec((length, D), lambda i, s: (i + first_seq, 0))
    both = pl.BlockSpec((2, length, D), lambda i, s: (0, i + first_seq, 0))
    narrow = pl.BlockSpec((length, 128), lambda i, s: (i + first_seq, 0))
    n = seqs * length
    o = lambda dt: jax.ShapeDtypeStruct((n, D), dt)
    any_spec = pl.BlockSpec(memory_space=pl.ANY)
    out_specs = [blk] * 4 + [both, narrow]
    out_shape = [o(F32), o(BF16), o(BF16), o(BF16), jax.ShapeDtypeStruct((2, n, D), BF16), jax.ShapeDtypeStruct((n, 128), F32)]
    scratch = [VMEM((length, length), F32)]
    if kept:
        weight_specs = [pl.BlockSpec((3 * D, D), lambda i, s: (0, 0), pipeline_mode=pl.Buffered(1))]
    else:
        weight_specs = [any_spec] * 4
        out_specs = out_specs + [whole((4 * D, D))]
        out_shape = out_shape + [jax.ShapeDtypeStruct((4 * D, D), BF16)]
        scratch = scratch + [pltpu.SemaphoreType.DMA]
    return pl.pallas_call(
        partial(k1_body, first_seq, offsets, len(kept)),
        grid_spec=pltpu.PrefetchScalarGridSpec(
            num_scalar_prefetch=1, grid=(count,),
            in_specs=[blk, whole(seg.shape), whole(feat.shape), whole(vec.shape)] + weight_specs + [any_spec] * len(kept),
            out_specs=out_specs, scratch_shapes=scratch,
        ),
        out_shape=out_shape,
        input_output_aliases={6 + j: j for j in range(len(kept))},
        cost_estimate=cost(count * 11, count * 4),
        name="mix_attend",
    )(me, tokens, seg, feat, vec, *weights, *kept)

MESH = pl.DeviceIdType.MESH


def flips(x, mask):
    bit = 1
    while bit <= mask:
        if mask & bit:
            x = x + bit - 2 * bit * ((x // bit) % 2)
        bit *= 2
    return x


class Spreading:
    def __init__(self, wide, narrow, shard, full, columns, sems):
        self.narrow, self.masks = narrow, wide // 2
        self.bits = [1 << b for b in range((wide // 2).bit_length() - 1)]
        w, self.z = lax.axis_index("wide"), lax.axis_index("narrow")
        self.o, self.c = w // 2, w % 2
        self.shard, self.full, self.columns = shard, full, columns
        self.line_out, self.line_in, self.tree_out, self.tree_in, self.core_out, self.core_in, self.own = sems

    def at(self, r, k, c=None, h=None):
        c = self.c if c is None else c
        rows = self.shard.shape[0]
        owner = (2 * flips(self.o, r) + c) * self.narrow + flips(self.z, k)
        where = pl.ds(pl.multiple_of(owner * rows, 8), rows)
        if h is None:
            return self.full.at[where, :]
        return self.full.at[where, pl.ds(*self.columns[h][:2])]

    def source(self, r, k, h=None):
        if r or k:
            return self.at(r, k, None, h)
        return self.shard if h is None else self.shard.at[:, pl.ds(*self.columns[h][:2])]

    def keep(self):
        return pltpu.make_async_copy(self.shard, self.at(0, 0), self.own)

    def line(self, k, arriving=False):
        return pltpu.make_async_remote_copy(
            self.shard, self.at(0, k if arriving else 0), self.line_out.at[k - 1], self.line_in.at[k - 1],
            device_id=(2 * self.o + self.c, flips(self.z, k)), device_id_type=MESH)

    def tree(self, r, k, h, bit, arriving=False):
        there = r if arriving else r ^ bit
        n = (k * len(self.columns) + h) * self.masks + there
        part = self.at(r, k, None, h)
        return pltpu.make_async_remote_copy(
            part if arriving else self.source(r, k, h), part, self.tree_out.at[n], self.tree_in.at[n],
            device_id=(2 * flips(self.o, bit) + self.c, self.z), device_id_type=MESH)

    def core(self, r, k, arriving=False):
        n = k * self.masks + r
        part = self.at(r, k, 1 - self.c if arriving else None)
        return pltpu.make_async_remote_copy(
            part if arriving else self.source(r, k), part, self.core_out.at[n], self.core_in.at[n],
            device_id=(2 * self.o + 1 - self.c, self.z), device_id_type=MESH)

    def onward(self, r, h):
        if self.columns[h][2]:
            return [b for b in reversed(self.bits) if r == 0 or b < (r & -r)]
        return [b for b in self.bits if b > r]

    def last_bit(self, r, h):
        if self.columns[h][2]:
            return r & -r
        return 1 << (r.bit_length() - 1)

    def open(self):
        self.keep().start()
        for k in range(1, self.narrow):
            self.line(k).start()

    def send_on(self, r, k, h):
        for bit in self.onward(r, h):
            self.tree(r, k, h, bit).start()

    def roots(self, k):
        if k:
            self.line(k, True).wait_recv()
        for h in range(len(self.columns)):
            self.send_on(0, k, h)
        self.core(0, k).start()

    def relay(self, r, k):
        for h in range(len(self.columns)):
            self.tree(r, k, h, self.last_bit(r, h), True).wait_recv()
            self.send_on(r, k, h)
        self.core(r, k).start()

    def close(self):
        for k in range(self.narrow):
            for r in range(self.masks):
                self.core(r, k, True).wait_recv()
        self.keep().wait()

    def drain(self):
        for k in range(self.narrow):
            if k:
                self.line(k).wait_send()
            for r in range(self.masks):
                for h in range(len(self.columns)):
                    for bit in self.onward(r, h):
                        self.tree(r, k, h, bit).wait_send()
                self.core(r, k).wait_send()


def spreading_sems(wide, narrow, halves):
    dma = pltpu.SemaphoreType.DMA
    tree, core = narrow * halves * (wide // 2), narrow * (wide // 2)
    return [dma((narrow - 1,)), dma((narrow - 1,)), dma((tree,)), dma((tree,)), dma((core,)), dma((core,)), dma]


def greet(wide, narrow):
    barrier = pltpu.get_barrier_semaphore()
    w, z = lax.axis_index("wide"), lax.axis_index("narrow")
    o, c = w // 2, w % 2
    peers = [(w, flips(z, k)) for k in range(1, narrow)] + [(2 * o + 1 - c, z)]
    bit = 1
    while bit < wide // 2:
        peers.append((2 * flips(o, bit) + c, z))
        bit *= 2
    for peer in peers:
        pl.semaphore_signal(barrier, inc=1, device_id=peer, device_id_type=MESH)
    pl.semaphore_wait(barrier, len(peers))


def gathering_k1_body(wide, narrow, cols, steps, tok_ref, seg_ref, feat_ref, att_ref, ff_ref, vs_ref,
                      mixed_ref, q_ref, k_ref, v_ref, ctx_ref, lse_ref, vec_ref, wout_ref, fout_ref,
                      bias_scr, w_ref, vs_scr, put_sem, *sems):
    i = pl.program_id(0)
    half = D // 2
    count = len(sems) // 3
    pairs = [(0, half, False), (half, half, True)]
    att = Spreading(wide, narrow, att_ref, w_ref, pairs, sems[:count])
    ff = Spreading(wide, narrow, ff_ref, fout_ref, pairs, sems[count:2 * count])
    vs = Spreading(wide, narrow, vs_ref, vs_scr, [(0, 128, False)], sems[2 * count:])
    singles = [r for r in range(1, wide // 2)]
    save = pltpu.make_async_copy(w_ref, wout_ref, put_sem)

    @pl.when(i == 0)
    def _():
        greet(wide, narrow)
        for one in (vs, att, ff):
            one.open()
        for k in range(narrow):
            vs.roots(k)
            att.roots(k)
        ff.roots(0)
        for r in singles:
            for k in range(narrow):
                vs.relay(r, k)
                att.relay(r, k)
        vs.close()
        vec = jnp.zeros((16, D), F32)
        row = lax.broadcasted_iota(jnp.int32, (128, D), 0)
        col = lax.broadcasted_iota(jnp.int32, (128, D), 1)
        for d in range(wide * narrow):
            pick = jnp.logical_and(row < cols, col == row + cols * d).astype(F32).astype(BF16)
            vec = vec + nn(vs_scr[16 * d:16 * d + 16, :], pick)
        vec_ref[...] = vec
        att.close()
        save.start()

    plan = [lambda k=k: ff.roots(k) for k in range(1, narrow)]
    for r in singles:
        plan += [lambda r=r, k=k: ff.relay(r, k) for k in range(narrow)]

    def service(point):
        for s in range(steps):
            todo = slots.get((s, point), ())
            if todo:
                @pl.when(i == s)
                def _(todo=todo):
                    for act in todo:
                        act()
    total = steps * 3 - 1
    slots = {}
    for n, act in enumerate(plan):
        spot = n * total // len(plan)
        slots.setdefault((spot // 3, spot % 3), []).append(act)

    attend_forward(i, tok_ref, seg_ref, feat_ref, w_ref, vec_ref, mixed_ref, q_ref, k_ref, v_ref, ctx_ref, lse_ref, bias_scr, service)

    @pl.when(i == steps - 1)
    def _():
        ff.close()
        for one in (vs, att, ff):
            one.drain()
        save.wait()


def gathering_k1(wide, narrow, tokens, seg, feat, att_shard, ff_shard, vec_shard):
    seqs, length = seg.shape
    n, devices = seqs * length, wide * narrow
    vs = jnp.pad(vec_shard, ((0, 16 - vec_shard.shape[0]), (0, 128 - vec_shard.shape[1])))
    blk = pl.BlockSpec((length, D), lambda i: (i, 0))
    any_spec = pl.BlockSpec(memory_space=pl.ANY)
    o = lambda dt: jax.ShapeDtypeStruct((n, D), dt)
    sems = spreading_sems(wide, narrow, 2) * 2 + spreading_sems(wide, narrow, 1)
    return pl.pallas_call(
        partial(gathering_k1_body, wide, narrow, vec_shard.shape[1], seqs), grid=(seqs,),
        in_specs=[blk, whole(seg.shape), whole(feat.shape), any_spec, any_spec, any_spec],
        out_specs=[blk] * 4 + [pl.BlockSpec((2, length, D), lambda i: (0, i, 0)), pl.BlockSpec((length, 128), lambda i: (i, 0)),
                               whole((16, D)), any_spec, any_spec],
        out_shape=[o(F32), o(BF16), o(BF16), o(BF16), jax.ShapeDtypeStruct((2, n, D), BF16), jax.ShapeDtypeStruct((n, 128), F32),
                   jax.ShapeDtypeStruct((16, D), F32), jax.ShapeDtypeStruct((4 * D, D), BF16), jax.ShapeDtypeStruct((2 * FF, D), BF16)],
        scratch_shapes=[VMEM((length, length), F32), VMEM((4 * D, D), BF16), VMEM((16 * devices, 128), BF16), pltpu.SemaphoreType.DMA, *sems],
        compiler_params=pltpu.CompilerParams(collective_id=0, has_side_effects=True),
        cost_estimate=cost(60, 60),
        name="gather_attend",
    )(tokens, seg, feat, att_shard, ff_shard, vs)

def norm_parts(z):
    mean = jnp.mean(z, axis=1, keepdims=True)
    c = z - mean
    var = jnp.mean(c * c, axis=1, keepdims=True)
    inv = lax.rsqrt(var + NORM_EPS)
    return c * inv, inv

def norm_pull(g, xhat, inv):
    a = jnp.mean(g, axis=1, keepdims=True)
    b = jnp.mean(g * xhat, axis=1, keepdims=True)
    return (g - a - xhat * b) * inv

def colsum(x):
    return jnp.sum(x, axis=0, keepdims=True)

def k2_body(offsets, self_ref, mixed_ref, ctx_ref, cot_ref, wo_ref, vec_ref, *rest):
    if offsets:
        pieces, rest = rest[:4], rest[4:]
        out_ref, first_ref, fb_ref, dctx_ref, wide_ref, slim_ref, vg_ref, gp_scr, sum_scr, wf_ref, sem = rest
    else:
        wf_ref, out_ref, first_ref, fb_ref, dctx_ref, wide_ref, slim_ref, vg_ref, gp_scr, sum_scr = rest
    ctx_ref = ctx_ref.at[0]
    hg_ref, act_ref = wide_ref.at[0], wide_ref.at[1]
    nb_ref, bg_ref = slim_ref.at[0], slim_ref.at[1]
    @pl.when(pl.program_id(0) == 0)
    def _():
        vg_ref[...] = jnp.zeros_like(vg_ref)
        if offsets:
            fetch_weights(self_ref[0], offsets, pieces, wf_ref, sem)

    ex = FF // D
    first_sum = mixed_ref[...] + nn(ctx_ref[...], wo_ref[...]) + vec_ref[3:4, :]
    xhat1, inv1 = norm_parts(first_sum)
    normed = xhat1 * vec_ref[4:5, :] + vec_ref[5:6, :]
    nb_ref[...] = normed.astype(BF16)
    sum_scr[...] = normed + vec_ref[6 + ex:7 + ex, :]
    for c in range(ex):
        at = pl.ds(c * D, D)
        h = nt(nb_ref[...], wf_ref[at, :]) + vec_ref[6 + c:7 + c, :]
        act, slope = gelu_pair(h)
        act_ref[:, at] = act.astype(BF16)
        gp_scr[:, at] = slope.astype(gp_scr.dtype)
        sum_scr[...] += nn(act_ref[:, at], wf_ref[pl.ds(FF + c * D, D), :])
    xhat2, inv2 = norm_parts(sum_scr[...])
    out_ref[...] = (xhat2 * vec_ref[7 + ex:8 + ex, :] + vec_ref[8 + ex:9 + ex, :]).astype(BF16)
    cot = cot_ref[...].astype(F32)
    vg_ref[4 + ex:5 + ex, :] += colsum(cot * xhat2)
    vg_ref[5 + ex:6 + ex, :] += colsum(cot)
    gs = norm_pull(cot * vec_ref[7 + ex:8 + ex, :], xhat2, inv2)
    vg_ref[3 + ex:4 + ex, :] += colsum(gs)
    bg_ref[...] = gs.astype(BF16)
    sum_scr[...] = gs
    for c in range(ex):
        at = pl.ds(c * D, D)
        hg = nt(bg_ref[...], wf_ref[pl.ds(FF + c * D, D), :]) * gp_scr[:, at].astype(F32)
        vg_ref[3 + c:4 + c, :] += colsum(hg)
        hg_ref[:, at] = hg.astype(BF16)
        sum_scr[...] += nn(hg_ref[:, at], wf_ref[at, :])
    ng = sum_scr[...]
    vg_ref[1:2, :] += colsum(ng * xhat1)
    vg_ref[2:3, :] += colsum(ng)
    fgr = norm_pull(ng * vec_ref[4:5, :], xhat1, inv1)
    vg_ref[0:1, :] += colsum(fgr)
    first_ref[...] = fgr
    fb_ref[...] = fgr.astype(BF16)
    dctx_ref[...] = nt(fb_ref[...], wo_ref[...]).astype(BF16)


def k2(me, mixed, ctx, cot, att, ff, offsets, vec, tile=256):
    n = mixed.shape[0]
    blk = pl.BlockSpec((tile, D), lambda i, s: (i, 0))
    o = lambda *w, dt=BF16: jax.ShapeDtypeStruct(w, dt)
    any_spec = pl.BlockSpec(memory_space=pl.ANY)
    return pl.pallas_call(
        partial(k2_body, offsets),
        grid_spec=pltpu.PrefetchScalarGridSpec(
            num_scalar_prefetch=1, grid=(n // tile,),
            in_specs=[blk, pl.BlockSpec((1, tile, D), lambda i, s: (1, i, 0)), blk,
                      pl.BlockSpec((D, D), lambda i, s: (3, 0), pipeline_mode=pl.Buffered(1)), whole(vec.shape)]
            + ([any_spec] * 4 if offsets else [whole(ff[0].shape)]),
            out_specs=[blk, blk, blk, blk, pl.BlockSpec((2, tile, FF), lambda i, s: (0, i, 0)),
                       pl.BlockSpec((2, tile, D), lambda i, s: (0, i, 0)), pl.BlockSpec((16, D), lambda i, s: (0, 0))],
            scratch_shapes=[VMEM((tile, FF), F32), VMEM((tile, D), F32)]
            + ([VMEM((2 * FF, D), BF16), pltpu.SemaphoreType.DMA] if offsets else []),
        ),
        out_shape=[o(n, D), o(n, D, dt=F32), o(n, D), o(n, D), o(2, n, FF), o(2, n, D), o(16, D, dt=F32)],
        cost_estimate=cost(60, 80),
        name="feed_forward",
    )(me, mixed, ctx, cot, att, vec, *ff)

def dw_body(rows, side_ref, lhs_ref, rhs_ref, out_ref):
    step = 128 if rows % 256 else 256

    def chunk(c, carry):
        at = pl.ds(pl.multiple_of(c * step, step), step)
        out_ref[0, at, :] = tn(lhs_ref[0, :, at], rhs_ref[0]).astype(BF16)
        return carry
    lax.fori_loop(0, rows // step, chunk, 0)


def dw(side, lhs, rhs, rows, count):
    n, span = lhs.shape[1:]
    per = span // rows
    repeats = rhs.shape[0] // lhs.shape[0]
    tall = lambda i, s: (2 * i + s[0]) // per
    left = (lambda t: t // 3) if repeats == 2 else (lambda t: t)
    return pl.pallas_call(
        partial(dw_body, rows),
        grid_spec=pltpu.PrefetchScalarGridSpec(
            num_scalar_prefetch=1, grid=(count,),
            in_specs=[pl.BlockSpec((1, n, rows), lambda i, s: (left(tall(i, s)), 0, (2 * i + s[0]) % per)),
                      pl.BlockSpec((1, n, D), lambda i, s: (tall(i, s), 0, 0))],
            out_specs=pl.BlockSpec((1, rows, D), lambda i, s: (i, 0, 0)),
        ),
        out_shape=jax.ShapeDtypeStruct((count, rows, D), BF16),
        cost_estimate=cost(2e-9 * n * rows * D * count, 10),
        name="weight_grad",
    )(side, lhs, rhs)

def k3_body(first_seq, kept, q_ref, k_ref, v_ref, ctx_ref, dctx_ref, fb_ref, lse_ref, seg_ref, *rest):
    d_ref, vg_ref, bias_scr, lse_scr, del_scr = rest[kept:]
    ctx_ref = ctx_ref.at[0]
    dq_ref, dk_ref, dv_ref = d_ref.at[0], d_ref.at[1], d_ref.at[2]
    d_ref[3] = fb_ref[...]
    i = pl.program_id(0) + first_seq

    @pl.when(pl.program_id(0) == 0)
    def _():
        vg_ref[...] = jnp.zeros_like(vg_ref)
    seg = seg_ref[pl.ds(i, 1), :]
    length = seg.shape[1]
    bias_scr[...] = jnp.where(column_of(seg) == seg, 0.0, AWAY)
    lse_scr[...] = jnp.transpose(lse_ref[...])[:16, :]
    prod = dctx_ref[...].astype(F32) * ctx_ref[...].astype(F32)
    pick = (lax.broadcasted_iota(jnp.int32, (16, D), 1) // HEAD_DIM == lax.broadcasted_iota(jnp.int32, (16, D), 0)).astype(F32)
    del_scr[...] = lax.dot_general(pick, prod, (((1,), (1,)), ((), ())), precision=lax.Precision.HIGHEST, preferred_element_type=F32)
    low = lax.broadcasted_iota(jnp.int32, (length, 128), 1) < HEAD_DIM

    def pair(p, carry):
        at = pl.ds(pl.multiple_of(p * 128, 128), 128)
        qp, kp, vp, op = q_ref[:, at], k_ref[:, at], v_ref[:, at], dctx_ref[:, at]
        zero = jnp.zeros_like(qp)
        got = []
        for half in range(2):
            mine = low if half == 0 else jnp.logical_not(low)
            st = nt(jnp.where(mine, kp, zero), qp) + bias_scr[...]
            pt = jnp.exp(st - lse_scr[pl.ds(2 * p + half, 1), :])
            dv = nn(pt.astype(BF16), op)
            dpt = nt(jnp.where(mine, vp, zero), op)
            dst = (pt * (dpt - del_scr[pl.ds(2 * p + half, 1), :])).astype(BF16)
            dk = nn(dst, qp)
            dq = tn(dst, kp)
            got.append((dq, dk, dv))
        dq, dk, dv = (jnp.where(low, a, b) for a, b in zip(*got))
        dqb = dq.astype(BF16) * jnp.bfloat16(0.125)
        dvb = dv.astype(BF16)
        dq_ref[:, at] = dqb
        dk_ref[:, at] = dk.astype(BF16)
        dv_ref[:, at] = dvb
        vg_ref[0:1, at] += colsum(dqb.astype(F32))
        vg_ref[1:2, at] += colsum(dvb.astype(F32))
        return carry
    lax.fori_loop(0, HEADS // 2, pair, 0)


def k3(first_seq, count, q, k, v, ctx, dctx, fb, lse, seg, kept):
    seqs, length = seg.shape
    n = seqs * length
    blk = pl.BlockSpec((length, D), lambda i: (i + first_seq, 0))
    return pl.pallas_call(
        partial(k3_body, first_seq, len(kept)), grid=(count,),
        in_specs=[blk] * 3 + [pl.BlockSpec((1, length, D), lambda i: (1, i + first_seq, 0)), blk, blk,
                              pl.BlockSpec((length, 128), lambda i: (i + first_seq, 0)), whole((seqs, length))]
        + [pl.BlockSpec(memory_space=pl.ANY)] * len(kept),
        out_specs=[pl.BlockSpec((4, length, D), lambda i: (0, i + first_seq, 0)), pl.BlockSpec((8, D), lambda i: (0, 0))],
        out_shape=[jax.ShapeDtypeStruct((4, n, D), BF16), jax.ShapeDtypeStruct((8, D), F32)],
        scratch_shapes=[VMEM((length, length), F32), VMEM((16, length), F32), VMEM((16, length), F32)],
        input_output_aliases={8 + j: j for j in range(len(kept))},
        cost_estimate=cost(count * 12, count * 6),
        name="attend_back",
    )(q, k, v, ctx, dctx, fb, lse, seg, *kept)

def k4_body(first_seq, kept, first_ref, d_ref, tok_ref, seg_ref, feat_ref, w_ref, vec_ref, *rest):
    tg_ref, vg_ref = rest[kept:]
    i = pl.program_id(0) + first_seq
    dq_ref, dk_ref, dv_ref = d_ref.at[0], d_ref.at[1], d_ref.at[2]

    @pl.when(pl.program_id(0) == 0)
    def _():
        vg_ref[...] = jnp.zeros_like(vg_ref)
    group = group_of(seg_ref[pl.ds(i, 1), :], feat_ref[pl.ds(i, 1), :])
    gf = group.astype(F32)
    members = jnp.sum(gf, axis=1, keepdims=True)
    gb = gf.astype(BF16)
    tok = tok_ref[...]
    merging = nn(gb, tok) / members
    mg = (first_ref[...] + nt(dq_ref[...], w_ref[0:D, :]) + nt(dk_ref[...], w_ref[D:2 * D, :])
          + nt(dv_ref[...], w_ref[2 * D:3 * D, :]))
    vg_ref[0:1, :] += colsum(mg * merging)
    spread = (vec_ref[0:1, :] * mg / members).astype(BF16)
    tg_ref[...] = (mg + nn(gb, spread)).astype(BF16)


def k4(first_seq, count, first, d, tokens, seg, feat, att, vec, kept):
    seqs, length = seg.shape
    n = seqs * length
    blk = pl.BlockSpec((length, D), lambda i: (i + first_seq, 0))
    return pl.pallas_call(
        partial(k4_body, first_seq, len(kept)), grid=(count,),
        in_specs=[blk, pl.BlockSpec((3, length, D), lambda i: (0, i + first_seq, 0)), blk, whole(seg.shape), whole(feat.shape),
                  pl.BlockSpec((3 * D, D), lambda i: (0, 0), pipeline_mode=pl.Buffered(1)), whole(vec.shape)]
        + [pl.BlockSpec(memory_space=pl.ANY)] * len(kept),
        out_specs=[blk, pl.BlockSpec((8, D), lambda i: (0, 0))],
        out_shape=[jax.ShapeDtypeStruct((n, D), BF16), jax.ShapeDtypeStruct((8, D), F32)],
        input_output_aliases={7 + j: j for j in range(len(kept))},
        cost_estimate=cost(count * 3, count * 5),
        name="token_grad",
    )(first, d, tokens, seg, feat, att, vec, *kept)

def adam_step(master, first, second, gradient, rate):
    first_new = BETA * first + (1.0 - BETA) * gradient
    second_new = BETA * second + (1.0 - BETA) * gradient * gradient
    correction = 1.0 - BETA**ADAM_STEP
    master_new = master - rate * (
        first_new / correction / (jnp.sqrt(second_new / correction) + ADAM_EPS) + DECAY * master
    )
    return (master_new, first_new, second_new)


BETA = 0.5
ADAM_STEP = 3
ADAM_EPS = 1e-08
DECAY = 0.01
VECTOR_RATE = 0.1
BOTH = ("wide", "narrow")


def rates(rows, split, first_rate, second_rate):
    index = (lax.axis_index(BOTH) * rows + jnp.arange(rows))[:, None]
    return jnp.where(index < split, first_rate, second_rate)


def tie(*groups):
    return lax.optimization_barrier(groups)


def bit_steps(wide, narrow):
    inner = [1 << b for b in range(narrow.bit_length() - 1)]
    outer = [narrow << b for b in range(1, wide.bit_length() - 1)]
    return inner, outer, narrow


def swap(value, bit, devices):
    return lax.ppermute(value, BOTH, [(i, i ^ bit) for i in range(devices)])


class Gather:
    def __init__(self, shard, wide, narrow):
        self.devices = wide * narrow
        inner, outer, self.core = bit_steps(wide, narrow)
        self.turns = [(bit,) for bit in reversed(inner)] + list(zip(outer, reversed(outer))) + [(self.core, self.core)]
        self.held, self.offsets, self.last = [shard[None]], [[0]], None

    def turn(self):
        bits = self.turns.pop(0)
        if len(bits) == 2 and len(self.held) == 1:
            whole_rows = self.held[0]
            self.held = [whole_rows[:, :, :D // 2], whole_rows[:, :, D // 2:]]
            self.offsets = self.offsets * 2
        self.bits = bits
        self.got = [swap(h, bit, self.devices) for h, bit in zip(self.held, bits)]

    def take(self):
        if not self.turns:
            return (*self.held, *self.got), tuple((a, b, self.core) for a, b in zip(*self.offsets))
        self.held = [jnp.concatenate(pair) for pair in zip(self.held, self.got)]
        self.offsets = [o + [x ^ bit for x in o] for o, bit in zip(self.offsets, self.bits)]


def gather_small(shard, me, wide, narrow):
    devices = wide * narrow
    held = shard[None]
    bit = 1
    while bit < devices:
        held = jnp.concatenate([held, swap(held, bit, devices)])
        bit *= 2
    bit = 1
    while bit < devices:
        split = held.reshape(devices // (2 * bit), 2, bit, *shard.shape)
        held = jnp.where((me & bit) != 0, split[:, ::-1], split).reshape(held.shape)
        bit *= 2
    return held


def part(value, me, bit, axis, mine):
    index = (me & bit) != 0
    index = index.astype(jnp.int32) if mine else 1 - index.astype(jnp.int32)
    return lax.dynamic_index_in_dim(value, index, axis, keepdims=False)


def add(a, b, kind=BF16):
    return (a.astype(F32) + b.astype(F32)).astype(kind)


class Scatter:
    def __init__(self, me, wide, narrow):
        self.me, self.devices, self.narrow = me, wide * narrow, narrow
        self.inner, outer, _ = bit_steps(wide, narrow)
        self.orders = [list(outer), list(outer)[::-1]]
        self.turns = len(outer) + len(self.inner)
        self.done = 0

    def begin(self, mine, got):
        total = add(mine, got)
        width = len(self.orders[0])
        self.values = [h.reshape((2,) * width + h.shape[1:]) for h in (total[:, :, :D // 2], total[:, :, D // 2:])]
        self.split()

    def split(self):
        turn, outer = self.done, len(self.orders[0])
        if turn < outer:
            bits = [o[turn] for o in self.orders]
            axes = [sorted(o[turn:], reverse=True).index(bit) for o, bit in zip(self.orders, bits)]
        else:
            if turn == outer:
                self.values = [jnp.concatenate(self.values, axis=1)]
                self.values = [v.reshape(self.narrow, -1, D) for v in self.values]
            bits, axes = [self.inner[turn - outer]], [1]
            v = self.values[0]
            self.values = [v.reshape(v.shape[0] // 2, 2, *v.shape[1:])]
        self.bits = bits
        self.sends = [part(v, self.me, bit, axis, False) for v, bit, axis in zip(self.values, bits, axes)]
        self.keeps = [part(v, self.me, bit, axis, True) for v, bit, axis in zip(self.values, bits, axes)]

    def turn(self):
        self.got = [swap(s, bit, self.devices) for s, bit in zip(self.sends, self.bits)]

    def take(self):
        self.done += 1
        last = self.done == self.turns
        self.values = [add(a, b, F32 if last else BF16) for a, b in zip(self.keeps, self.got)]
        if last:
            return self.values[0][0]
        self.split()

    def over(self, inputs, work):
        self.sends, inputs = tie(self.sends, inputs)
        self.turn()
        result = work(inputs)
        self.got, result = tie(self.got, result)
        return result, self.take()


def scatter_small(grad, me, wide, narrow):
    devices = wide * narrow
    bit = devices // 2
    while bit:
        both = grad.reshape(2, bit, *grad.shape[1:])
        grad = add(part(both, me, bit, 0, True), swap(part(both, me, bit, 0, False), bit, devices), F32)
        bit //= 2
    return grad[0]


def split_grads(me, lhs, rhs, wide, narrow, owned):
    rows, side = narrow * owned, (me // narrow) % 2
    sides = [(1 - side).reshape(1).astype(jnp.int32), side.reshape(1).astype(jnp.int32)]
    if rows % 128 == 0:
        sent = dw(sides[0], lhs, rhs, rows, wide // 2)
        sent, lhs = tie(sent, lhs)
        got = swap(sent, narrow, wide * narrow)
        mine = dw(sides[1], lhs, rhs, rows, wide // 2)
        return mine, got
    repeats = rhs.shape[0] // lhs.shape[0]
    left = [lhs[0]] * 3 + [lhs[1]] if repeats == 2 else list(lhs)
    grad = jnp.concatenate([tn(a, b) for a, b in zip(left, rhs)], axis=0).astype(BF16)
    grad = grad.reshape(wide // 2, 2, rows, D)
    return part(grad, me, narrow, 1, True), swap(part(grad, me, narrow, 1, False), narrow, wide * narrow)


def spread(seqs, shares):
    runs, at = [], 0
    for j, share in enumerate(shares):
        upto = seqs * sum(shares[:j + 1]) // sum(shares)
        if upto > at:
            runs.append((at, upto - at))
        at = upto
    return runs


def forward_by_permutes(me, wide, narrow, tokens, seg, feat, attention, feedforward, vector):
    seqs = seg.shape[0]
    me1 = me.reshape(1).astype(jnp.int32)
    small = gather_small(vector, me, wide, narrow)
    vec = jnp.pad(jnp.transpose(small, (1, 0, 2)).reshape(small.shape[1], D).astype(F32), ((0, 3), (0, 0)))
    near = Gather(attention, wide, narrow)
    far = Gather(feedforward, wide, narrow)
    ready = narrow.bit_length() - 2
    early = len(far.turns) - 3
    for t in range(len(near.turns)):
        near.turn()
        behind = t > ready and early > 0
        if behind:
            far.turn()
            early -= 1
        near.got, far.held = tie(near.got, far.held)
        if behind:
            near.got, far.got = tie(near.got, far.got)
            far.take()
        weights = near.take()
    att, offsets = weights
    held = ()
    runs = spread(seqs, (1, 2, 1))
    for first_seq, count in runs:
        more = len(far.turns) > 0
        if more:
            far.held, source = tie(far.held, held if held else att)
            far.turn()
        else:
            source = held if held else att
        if held:
            *held, natural = *k1(first_seq, count, me1, tokens, seg, feat, [natural], offsets, vec, source), natural
        else:
            *held, natural = k1(first_seq, count, me1, tokens, seg, feat, source, offsets, vec, ())
        held = tuple(held)
        if more:
            far.got, held = tie(far.got, held)
            ff = far.take()
    while far.turns:
        far.turn()
        ff = far.take()
    ff = ff[0]
    return (*held, vec, natural, ff, offsets)


def local(wide, narrow, tokens, cotangent, segment_ids, feature_ids,
          attention_master, attention_first, attention_second,
          feedforward_master, feedforward_first, feedforward_second,
          vector_master, vector_first, vector_second):
    devices = wide * narrow
    me = lax.axis_index(BOTH)
    me1 = me.reshape(1).astype(jnp.int32)
    seg, feat = segment_ids, feature_ids
    seqs = seg.shape[0]
    shards = [m.astype(BF16) for m in (attention_master, feedforward_master, vector_master)]
    if devices <= 32:
        *held, vec, natural, ff = gathering_k1(wide, narrow, tokens, seg, feat, *shards)
        ff, offsets = [ff], ()
    else:
        *held, vec, natural, ff, offsets = forward_by_permutes(me, wide, narrow, tokens, seg, feat, *shards)
    mixed, q, k, v, ctx, lse = held
    out, first, fb, dctx, broad, slim, vg2 = k2(me1, mixed, ctx, cotangent, natural, ff, offsets, vec)
    ff_sum = Scatter(me, wide, narrow)
    ff_sum.begin(*split_grads(me, broad, slim, wide, narrow, feedforward_master.shape[0]))
    vg3, held, ff_owned = 0.0, (), None
    for first_seq, count in spread(seqs, (2, 1, 1)):
        def attend(given):
            source, kept = given
            return k3(first_seq, count, *source, ctx, dctx, fb, lse, seg, kept)
        (grads, more), ff_owned = ff_sum.over(((q, k, v), held), attend)
        held, vg3 = (grads,), vg3 + more
    d = held[0]
    if ff_owned is None:
        (mine, got), ff_owned = ff_sum.over((ctx, d), lambda g: split_grads(me, *g, wide, narrow, attention_master.shape[0]))
    else:
        mine, got = split_grads(me, ctx, d, wide, narrow, attention_master.shape[0])
    while ff_owned is None:
        _, ff_owned = ff_sum.over((), lambda g: ())
    att_sum = Scatter(me, wide, narrow)
    att_sum.begin(mine, got)
    vg4, held, att_owned = 0.0, (), None
    for first_seq, count in spread(seqs, (2, 1, 1)):
        def back(given):
            source, kept = given
            return k4(first_seq, count, source, d, tokens, seg, feat, natural, vec, kept)
        (grads, more), att_owned = att_sum.over((first, held), back)
        held, vg4 = (grads,), vg4 + more
    token_grads = held[0]
    vec_grad = jnp.concatenate([vg4[0:1], vg3[0:2], vg2[:10]], axis=0)
    vec_owned = scatter_small(jnp.transpose(vec_grad.reshape(vec_grad.shape[0], devices, -1), (1, 0, 2)), me, wide, narrow)
    while att_owned is None:
        att_sum.turn()
        att_owned = att_sum.take()
    ff_rate = rates(feedforward_master.shape[0], FF, D ** (-0.5), FF ** (-0.5))
    att_rate = rates(attention_master.shape[0], 3 * D, D ** (-0.5), (D // 64) ** (-0.5))
    f_new = adam_step(feedforward_master, feedforward_first, feedforward_second, ff_owned, ff_rate)
    a_new = adam_step(attention_master, attention_first, attention_second, att_owned, att_rate)
    v_new = adam_step(vector_master, vector_first, vector_second, vec_owned, VECTOR_RATE)
    result = [out, token_grads]
    for new in (a_new, f_new, v_new):
        result += [*new, new[0].astype(BF16)]
    return tuple(result)


def solution(mesh):
    rows, cols = P(BOTH, None), P(None, BOTH)
    return jax.shard_map(
        partial(local, mesh.shape["wide"], mesh.shape["narrow"]), mesh=mesh,
        in_specs=(rows,) * 10 + (cols,) * 3,
        out_specs=(rows,) * 10 + (cols,) * 4,
        check_vma=False,
    )
```

```python
from functools import partial
import jax, jax.numpy as jnp
from jax import lax
from jax.experimental import pallas as pl
from jax.experimental.pallas import tpu as pltpu
from jax.sharding import PartitionSpec as P

D = 768
FF = 3072
HEADS = 12
HEAD_DIM = 64
NORM_EPS = 1e-05
AWAY = -1e30
F32, BF16 = jnp.float32, jnp.bfloat16
ERFC = (0.11841221385764535, 0.11979147087435008, 0.09737185909338779, 0.13434283549706147,
        -0.0652102059595758, 0.2202795624136942, -0.16009561537425632, 0.035107795064101)
VMEM = pltpu.VMEM


def nn(a, b):
    return lax.dot_general(a, b, (((1,), (0,)), ((), ())), preferred_element_type=F32)

def nt(a, b):
    return lax.dot_general(a, b, (((1,), (1,)), ((), ())), preferred_element_type=F32)

def tn(a, b):
    return lax.dot_general(a, b, (((0,), (0,)), ((), ())), preferred_element_type=F32)

def whole(shape):
    return pl.BlockSpec(shape, lambda *_: (0,) * len(shape), pipeline_mode=pl.Buffered(1))

def gelu_pair(h):
    below = 0.5 + 0.5 * lax.erf(h * 0.7071067811865476)
    bell = jnp.exp(h * h * -0.5)
    return h * below, below + h * (bell * 0.3989422804014327)


def column_of(row):
    return jnp.transpose(jnp.broadcast_to(row, (8, row.shape[1])))[:, :1]

def group_of(seg, feat):
    both = seg * 16 + feat
    return column_of(both) == both

def cost(gigaflops, megabytes):
    return pl.CostEstimate(flops=int(gigaflops * 1e9), bytes_accessed=int(megabytes * 1e6), transcendentals=0)


def fetch_weights(me, offsets, pieces, w_ref, sem):
    rows = pieces[0].shape[1]
    half = D // 2
    copies = []
    for j, offset in enumerate(offsets):
        for side in range(2):
            for col in range(2):
                owner = (me ^ offset[col]) if side == 0 else (me ^ offset[col] ^ offset[2])
                at = pl.ds(pl.multiple_of(owner * rows, 8), rows)
                copies.append(pltpu.make_async_copy(pieces[2 * side + col].at[j], w_ref.at[at, pl.ds(col * half, half)], sem))
    for c in copies:
        c.start()
    for c in copies:
        c.wait()

def attend_forward(i, tok_ref, seg_ref, feat_ref, w_ref, vec_ref, mixed_ref, q_ref, k_ref, v_ref, ctx_ref, lse_ref, bias_scr, service):
    seg = seg_ref[pl.ds(i, 1), :]
    feat = feat_ref[pl.ds(i, 1), :]
    length = seg.shape[1]
    bias_scr[...] = jnp.where(column_of(seg) == seg, 0.0, AWAY)
    group = group_of(seg, feat)
    members = jnp.sum(group.astype(F32), axis=1, keepdims=True)
    tok = tok_ref[...]
    merging = nn(group.astype(F32).astype(BF16), tok) / members
    mixed = tok.astype(F32) + vec_ref[0:1, :] * merging
    mixed_ref[...] = mixed
    mb = mixed.astype(BF16)
    ctx_ref[0] = mb
    q_ref[...] = ((nn(mb, w_ref[0:D, :]) + vec_ref[1:2, :]) * 0.125).astype(BF16)
    k_ref[...] = nn(mb, w_ref[D:2 * D, :]).astype(BF16)
    v_ref[...] = (nn(mb, w_ref[2 * D:3 * D, :]) + vec_ref[2:3, :]).astype(BF16)
    lane = lax.broadcasted_iota(jnp.int32, (length, 128), 1)
    low = lane < HEAD_DIM
    lse_ref[...] = jnp.zeros_like(lse_ref)

    def pair(p, carry):
        at = pl.ds(pl.multiple_of(p * 128, 128), 128)
        qp = q_ref[:, at]
        kp = k_ref[:, at]
        vp = v_ref[:, at]
        outs = []
        zero = jnp.zeros_like(qp)
        for half in range(2):
            mine = low if half == 0 else jnp.logical_not(low)
            s = nt(jnp.where(mine, qp, zero), kp) + bias_scr[...]
            top = jnp.max(s, axis=1, keepdims=True)
            e = jnp.exp(s - top)
            total = jnp.sum(e, axis=1, keepdims=True)
            o = nn(e.astype(BF16), vp) * (1.0 / total)
            outs.append(o)
            lse_ref[...] = jnp.where(lane == 2 * p + half, top + jnp.log(total), lse_ref[...])
        ctx_ref[1, :, at] = jnp.where(low, outs[0], outs[1]).astype(BF16)
        return carry
    service(0)
    lax.fori_loop(0, HEADS // 4, pair, 0)
    service(1)
    lax.fori_loop(HEADS // 4, HEADS // 2, pair, 0)
    service(2)


def k1_body(first_seq, offsets, kept, self_ref, tok_ref, seg_ref, feat_ref, vec_ref, *rest):
    if kept:
        w_ref, rest = rest[0], rest[1 + kept:]
        mixed_ref, q_ref, k_ref, v_ref, ctx_ref, lse_ref, bias_scr = rest
    else:
        pieces, rest = rest[:4], rest[4:]
        mixed_ref, q_ref, k_ref, v_ref, ctx_ref, lse_ref, w_ref, bias_scr, sem = rest
    i = pl.program_id(0) + first_seq

    if not kept:
        @pl.when(pl.program_id(0) == 0)
        def _():
            fetch_weights(self_ref[0], offsets, pieces, w_ref, sem)

    attend_forward(i, tok_ref, seg_ref, feat_ref, w_ref, vec_ref, mixed_ref, q_ref, k_ref, v_ref, ctx_ref, lse_ref, bias_scr, lambda point: None)


def k1(first_seq, count, me, tokens, seg, feat, weights, offsets, vec, kept):
    seqs, length = seg.shape
    blk = pl.BlockSpec((length, D), lambda i, s: (i + first_seq, 0))
    both = pl.BlockSpec((2, length, D), lambda i, s: (0, i + first_seq, 0))
    narrow = pl.BlockSpec((length, 128), lambda i, s: (i + first_seq, 0))
    n = seqs * length
    o = lambda dt: jax.ShapeDtypeStruct((n, D), dt)
    any_spec = pl.BlockSpec(memory_space=pl.ANY)
    out_specs = [blk] * 4 + [both, narrow]
    out_shape = [o(F32), o(BF16), o(BF16), o(BF16), jax.ShapeDtypeStruct((2, n, D), BF16), jax.ShapeDtypeStruct((n, 128), F32)]
    scratch = [VMEM((length, length), F32)]
    if kept:
        weight_specs = [pl.BlockSpec((3 * D, D), lambda i, s: (0, 0), pipeline_mode=pl.Buffered(1))]
    else:
        weight_specs = [any_spec] * 4
        out_specs = out_specs + [whole((4 * D, D))]
        out_shape = out_shape + [jax.ShapeDtypeStruct((4 * D, D), BF16)]
        scratch = scratch + [pltpu.SemaphoreType.DMA]
    return pl.pallas_call(
        partial(k1_body, first_seq, offsets, len(kept)),
        grid_spec=pltpu.PrefetchScalarGridSpec(
            num_scalar_prefetch=1, grid=(count,),
            in_specs=[blk, whole(seg.shape), whole(feat.shape), whole(vec.shape)] + weight_specs + [any_spec] * len(kept),
            out_specs=out_specs, scratch_shapes=scratch,
        ),
        out_shape=out_shape,
        input_output_aliases={6 + j: j for j in range(len(kept))},
        cost_estimate=cost(count * 11, count * 4),
        name="mix_attend",
    )(me, tokens, seg, feat, vec, *weights, *kept)

MESH = pl.DeviceIdType.MESH


def flips(x, mask):
    bit = 1
    while bit <= mask:
        if mask & bit:
            x = x + bit - 2 * bit * ((x // bit) % 2)
        bit *= 2
    return x


class Spreading:
    def __init__(self, wide, narrow, shard, full, columns, sems):
        self.narrow, self.masks = narrow, wide // 2
        self.bits = [1 << b for b in range((wide // 2).bit_length() - 1)]
        w, self.z = lax.axis_index("wide"), lax.axis_index("narrow")
        self.o, self.c = w // 2, w % 2
        self.shard, self.full, self.columns = shard, full, columns
        self.line_out, self.line_in, self.tree_out, self.tree_in, self.core_out, self.core_in, self.own = sems

    def at(self, r, k, c=None, h=None):
        c = self.c if c is None else c
        rows = self.shard.shape[0]
        owner = (2 * flips(self.o, r) + c) * self.narrow + flips(self.z, k)
        where = pl.ds(pl.multiple_of(owner * rows, 8), rows)
        if h is None:
            return self.full.at[where, :]
        return self.full.at[where, pl.ds(*self.columns[h][:2])]

    def source(self, r, k, h=None):
        if r or k:
            return self.at(r, k, None, h)
        return self.shard if h is None else self.shard.at[:, pl.ds(*self.columns[h][:2])]

    def keep(self):
        return pltpu.make_async_copy(self.shard, self.at(0, 0), self.own)

    def line(self, k, arriving=False):
        return pltpu.make_async_remote_copy(
            self.shard, self.at(0, k if arriving else 0), self.line_out.at[k - 1], self.line_in.at[k - 1],
            device_id=(2 * self.o + self.c, flips(self.z, k)), device_id_type=MESH)

    def tree(self, r, k, h, bit, arriving=False):
        there = r if arriving else r ^ bit
        n = (k * len(self.columns) + h) * self.masks + there
        part = self.at(r, k, None, h)
        return pltpu.make_async_remote_copy(
            part if arriving else self.source(r, k, h), part, self.tree_out.at[n], self.tree_in.at[n],
            device_id=(2 * flips(self.o, bit) + self.c, self.z), device_id_type=MESH)

    def core(self, r, k, arriving=False):
        n = k * self.masks + r
        part = self.at(r, k, 1 - self.c if arriving else None)
        return pltpu.make_async_remote_copy(
            part if arriving else self.source(r, k), part, self.core_out.at[n], self.core_in.at[n],
            device_id=(2 * self.o + 1 - self.c, self.z), device_id_type=MESH)

    def onward(self, r, h):
        if self.columns[h][2]:
            return [b for b in reversed(self.bits) if r == 0 or b < (r & -r)]
        return [b for b in self.bits if b > r]

    def last_bit(self, r, h):
        if self.columns[h][2]:
            return r & -r
        return 1 << (r.bit_length() - 1)

    def open(self):
        self.keep().start()
        for k in range(1, self.narrow):
            self.line(k).start()

    def send_on(self, r, k, h):
        for bit in self.onward(r, h):
            self.tree(r, k, h, bit).start()

    def roots(self, k):
        if k:
            self.line(k, True).wait_recv()
        for h in range(len(self.columns)):
            self.send_on(0, k, h)
        self.core(0, k).start()

    def relay(self, r, k):
        for h in range(len(self.columns)):
            self.tree(r, k, h, self.last_bit(r, h), True).wait_recv()
            self.send_on(r, k, h)
        self.core(r, k).start()

    def close(self):
        for k in range(self.narrow):
            for r in range(self.masks):
                self.core(r, k, True).wait_recv()
        self.keep().wait()

    def drain(self):
        for k in range(self.narrow):
            if k:
                self.line(k).wait_send()
            for r in range(self.masks):
                for h in range(len(self.columns)):
                    for bit in self.onward(r, h):
                        self.tree(r, k, h, bit).wait_send()
                self.core(r, k).wait_send()


def spreading_sems(wide, narrow, halves):
    dma = pltpu.SemaphoreType.DMA
    tree, core = narrow * halves * (wide // 2), narrow * (wide // 2)
    return [dma((narrow - 1,)), dma((narrow - 1,)), dma((tree,)), dma((tree,)), dma((core,)), dma((core,)), dma]


def greet(wide, narrow):
    barrier = pltpu.get_barrier_semaphore()
    w, z = lax.axis_index("wide"), lax.axis_index("narrow")
    o, c = w // 2, w % 2
    peers = [(w, flips(z, k)) for k in range(1, narrow)] + [(2 * o + 1 - c, z)]
    bit = 1
    while bit < wide // 2:
        peers.append((2 * flips(o, bit) + c, z))
        bit *= 2
    for peer in peers:
        pl.semaphore_signal(barrier, inc=1, device_id=peer, device_id_type=MESH)
    pl.semaphore_wait(barrier, len(peers))


def gathering_k1_body(wide, narrow, cols, steps, tok_ref, seg_ref, feat_ref, att_ref, ff_ref, vs_ref,
                      mixed_ref, q_ref, k_ref, v_ref, ctx_ref, lse_ref, vec_ref, wout_ref, fout_ref,
                      bias_scr, w_ref, vs_scr, put_sem, *sems):
    i = pl.program_id(0)
    half = D // 2
    count = len(sems) // 3
    pairs = [(0, half, False), (half, half, True)]
    att = Spreading(wide, narrow, att_ref, w_ref, pairs, sems[:count])
    ff = Spreading(wide, narrow, ff_ref, fout_ref, pairs, sems[count:2 * count])
    vs = Spreading(wide, narrow, vs_ref, vs_scr, [(0, 128, False)], sems[2 * count:])
    singles = [r for r in range(1, wide // 2)]
    save = pltpu.make_async_copy(w_ref, wout_ref, put_sem)

    @pl.when(i == 0)
    def _():
        greet(wide, narrow)
        for one in (vs, att, ff):
            one.open()
        for k in range(narrow):
            vs.roots(k)
            att.roots(k)
        ff.roots(0)
        for r in singles:
            for k in range(narrow):
                vs.relay(r, k)
                att.relay(r, k)
        vs.close()
        vec = jnp.zeros((16, D), F32)
        row = lax.broadcasted_iota(jnp.int32, (128, D), 0)
        col = lax.broadcasted_iota(jnp.int32, (128, D), 1)
        for d in range(wide * narrow):
            pick = jnp.logical_and(row < cols, col == row + cols * d).astype(F32).astype(BF16)
            vec = vec + nn(vs_scr[16 * d:16 * d + 16, :], pick)
        vec_ref[...] = vec
        att.close()
        save.start()

    plan = [lambda k=k: ff.roots(k) for k in range(1, narrow)]
    for r in singles:
        plan += [lambda r=r, k=k: ff.relay(r, k) for k in range(narrow)]

    def service(point):
        for s in range(steps):
            todo = slots.get((s, point), ())
            if todo:
                @pl.when(i == s)
                def _(todo=todo):
                    for act in todo:
                        act()
    total = steps * 3 - 1
    slots = {}
    for n, act in enumerate(plan):
        spot = n * total // len(plan)
        slots.setdefault((spot // 3, spot % 3), []).append(act)

    attend_forward(i, tok_ref, seg_ref, feat_ref, w_ref, vec_ref, mixed_ref, q_ref, k_ref, v_ref, ctx_ref, lse_ref, bias_scr, service)

    @pl.when(i == steps - 1)
    def _():
        ff.close()
        for one in (vs, att, ff):
            one.drain()
        save.wait()


def gathering_k1(wide, narrow, tokens, seg, feat, att_shard, ff_shard, vec_shard):
    seqs, length = seg.shape
    n, devices = seqs * length, wide * narrow
    vs = jnp.pad(vec_shard, ((0, 16 - vec_shard.shape[0]), (0, 128 - vec_shard.shape[1])))
    blk = pl.BlockSpec((length, D), lambda i: (i, 0))
    any_spec = pl.BlockSpec(memory_space=pl.ANY)
    o = lambda dt: jax.ShapeDtypeStruct((n, D), dt)
    sems = spreading_sems(wide, narrow, 2) * 2 + spreading_sems(wide, narrow, 1)
    return pl.pallas_call(
        partial(gathering_k1_body, wide, narrow, vec_shard.shape[1], seqs), grid=(seqs,),
        in_specs=[blk, whole(seg.shape), whole(feat.shape), any_spec, any_spec, any_spec],
        out_specs=[blk] * 4 + [pl.BlockSpec((2, length, D), lambda i: (0, i, 0)), pl.BlockSpec((length, 128), lambda i: (i, 0)),
                               whole((16, D)), any_spec, any_spec],
        out_shape=[o(F32), o(BF16), o(BF16), o(BF16), jax.ShapeDtypeStruct((2, n, D), BF16), jax.ShapeDtypeStruct((n, 128), F32),
                   jax.ShapeDtypeStruct((16, D), F32), jax.ShapeDtypeStruct((4 * D, D), BF16), jax.ShapeDtypeStruct((2 * FF, D), BF16)],
        scratch_shapes=[VMEM((length, length), F32), VMEM((4 * D, D), BF16), VMEM((16 * devices, 128), BF16), pltpu.SemaphoreType.DMA, *sems],
        compiler_params=pltpu.CompilerParams(collective_id=0, has_side_effects=True),
        cost_estimate=cost(60, 60),
        name="gather_attend",
    )(tokens, seg, feat, att_shard, ff_shard, vs)

def norm_parts(z):
    mean = jnp.mean(z, axis=1, keepdims=True)
    c = z - mean
    var = jnp.mean(c * c, axis=1, keepdims=True)
    inv = lax.rsqrt(var + NORM_EPS)
    return c * inv, inv

def norm_pull(g, xhat, inv):
    a = jnp.mean(g, axis=1, keepdims=True)
    b = jnp.mean(g * xhat, axis=1, keepdims=True)
    return (g - a - xhat * b) * inv

def colsum(x):
    return jnp.sum(x, axis=0, keepdims=True)

def k2_body(offsets, self_ref, mixed_ref, ctx_ref, cot_ref, wo_ref, vec_ref, *rest):
    if offsets:
        pieces, rest = rest[:4], rest[4:]
        out_ref, first_ref, fb_ref, dctx_ref, wide_ref, slim_ref, vg_ref, gp_scr, sum_scr, wf_ref, sem = rest
    else:
        wf_ref, out_ref, first_ref, fb_ref, dctx_ref, wide_ref, slim_ref, vg_ref, gp_scr, sum_scr = rest
    ctx_ref = ctx_ref.at[0]
    hg_ref, act_ref = wide_ref.at[0], wide_ref.at[1]
    nb_ref, bg_ref = slim_ref.at[0], slim_ref.at[1]
    @pl.when(pl.program_id(0) == 0)
    def _():
        vg_ref[...] = jnp.zeros_like(vg_ref)
        if offsets:
            fetch_weights(self_ref[0], offsets, pieces, wf_ref, sem)

    ex = FF // D
    first_sum = mixed_ref[...] + nn(ctx_ref[...], wo_ref[...]) + vec_ref[3:4, :]
    xhat1, inv1 = norm_parts(first_sum)
    normed = xhat1 * vec_ref[4:5, :] + vec_ref[5:6, :]
    nb_ref[...] = normed.astype(BF16)
    sum_scr[...] = normed + vec_ref[6 + ex:7 + ex, :]
    for c in range(ex):
        at = pl.ds(c * D, D)
        h = nt(nb_ref[...], wf_ref[at, :]) + vec_ref[6 + c:7 + c, :]
        act, slope = gelu_pair(h)
        act_ref[:, at] = act.astype(BF16)
        gp_scr[:, at] = slope.astype(gp_scr.dtype)
        sum_scr[...] += nn(act_ref[:, at], wf_ref[pl.ds(FF + c * D, D), :])
    xhat2, inv2 = norm_parts(sum_scr[...])
    out_ref[...] = (xhat2 * vec_ref[7 + ex:8 + ex, :] + vec_ref[8 + ex:9 + ex, :]).astype(BF16)
    cot = cot_ref[...].astype(F32)
    vg_ref[4 + ex:5 + ex, :] += colsum(cot * xhat2)
    vg_ref[5 + ex:6 + ex, :] += colsum(cot)
    gs = norm_pull(cot * vec_ref[7 + ex:8 + ex, :], xhat2, inv2)
    vg_ref[3 + ex:4 + ex, :] += colsum(gs)
    bg_ref[...] = gs.astype(BF16)
    sum_scr[...] = gs
    for c in range(ex):
        at = pl.ds(c * D, D)
        hg = nt(bg_ref[...], wf_ref[pl.ds(FF + c * D, D), :]) * gp_scr[:, at].astype(F32)
        vg_ref[3 + c:4 + c, :] += colsum(hg)
        hg_ref[:, at] = hg.astype(BF16)
        sum_scr[...] += nn(hg_ref[:, at], wf_ref[at, :])
    ng = sum_scr[...]
    vg_ref[1:2, :] += colsum(ng * xhat1)
    vg_ref[2:3, :] += colsum(ng)
    fgr = norm_pull(ng * vec_ref[4:5, :], xhat1, inv1)
    vg_ref[0:1, :] += colsum(fgr)
    first_ref[...] = fgr
    fb_ref[...] = fgr.astype(BF16)
    dctx_ref[...] = nt(fb_ref[...], wo_ref[...]).astype(BF16)


def k2(me, mixed, ctx, cot, att, ff, offsets, vec, tile=256):
    n = mixed.shape[0]
    blk = pl.BlockSpec((tile, D), lambda i, s: (i, 0))
    o = lambda *w, dt=BF16: jax.ShapeDtypeStruct(w, dt)
    any_spec = pl.BlockSpec(memory_space=pl.ANY)
    return pl.pallas_call(
        partial(k2_body, offsets),
        grid_spec=pltpu.PrefetchScalarGridSpec(
            num_scalar_prefetch=1, grid=(n // tile,),
            in_specs=[blk, pl.BlockSpec((1, tile, D), lambda i, s: (1, i, 0)), blk,
                      pl.BlockSpec((D, D), lambda i, s: (3, 0), pipeline_mode=pl.Buffered(1)), whole(vec.shape)]
            + ([any_spec] * 4 if offsets else [whole(ff[0].shape)]),
            out_specs=[blk, blk, blk, blk, pl.BlockSpec((2, tile, FF), lambda i, s: (0, i, 0)),
                       pl.BlockSpec((2, tile, D), lambda i, s: (0, i, 0)), pl.BlockSpec((16, D), lambda i, s: (0, 0))],
            scratch_shapes=[VMEM((tile, FF), F32), VMEM((tile, D), F32)]
            + ([VMEM((2 * FF, D), BF16), pltpu.SemaphoreType.DMA] if offsets else []),
        ),
        out_shape=[o(n, D), o(n, D, dt=F32), o(n, D), o(n, D), o(2, n, FF), o(2, n, D), o(16, D, dt=F32)],
        cost_estimate=cost(60, 80),
        name="feed_forward",
    )(me, mixed, ctx, cot, att, vec, *ff)

def dw_body(rows, side_ref, lhs_ref, rhs_ref, out_ref):
    step = 384 if rows % 384 == 0 else 128
    for at in range(0, rows, step):
        out_ref[0, at:at + step, :] = tn(lhs_ref[0, :, at:at + step], rhs_ref[0]).astype(BF16)


def dw(side, lhs, rhs, rows, count):
    n, span = lhs.shape[1:]
    per = span // rows
    repeats = rhs.shape[0] // lhs.shape[0]
    tall = lambda i, s: (2 * i + s[0]) // per
    left = (lambda t: t // 3) if repeats == 2 else (lambda t: t)
    return pl.pallas_call(
        partial(dw_body, rows),
        grid_spec=pltpu.PrefetchScalarGridSpec(
            num_scalar_prefetch=1, grid=(count,),
            in_specs=[pl.BlockSpec((1, n, rows), lambda i, s: (left(tall(i, s)), 0, (2 * i + s[0]) % per)),
                      pl.BlockSpec((1, n, D), lambda i, s: (tall(i, s), 0, 0))],
            out_specs=pl.BlockSpec((1, rows, D), lambda i, s: (i, 0, 0)),
        ),
        out_shape=jax.ShapeDtypeStruct((count, rows, D), BF16),
        cost_estimate=cost(2e-9 * n * rows * D * count, 10),
        name="weight_grad",
    )(side, lhs, rhs)

def k3_body(first_seq, kept, q_ref, k_ref, v_ref, ctx_ref, dctx_ref, fb_ref, lse_ref, seg_ref, *rest):
    d_ref, vg_ref, bias_scr, lse_scr, del_scr = rest[kept:]
    ctx_ref = ctx_ref.at[0]
    dq_ref, dk_ref, dv_ref = d_ref.at[0], d_ref.at[1], d_ref.at[2]
    d_ref[3] = fb_ref[...]
    i = pl.program_id(0) + first_seq

    @pl.when(pl.program_id(0) == 0)
    def _():
        vg_ref[...] = jnp.zeros_like(vg_ref)
    seg = seg_ref[pl.ds(i, 1), :]
    length = seg.shape[1]
    bias_scr[...] = jnp.where(column_of(seg) == seg, 0.0, AWAY)
    lse_scr[...] = jnp.transpose(lse_ref[...])[:16, :]
    prod = dctx_ref[...].astype(F32) * ctx_ref[...].astype(F32)
    pick = (lax.broadcasted_iota(jnp.int32, (16, D), 1) // HEAD_DIM == lax.broadcasted_iota(jnp.int32, (16, D), 0)).astype(F32).astype(BF16)
    high = prod.astype(BF16)
    del_scr[...] = nt(pick, high) + nt(pick, (prod - high.astype(F32)).astype(BF16))
    low = lax.broadcasted_iota(jnp.int32, (length, 128), 1) < HEAD_DIM

    def pair(p, carry):
        at = pl.ds(pl.multiple_of(p * 128, 128), 128)
        qp, kp, vp, op = q_ref[:, at], k_ref[:, at], v_ref[:, at], dctx_ref[:, at]
        zero = jnp.zeros_like(qp)
        got = []
        for half in range(2):
            mine = low if half == 0 else jnp.logical_not(low)
            st = nt(jnp.where(mine, kp, zero), qp) + bias_scr[...]
            pt = jnp.exp(st - lse_scr[pl.ds(2 * p + half, 1), :])
            dv = nn(pt.astype(BF16), op)
            dpt = nt(jnp.where(mine, vp, zero), op)
            dst = (pt * (dpt - del_scr[pl.ds(2 * p + half, 1), :])).astype(BF16)
            dk = nn(dst, qp)
            dq = tn(dst, kp)
            got.append((dq, dk, dv))
        dq, dk, dv = (jnp.where(low, a, b) for a, b in zip(*got))
        dqb = dq.astype(BF16) * jnp.bfloat16(0.125)
        dvb = dv.astype(BF16)
        dq_ref[:, at] = dqb
        dk_ref[:, at] = dk.astype(BF16)
        dv_ref[:, at] = dvb
        vg_ref[0:1, at] += colsum(dqb.astype(F32))
        vg_ref[1:2, at] += colsum(dvb.astype(F32))
        return carry
    lax.fori_loop(0, HEADS // 2, pair, 0)


def k3(first_seq, count, q, k, v, ctx, dctx, fb, lse, seg, kept):
    seqs, length = seg.shape
    n = seqs * length
    blk = pl.BlockSpec((length, D), lambda i: (i + first_seq, 0))
    return pl.pallas_call(
        partial(k3_body, first_seq, len(kept)), grid=(count,),
        in_specs=[blk] * 3 + [pl.BlockSpec((1, length, D), lambda i: (1, i + first_seq, 0)), blk, blk,
                              pl.BlockSpec((length, 128), lambda i: (i + first_seq, 0)), whole((seqs, length))]
        + [pl.BlockSpec(memory_space=pl.ANY)] * len(kept),
        out_specs=[pl.BlockSpec((4, length, D), lambda i: (0, i + first_seq, 0)), pl.BlockSpec((8, D), lambda i: (0, 0))],
        out_shape=[jax.ShapeDtypeStruct((4, n, D), BF16), jax.ShapeDtypeStruct((8, D), F32)],
        scratch_shapes=[VMEM((length, length), F32), VMEM((16, length), F32), VMEM((16, length), F32)],
        input_output_aliases={8 + j: j for j in range(len(kept))},
        cost_estimate=cost(count * 12, count * 6),
        name="attend_back",
    )(q, k, v, ctx, dctx, fb, lse, seg, *kept)

def k4_body(first_seq, kept, first_ref, d_ref, tok_ref, seg_ref, feat_ref, w_ref, vec_ref, *rest):
    tg_ref, vg_ref = rest[kept:]
    i = pl.program_id(0) + first_seq
    dq_ref, dk_ref, dv_ref = d_ref.at[0], d_ref.at[1], d_ref.at[2]

    @pl.when(pl.program_id(0) == 0)
    def _():
        vg_ref[...] = jnp.zeros_like(vg_ref)
    group = group_of(seg_ref[pl.ds(i, 1), :], feat_ref[pl.ds(i, 1), :])
    gf = group.astype(F32)
    members = jnp.sum(gf, axis=1, keepdims=True)
    gb = gf.astype(BF16)
    tok = tok_ref[...]
    merging = nn(gb, tok) / members
    mg = (first_ref[...] + nt(dq_ref[...], w_ref[0:D, :]) + nt(dk_ref[...], w_ref[D:2 * D, :])
          + nt(dv_ref[...], w_ref[2 * D:3 * D, :]))
    vg_ref[0:1, :] += colsum(mg * merging)
    spread = (vec_ref[0:1, :] * mg / members).astype(BF16)
    tg_ref[...] = (mg + nn(gb, spread)).astype(BF16)


def k4(first_seq, count, first, d, tokens, seg, feat, att, vec, kept):
    seqs, length = seg.shape
    n = seqs * length
    blk = pl.BlockSpec((length, D), lambda i: (i + first_seq, 0))
    return pl.pallas_call(
        partial(k4_body, first_seq, len(kept)), grid=(count,),
        in_specs=[blk, pl.BlockSpec((3, length, D), lambda i: (0, i + first_seq, 0)), blk, whole(seg.shape), whole(feat.shape),
                  pl.BlockSpec((3 * D, D), lambda i: (0, 0), pipeline_mode=pl.Buffered(1)), whole(vec.shape)]
        + [pl.BlockSpec(memory_space=pl.ANY)] * len(kept),
        out_specs=[blk, pl.BlockSpec((8, D), lambda i: (0, 0))],
        out_shape=[jax.ShapeDtypeStruct((n, D), BF16), jax.ShapeDtypeStruct((8, D), F32)],
        input_output_aliases={7 + j: j for j in range(len(kept))},
        cost_estimate=cost(count * 3, count * 5),
        name="token_grad",
    )(first, d, tokens, seg, feat, att, vec, *kept)

def adam_step(master, first, second, gradient, rate):
    first_new = BETA * first + (1.0 - BETA) * gradient
    second_new = BETA * second + (1.0 - BETA) * gradient * gradient
    correction = 1.0 - BETA**ADAM_STEP
    master_new = master - rate * (
        first_new / correction / (jnp.sqrt(second_new / correction) + ADAM_EPS) + DECAY * master
    )
    return (master_new, first_new, second_new)


BETA = 0.5
ADAM_STEP = 3
ADAM_EPS = 1e-08
DECAY = 0.01
VECTOR_RATE = 0.1
BOTH = ("wide", "narrow")


def rates(rows, split, first_rate, second_rate):
    index = (lax.axis_index(BOTH) * rows + jnp.arange(rows))[:, None]
    return jnp.where(index < split, first_rate, second_rate)


def tie(*groups):
    return lax.optimization_barrier(groups)


def bit_steps(wide, narrow):
    inner = [1 << b for b in range(narrow.bit_length() - 1)]
    outer = [narrow << b for b in range(1, wide.bit_length() - 1)]
    return inner, outer, narrow


def swap(value, bit, devices):
    return lax.ppermute(value, BOTH, [(i, i ^ bit) for i in range(devices)])


class Gather:
    def __init__(self, shard, wide, narrow):
        self.devices = wide * narrow
        inner, outer, self.core = bit_steps(wide, narrow)
        self.turns = [(bit,) for bit in reversed(inner)] + list(zip(outer, reversed(outer))) + [(self.core, self.core)]
        self.held, self.offsets, self.last = [shard[None]], [[0]], None

    def turn(self):
        bits = self.turns.pop(0)
        if len(bits) == 2 and len(self.held) == 1:
            whole_rows = self.held[0]
            self.held = [whole_rows[:, :, :D // 2], whole_rows[:, :, D // 2:]]
            self.offsets = self.offsets * 2
        self.bits = bits
        self.got = [swap(h, bit, self.devices) for h, bit in zip(self.held, bits)]

    def take(self):
        if not self.turns:
            return (*self.held, *self.got), tuple((a, b, self.core) for a, b in zip(*self.offsets))
        self.held = [jnp.concatenate(pair) for pair in zip(self.held, self.got)]
        self.offsets = [o + [x ^ bit for x in o] for o, bit in zip(self.offsets, self.bits)]


def gather_small(shard, me, wide, narrow):
    devices = wide * narrow
    held = shard[None]
    bit = 1
    while bit < devices:
        held = jnp.concatenate([held, swap(held, bit, devices)])
        bit *= 2
    bit = 1
    while bit < devices:
        split = held.reshape(devices // (2 * bit), 2, bit, *shard.shape)
        held = jnp.where((me & bit) != 0, split[:, ::-1], split).reshape(held.shape)
        bit *= 2
    return held


def part(value, me, bit, axis, mine):
    index = (me & bit) != 0
    index = index.astype(jnp.int32) if mine else 1 - index.astype(jnp.int32)
    return lax.dynamic_index_in_dim(value, index, axis, keepdims=False)


def add(a, b, kind=BF16):
    return (a.astype(F32) + b.astype(F32)).astype(kind)


class Scatter:
    def __init__(self, me, wide, narrow):
        self.me, self.devices, self.narrow = me, wide * narrow, narrow
        self.inner, outer, _ = bit_steps(wide, narrow)
        self.orders = [list(outer), list(outer)[::-1]]
        self.turns = len(outer) + len(self.inner)
        self.done = 0

    def begin(self, mine, got):
        total = add(mine, got)
        width = len(self.orders[0])
        self.values = [h.reshape((2,) * width + h.shape[1:]) for h in (total[:, :, :D // 2], total[:, :, D // 2:])]
        self.split()

    def split(self):
        turn, outer = self.done, len(self.orders[0])
        if turn < outer:
            bits = [o[turn] for o in self.orders]
            axes = [sorted(o[turn:], reverse=True).index(bit) for o, bit in zip(self.orders, bits)]
        else:
            if turn == outer:
                self.values = [jnp.concatenate(self.values, axis=1)]
                self.values = [v.reshape(self.narrow, -1, D) for v in self.values]
            bits, axes = [self.inner[turn - outer]], [1]
            v = self.values[0]
            self.values = [v.reshape(v.shape[0] // 2, 2, *v.shape[1:])]
        self.bits = bits
        self.sends = [part(v, self.me, bit, axis, False) for v, bit, axis in zip(self.values, bits, axes)]
        self.keeps = [part(v, self.me, bit, axis, True) for v, bit, axis in zip(self.values, bits, axes)]

    def turn(self):
        self.got = [swap(s, bit, self.devices) for s, bit in zip(self.sends, self.bits)]

    def take(self):
        self.done += 1
        last = self.done == self.turns
        self.values = [add(a, b, F32 if last else BF16) for a, b in zip(self.keeps, self.got)]
        if last:
            return self.values[0][0]
        self.split()

    def over(self, inputs, work):
        self.sends, inputs = tie(self.sends, inputs)
        self.turn()
        result = work(inputs)
        self.got, result = tie(self.got, result)
        return result, self.take()


def scatter_small(grad, me, wide, narrow):
    devices = wide * narrow
    bit = devices // 2
    while bit:
        both = grad.reshape(2, bit, *grad.shape[1:])
        grad = add(part(both, me, bit, 0, True), swap(part(both, me, bit, 0, False), bit, devices), F32)
        bit //= 2
    return grad[0]


def split_grads(me, lhs, rhs, wide, narrow, owned):
    rows, side = narrow * owned, (me // narrow) % 2
    sides = [(1 - side).reshape(1).astype(jnp.int32), side.reshape(1).astype(jnp.int32)]
    if rows % 128 == 0:
        sent = dw(sides[0], lhs, rhs, rows, wide // 2)
        sent, lhs = tie(sent, lhs)
        got = swap(sent, narrow, wide * narrow)
        mine = dw(sides[1], lhs, rhs, rows, wide // 2)
        return mine, got
    repeats = rhs.shape[0] // lhs.shape[0]
    left = [lhs[0]] * 3 + [lhs[1]] if repeats == 2 else list(lhs)
    grad = jnp.concatenate([tn(a, b) for a, b in zip(left, rhs)], axis=0).astype(BF16)
    grad = grad.reshape(wide // 2, 2, rows, D)
    return part(grad, me, narrow, 1, True), swap(part(grad, me, narrow, 1, False), narrow, wide * narrow)


def spread(seqs, shares):
    runs, at = [], 0
    for j, share in enumerate(shares):
        upto = seqs * sum(shares[:j + 1]) // sum(shares)
        if upto > at:
            runs.append((at, upto - at))
        at = upto
    return runs


def forward_by_permutes(me, wide, narrow, tokens, seg, feat, attention, feedforward, vector):
    seqs = seg.shape[0]
    me1 = me.reshape(1).astype(jnp.int32)
    small = gather_small(vector, me, wide, narrow)
    vec = jnp.pad(jnp.transpose(small, (1, 0, 2)).reshape(small.shape[1], D).astype(F32), ((0, 3), (0, 0)))
    near = Gather(attention, wide, narrow)
    far = Gather(feedforward, wide, narrow)
    ready = narrow.bit_length() - 2
    early = len(far.turns) - 3
    for t in range(len(near.turns)):
        near.turn()
        behind = t > ready and early > 0
        if behind:
            far.turn()
            early -= 1
        near.got, far.held = tie(near.got, far.held)
        if behind:
            near.got, far.got = tie(near.got, far.got)
            far.take()
        weights = near.take()
    att, offsets = weights
    held = ()
    runs = spread(seqs, (1, 2, 1))
    for first_seq, count in runs:
        more = len(far.turns) > 0
        if more:
            far.held, source = tie(far.held, held if held else att)
            far.turn()
        else:
            source = held if held else att
        if held:
            *held, natural = *k1(first_seq, count, me1, tokens, seg, feat, [natural], offsets, vec, source), natural
        else:
            *held, natural = k1(first_seq, count, me1, tokens, seg, feat, source, offsets, vec, ())
        held = tuple(held)
        if more:
            far.got, held = tie(far.got, held)
            ff = far.take()
    while far.turns:
        far.turn()
        ff = far.take()
    ff = ff[0]
    return (*held, vec, natural, ff, offsets)


def local(wide, narrow, tokens, cotangent, segment_ids, feature_ids,
          attention_master, attention_first, attention_second,
          feedforward_master, feedforward_first, feedforward_second,
          vector_master, vector_first, vector_second):
    devices = wide * narrow
    me = lax.axis_index(BOTH)
    me1 = me.reshape(1).astype(jnp.int32)
    seg, feat = segment_ids, feature_ids
    seqs = seg.shape[0]
    shards = [m.astype(BF16) for m in (attention_master, feedforward_master, vector_master)]
    if devices <= 32:
        *held, vec, natural, ff = gathering_k1(wide, narrow, tokens, seg, feat, *shards)
        ff, offsets = [ff], ()
    else:
        *held, vec, natural, ff, offsets = forward_by_permutes(me, wide, narrow, tokens, seg, feat, *shards)
    mixed, q, k, v, ctx, lse = held
    out, first, fb, dctx, broad, slim, vg2 = k2(me1, mixed, ctx, cotangent, natural, ff, offsets, vec)
    ff_sum = Scatter(me, wide, narrow)
    ff_sum.begin(*split_grads(me, broad, slim, wide, narrow, feedforward_master.shape[0]))
    vg3, held, ff_owned = 0.0, (), None
    for first_seq, count in spread(seqs, (2, 1, 1)):
        def attend(given):
            source, kept = given
            return k3(first_seq, count, *source, ctx, dctx, fb, lse, seg, kept)
        (grads, more), ff_owned = ff_sum.over(((q, k, v), held), attend)
        held, vg3 = (grads,), vg3 + more
    d = held[0]
    if ff_owned is None:
        (mine, got), ff_owned = ff_sum.over((ctx, d), lambda g: split_grads(me, *g, wide, narrow, attention_master.shape[0]))
    else:
        mine, got = split_grads(me, ctx, d, wide, narrow, attention_master.shape[0])
    while ff_owned is None:
        _, ff_owned = ff_sum.over((), lambda g: ())
    att_sum = Scatter(me, wide, narrow)
    att_sum.begin(mine, got)
    vg4, held, att_owned = 0.0, (), None
    for first_seq, count in spread(seqs, (2, 1, 1)):
        def back(given):
            source, kept = given
            return k4(first_seq, count, source, d, tokens, seg, feat, natural, vec, kept)
        (grads, more), att_owned = att_sum.over((first, held), back)
        held, vg4 = (grads,), vg4 + more
    token_grads = held[0]
    vec_grad = jnp.concatenate([vg4[0:1], vg3[0:2], vg2[:10]], axis=0)
    vec_owned = scatter_small(jnp.transpose(vec_grad.reshape(vec_grad.shape[0], devices, -1), (1, 0, 2)), me, wide, narrow)
    while att_owned is None:
        att_sum.turn()
        att_owned = att_sum.take()
    ff_rate = rates(feedforward_master.shape[0], FF, D ** (-0.5), FF ** (-0.5))
    att_rate = rates(attention_master.shape[0], 3 * D, D ** (-0.5), (D // 64) ** (-0.5))
    f_new = adam_step(feedforward_master, feedforward_first, feedforward_second, ff_owned, ff_rate)
    a_new = adam_step(attention_master, attention_first, attention_second, att_owned, att_rate)
    v_new = adam_step(vector_master, vector_first, vector_second, vec_owned, VECTOR_RATE)
    result = [out, token_grads]
    for new in (a_new, f_new, v_new):
        result += [*new, new[0].astype(BF16)]
    return tuple(result)


def solution(mesh):
    rows, cols = P(BOTH, None), P(None, BOTH)
    return jax.shard_map(
        partial(local, mesh.shape["wide"], mesh.shape["narrow"]), mesh=mesh,
        in_specs=(rows,) * 10 + (cols,) * 3,
        out_specs=(rows,) * 10 + (cols,) * 4,
        check_vma=False,
    )
```

```python
from functools import partial
import jax, jax.numpy as jnp
from jax import lax
from jax.experimental import pallas as pl
from jax.experimental.pallas import tpu as pltpu
from jax.sharding import PartitionSpec as P

D = 768
FF = 3072
HEADS = 12
HEAD_DIM = 64
NORM_EPS = 1e-05
AWAY = -1e30
F32, BF16 = jnp.float32, jnp.bfloat16
ERFC = (0.11841221385764535, 0.11979147087435008, 0.09737185909338779, 0.13434283549706147,
        -0.0652102059595758, 0.2202795624136942, -0.16009561537425632, 0.035107795064101)
VMEM = pltpu.VMEM


def nn(a, b):
    return lax.dot_general(a, b, (((1,), (0,)), ((), ())), preferred_element_type=F32)

def nt(a, b):
    return lax.dot_general(a, b, (((1,), (1,)), ((), ())), preferred_element_type=F32)

def tn(a, b):
    return lax.dot_general(a, b, (((0,), (0,)), ((), ())), preferred_element_type=F32)

def whole(shape):
    return pl.BlockSpec(shape, lambda *_: (0,) * len(shape), pipeline_mode=pl.Buffered(1))

def gelu_pair(h):
    below = 0.5 + 0.5 * lax.erf(h * 0.7071067811865476)
    bell = jnp.exp(h * h * -0.5)
    return h * below, below + h * (bell * 0.3989422804014327)


def column_of(row):
    return jnp.transpose(jnp.broadcast_to(row, (8, row.shape[1])))[:, :1]

def group_of(seg, feat):
    both = seg * 16 + feat
    return column_of(both) == both

def cost(gigaflops, megabytes):
    return pl.CostEstimate(flops=int(gigaflops * 1e9), bytes_accessed=int(megabytes * 1e6), transcendentals=0)


def fetch_weights(me, offsets, pieces, w_ref, sem):
    rows = pieces[0].shape[1]
    half = D // 2
    copies = []
    for j, offset in enumerate(offsets):
        for side in range(2):
            for col in range(2):
                owner = (me ^ offset[col]) if side == 0 else (me ^ offset[col] ^ offset[2])
                at = pl.ds(pl.multiple_of(owner * rows, 8), rows)
                copies.append(pltpu.make_async_copy(pieces[2 * side + col].at[j], w_ref.at[at, pl.ds(col * half, half)], sem))
    for c in copies:
        c.start()
    for c in copies:
        c.wait()

def attend_forward(i, tok_ref, seg_ref, feat_ref, w_ref, vec_ref, mixed_ref, q_ref, k_ref, v_ref, ctx_ref, lse_ref, bias_scr, service):
    seg = seg_ref[pl.ds(i, 1), :]
    feat = feat_ref[pl.ds(i, 1), :]
    length = seg.shape[1]
    bias_scr[...] = jnp.where(column_of(seg) == seg, 0.0, AWAY)
    group = group_of(seg, feat)
    members = jnp.sum(group.astype(F32), axis=1, keepdims=True)
    tok = tok_ref[...]
    merging = nn(group.astype(F32).astype(BF16), tok) / members
    mixed = tok.astype(F32) + vec_ref[0:1, :] * merging
    mixed_ref[...] = mixed
    mb = mixed.astype(BF16)
    ctx_ref[0] = mb
    q_ref[...] = ((nn(mb, w_ref[0:D, :]) + vec_ref[1:2, :]) * 0.125).astype(BF16)
    k_ref[...] = nn(mb, w_ref[D:2 * D, :]).astype(BF16)
    v_ref[...] = (nn(mb, w_ref[2 * D:3 * D, :]) + vec_ref[2:3, :]).astype(BF16)
    lane = lax.broadcasted_iota(jnp.int32, (length, 128), 1)
    low = lane < HEAD_DIM
    lse_ref[...] = jnp.zeros_like(lse_ref)

    def pair(p, carry):
        at = pl.ds(pl.multiple_of(p * 128, 128), 128)
        qp = q_ref[:, at]
        kp = k_ref[:, at]
        vp = v_ref[:, at]
        outs = []
        zero = jnp.zeros_like(qp)
        for half in range(2):
            mine = low if half == 0 else jnp.logical_not(low)
            s = nt(jnp.where(mine, qp, zero), kp) + bias_scr[...]
            top = jnp.max(s, axis=1, keepdims=True)
            e = jnp.exp(s - top)
            total = jnp.sum(e, axis=1, keepdims=True)
            o = nn(e.astype(BF16), vp) * (1.0 / total)
            outs.append(o)
            lse_ref[...] = jnp.where(lane == 2 * p + half, top + jnp.log(total), lse_ref[...])
        ctx_ref[1, :, at] = jnp.where(low, outs[0], outs[1]).astype(BF16)
        return carry
    service(0)
    lax.fori_loop(0, HEADS // 4, pair, 0)
    service(1)
    lax.fori_loop(HEADS // 4, HEADS // 2, pair, 0)
    service(2)


def k1_body(first_seq, offsets, kept, self_ref, tok_ref, seg_ref, feat_ref, vec_ref, *rest):
    if kept:
        w_ref, rest = rest[0], rest[1 + kept:]
        mixed_ref, q_ref, k_ref, v_ref, ctx_ref, lse_ref, bias_scr = rest
    else:
        pieces, rest = rest[:4], rest[4:]
        mixed_ref, q_ref, k_ref, v_ref, ctx_ref, lse_ref, w_ref, bias_scr, sem = rest
    i = pl.program_id(0) + first_seq

    if not kept:
        @pl.when(pl.program_id(0) == 0)
        def _():
            fetch_weights(self_ref[0], offsets, pieces, w_ref, sem)

    attend_forward(i, tok_ref, seg_ref, feat_ref, w_ref, vec_ref, mixed_ref, q_ref, k_ref, v_ref, ctx_ref, lse_ref, bias_scr, lambda point: None)


def k1(first_seq, count, me, tokens, seg, feat, weights, offsets, vec, kept):
    seqs, length = seg.shape
    blk = pl.BlockSpec((length, D), lambda i, s: (i + first_seq, 0))
    both = pl.BlockSpec((2, length, D), lambda i, s: (0, i + first_seq, 0))
    narrow = pl.BlockSpec((length, 128), lambda i, s: (i + first_seq, 0))
    n = seqs * length
    o = lambda dt: jax.ShapeDtypeStruct((n, D), dt)
    any_spec = pl.BlockSpec(memory_space=pl.ANY)
    out_specs = [blk] * 4 + [both, narrow]
    out_shape = [o(F32), o(BF16), o(BF16), o(BF16), jax.ShapeDtypeStruct((2, n, D), BF16), jax.ShapeDtypeStruct((n, 128), F32)]
    scratch = [VMEM((length, length), F32)]
    if kept:
        weight_specs = [pl.BlockSpec((3 * D, D), lambda i, s: (0, 0), pipeline_mode=pl.Buffered(1))]
    else:
        weight_specs = [any_spec] * 4
        out_specs = out_specs + [whole((4 * D, D))]
        out_shape = out_shape + [jax.ShapeDtypeStruct((4 * D, D), BF16)]
        scratch = scratch + [pltpu.SemaphoreType.DMA]
    return pl.pallas_call(
        partial(k1_body, first_seq, offsets, len(kept)),
        grid_spec=pltpu.PrefetchScalarGridSpec(
            num_scalar_prefetch=1, grid=(count,),
            in_specs=[blk, whole(seg.shape), whole(feat.shape), whole(vec.shape)] + weight_specs + [any_spec] * len(kept),
            out_specs=out_specs, scratch_shapes=scratch,
        ),
        out_shape=out_shape,
        input_output_aliases={6 + j: j for j in range(len(kept))},
        cost_estimate=cost(count * 11, count * 4),
        name="mix_attend",
    )(me, tokens, seg, feat, vec, *weights, *kept)

MESH = pl.DeviceIdType.MESH


def flips(x, mask):
    bit = 1
    while bit <= mask:
        if mask & bit:
            x = x + bit - 2 * bit * ((x // bit) % 2)
        bit *= 2
    return x


class Spreading:
    def __init__(self, wide, narrow, shard, full, columns, sems):
        self.narrow, self.masks = narrow, wide // 2
        self.bits = [1 << b for b in range((wide // 2).bit_length() - 1)]
        w, self.z = lax.axis_index("wide"), lax.axis_index("narrow")
        self.o, self.c = w // 2, w % 2
        self.shard, self.full, self.columns = shard, full, columns
        self.line_out, self.line_in, self.tree_out, self.tree_in, self.core_out, self.core_in, self.own = sems

    def at(self, r, k, c=None, h=None):
        c = self.c if c is None else c
        rows = self.shard.shape[0]
        owner = (2 * flips(self.o, r) + c) * self.narrow + flips(self.z, k)
        where = pl.ds(pl.multiple_of(owner * rows, 8), rows)
        if h is None:
            return self.full.at[where, :]
        return self.full.at[where, pl.ds(*self.columns[h][:2])]

    def source(self, r, k, h=None):
        if r or k:
            return self.at(r, k, None, h)
        return self.shard if h is None else self.shard.at[:, pl.ds(*self.columns[h][:2])]

    def keep(self):
        return pltpu.make_async_copy(self.shard, self.at(0, 0), self.own)

    def line(self, k, arriving=False):
        return pltpu.make_async_remote_copy(
            self.shard, self.at(0, k if arriving else 0), self.line_out.at[k - 1], self.line_in.at[k - 1],
            device_id=(2 * self.o + self.c, flips(self.z, k)), device_id_type=MESH)

    def tree(self, r, k, h, bit, arriving=False):
        there = r if arriving else r ^ bit
        n = (k * len(self.columns) + h) * self.masks + there
        part = self.at(r, k, None, h)
        return pltpu.make_async_remote_copy(
            part if arriving else self.source(r, k, h), part, self.tree_out.at[n], self.tree_in.at[n],
            device_id=(2 * flips(self.o, bit) + self.c, self.z), device_id_type=MESH)

    def core(self, r, k, arriving=False):
        n = k * self.masks + r
        part = self.at(r, k, 1 - self.c if arriving else None)
        return pltpu.make_async_remote_copy(
            part if arriving else self.source(r, k), part, self.core_out.at[n], self.core_in.at[n],
            device_id=(2 * self.o + 1 - self.c, self.z), device_id_type=MESH)

    def onward(self, r, h):
        if self.columns[h][2]:
            return [b for b in reversed(self.bits) if r == 0 or b < (r & -r)]
        return [b for b in self.bits if b > r]

    def last_bit(self, r, h):
        if self.columns[h][2]:
            return r & -r
        return 1 << (r.bit_length() - 1)

    def open(self):
        self.keep().start()
        for k in range(1, self.narrow):
            self.line(k).start()

    def send_on(self, r, k, h):
        for bit in self.onward(r, h):
            self.tree(r, k, h, bit).start()

    def roots(self, k):
        if k:
            self.line(k, True).wait_recv()
        for h in range(len(self.columns)):
            self.send_on(0, k, h)
        self.core(0, k).start()

    def relay(self, r, k):
        for h in range(len(self.columns)):
            self.tree(r, k, h, self.last_bit(r, h), True).wait_recv()
            self.send_on(r, k, h)
        self.core(r, k).start()

    def close(self):
        for k in range(self.narrow):
            for r in range(self.masks):
                self.core(r, k, True).wait_recv()
        self.keep().wait()

    def drain(self):
        for k in range(self.narrow):
            if k:
                self.line(k).wait_send()
            for r in range(self.masks):
                for h in range(len(self.columns)):
                    for bit in self.onward(r, h):
                        self.tree(r, k, h, bit).wait_send()
                self.core(r, k).wait_send()


def spreading_sems(wide, narrow, halves):
    dma = pltpu.SemaphoreType.DMA
    tree, core = narrow * halves * (wide // 2), narrow * (wide // 2)
    return [dma((narrow - 1,)), dma((narrow - 1,)), dma((tree,)), dma((tree,)), dma((core,)), dma((core,)), dma]


def greet(wide, narrow):
    barrier = pltpu.get_barrier_semaphore()
    w, z = lax.axis_index("wide"), lax.axis_index("narrow")
    o, c = w // 2, w % 2
    peers = [(w, flips(z, k)) for k in range(1, narrow)] + [(2 * o + 1 - c, z)]
    bit = 1
    while bit < wide // 2:
        peers.append((2 * flips(o, bit) + c, z))
        bit *= 2
    for peer in peers:
        pl.semaphore_signal(barrier, inc=1, device_id=peer, device_id_type=MESH)
    pl.semaphore_wait(barrier, len(peers))


def gathering_k1_body(wide, narrow, cols, steps, tok_ref, seg_ref, feat_ref, att_ref, ff_ref, vs_ref,
                      mixed_ref, q_ref, k_ref, v_ref, ctx_ref, lse_ref, vec_ref, wout_ref, fout_ref,
                      bias_scr, w_ref, vs_scr, put_sem, *sems):
    i = pl.program_id(0)
    half = D // 2
    count = len(sems) // 3
    pairs = [(0, half, False), (half, half, True)]
    att = Spreading(wide, narrow, att_ref, w_ref, pairs, sems[:count])
    ff = Spreading(wide, narrow, ff_ref, fout_ref, pairs, sems[count:2 * count])
    vs = Spreading(wide, narrow, vs_ref, vs_scr, [(0, 128, False)], sems[2 * count:])
    levels = {deep: [r for r in range(1, wide // 2) if (r & (r - 1) != 0) == deep] for deep in (False, True)}
    save = pltpu.make_async_copy(w_ref, wout_ref, put_sem)

    @pl.when(i == 0)
    def _():
        greet(wide, narrow)
        for one in (vs, att, ff):
            one.open()
        for k in range(narrow):
            vs.roots(k)
            att.roots(k)
        ff.roots(0)
        for r in range(1, wide // 2):
            for k in range(narrow):
                vs.relay(r, k)
                att.relay(r, k)
        vs.close()
        vec = jnp.zeros((16, D), F32)
        row = lax.broadcasted_iota(jnp.int32, (128, D), 0)
        col = lax.broadcasted_iota(jnp.int32, (128, D), 1)
        for d in range(wide * narrow):
            pick = jnp.logical_and(row < cols, col == row + cols * d).astype(F32).astype(BF16)
            vec = vec + nn(vs_scr[16 * d:16 * d + 16, :], pick)
        vec_ref[...] = vec
        att.close()
        save.start()

    plan = [[lambda k=k: ff.roots(k)] for k in range(1, narrow)]
    for r in range(1, wide // 2):
        plan += [[lambda r=r, k=k: ff.relay(r, k)] for k in range(narrow)]

    def service(point):
        for s in range(steps):
            todo = slots.get((s, point), ())
            if todo:
                @pl.when(i == s)
                def _(todo=todo):
                    for act in todo:
                        act()
    total = steps * 3 - 1
    slots = {}
    for n, group in enumerate(plan):
        spot = n * total // len(plan)
        slots.setdefault((spot // 3, spot % 3), []).extend(group)

    attend_forward(i, tok_ref, seg_ref, feat_ref, w_ref, vec_ref, mixed_ref, q_ref, k_ref, v_ref, ctx_ref, lse_ref, bias_scr, service)

    @pl.when(i == steps - 1)
    def _():
        ff.close()
        for one in (vs, att, ff):
            one.drain()
        save.wait()


def gathering_k1(wide, narrow, tokens, seg, feat, att_shard, ff_shard, vec_shard):
    seqs, length = seg.shape
    n, devices = seqs * length, wide * narrow
    vs = jnp.pad(vec_shard, ((0, 16 - vec_shard.shape[0]), (0, 128 - vec_shard.shape[1])))
    blk = pl.BlockSpec((length, D), lambda i: (i, 0))
    any_spec = pl.BlockSpec(memory_space=pl.ANY)
    o = lambda dt: jax.ShapeDtypeStruct((n, D), dt)
    sems = spreading_sems(wide, narrow, 2) * 2 + spreading_sems(wide, narrow, 1)
    return pl.pallas_call(
        partial(gathering_k1_body, wide, narrow, vec_shard.shape[1], seqs), grid=(seqs,),
        in_specs=[blk, whole(seg.shape), whole(feat.shape), any_spec, any_spec, any_spec],
        out_specs=[blk] * 4 + [pl.BlockSpec((2, length, D), lambda i: (0, i, 0)), pl.BlockSpec((length, 128), lambda i: (i, 0)),
                               whole((16, D)), any_spec, any_spec],
        out_shape=[o(F32), o(BF16), o(BF16), o(BF16), jax.ShapeDtypeStruct((2, n, D), BF16), jax.ShapeDtypeStruct((n, 128), F32),
                   jax.ShapeDtypeStruct((16, D), F32), jax.ShapeDtypeStruct((4 * D, D), BF16), jax.ShapeDtypeStruct((2 * FF, D), BF16)],
        scratch_shapes=[VMEM((length, length), F32), VMEM((4 * D, D), BF16), VMEM((16 * devices, 128), BF16), pltpu.SemaphoreType.DMA, *sems],
        compiler_params=pltpu.CompilerParams(collective_id=0, has_side_effects=True),
        cost_estimate=cost(60, 60),
        name="gather_attend",
    )(tokens, seg, feat, att_shard, ff_shard, vs)

def masks_of(bits):
    found = [0]
    for b in bits:
        found = found + [m | b for m in found]
    return sorted(found, key=lambda m: (-bin(m).count("1"), m))


class Halving:
    def __init__(self, wide, narrow, total, tree_refs, line_refs, sems):
        bits = [1 << b for b in range((wide // 2).bit_length() - 1)]
        w, self.z = lax.axis_index("wide"), lax.axis_index("narrow")
        self.o, self.c = w // 2, w % 2
        self.total, self.tree_refs, self.line_refs, self.sems = total, tree_refs, line_refs, sems
        self.rows = total.shape[1] // narrow
        self.orders = [bits, bits[::-1]]
        self.line_bits = [1 << b for b in range(narrow.bit_length() - 1)]
        self.names = [("tree", h, t, m) for t in range(len(bits)) for h in range(2) for m in masks_of(self.orders[h][t + 1:])]
        if line_refs:
            self.names += [("line", 0, t, m) for t in range(len(self.line_bits)) for m in masks_of(self.line_bits[t + 1:])]

    def copy(self, name):
        kind, h, t, m = name
        n = self.names.index(name)
        if kind == "tree":
            bit = self.orders[h][t]
            cols = pl.ds(h * (D // 2), D // 2)
            slot = masks_of(self.orders[h][t + 1:]).index(m)
            source = self.total.at[flips(self.o, bit | m), :, cols]
            landing = self.tree_refs[t].at[h, slot]
            device = (2 * flips(self.o, bit) + self.c, self.z)
        else:
            bit = self.line_bits[t]
            slot = masks_of(self.line_bits[t + 1:]).index(m)
            source = self.total.at[self.o, pl.ds(pl.multiple_of(flips(self.z, bit | m) * self.rows, 8), self.rows), :]
            landing = self.line_refs[t].at[slot]
            device = (2 * self.o + self.c, flips(self.z, bit))
        return pltpu.make_async_remote_copy(source, landing, self.sems[0].at[n], self.sems[1].at[n], device_id=device, device_id_type=MESH)

    def pick(self, kind, turn, deep):
        return [n for n in self.names if n[0] == kind and n[2] == turn and (n[3] != 0) == deep]

    def send(self, kind, turn):
        for deep in (True, False):
            for name in self.pick(kind, turn, deep):
                self.copy(name).start()

    def take(self, kind, turn, deep):
        for name in self.pick(kind, turn, deep):
            self.copy(name).wait_recv()
            _, h, t, m = name
            if kind == "tree":
                cols = pl.ds(h * (D // 2), D // 2)
                slot = masks_of(self.orders[h][t + 1:]).index(m)
                self.total[flips(self.o, m), :, cols] = self.total[flips(self.o, m), :, cols] + self.tree_refs[t][h, slot]
            else:
                slot = masks_of(self.line_bits[t + 1:]).index(m)
                at = pl.ds(pl.multiple_of(flips(self.z, m) * self.rows, 8), self.rows)
                self.total[self.o, at, :] = self.total[self.o, at, :] + self.line_refs[t][slot]

    def drain(self):
        for name in self.names:
            self.copy(name).wait_send()


def halving_scratch(wide, narrow, rows, line):
    outer, inner = (wide // 2).bit_length() - 1, narrow.bit_length() - 1
    groups = wide // 2
    shapes = [VMEM((groups, narrow * rows, D), BF16)]
    shapes += [VMEM((2, groups >> (t + 1), narrow * rows, D // 2), BF16) for t in range(outer)]
    count = 2 * (groups - 1)
    if line:
        shapes += [VMEM((narrow >> (t + 1), rows, D), BF16) for t in range(inner)]
        count += narrow - 1
    return shapes + [pltpu.SemaphoreType.DMA((count,)), pltpu.SemaphoreType.DMA((count,))]


def begin_total(total, mine_ref, got_ref):
    def one(g, carry):
        total[g] = mine_ref[g] + got_ref[g]
        return carry
    lax.fori_loop(0, total.shape[0], one, 0)

def norm_parts(z):
    mean = jnp.mean(z, axis=1, keepdims=True)
    c = z - mean
    var = jnp.mean(c * c, axis=1, keepdims=True)
    inv = lax.rsqrt(var + NORM_EPS)
    return c * inv, inv

def norm_pull(g, xhat, inv):
    a = jnp.mean(g, axis=1, keepdims=True)
    b = jnp.mean(g * xhat, axis=1, keepdims=True)
    return (g - a - xhat * b) * inv

def colsum(x):
    return jnp.sum(x, axis=0, keepdims=True)

def k2_body(offsets, self_ref, mixed_ref, ctx_ref, cot_ref, wo_ref, vec_ref, *rest):
    if offsets:
        pieces, rest = rest[:4], rest[4:]
        out_ref, first_ref, fb_ref, dctx_ref, wide_ref, slim_ref, vg_ref, gp_scr, sum_scr, wf_ref, sem = rest
    else:
        wf_ref, out_ref, first_ref, fb_ref, dctx_ref, wide_ref, slim_ref, vg_ref, gp_scr, sum_scr = rest
    ctx_ref = ctx_ref.at[0]
    hg_ref, act_ref = wide_ref.at[0], wide_ref.at[1]
    nb_ref, bg_ref = slim_ref.at[0], slim_ref.at[1]
    @pl.when(pl.program_id(0) == 0)
    def _():
        vg_ref[...] = jnp.zeros_like(vg_ref)
        if offsets:
            fetch_weights(self_ref[0], offsets, pieces, wf_ref, sem)

    ex = FF // D
    first_sum = mixed_ref[...] + nn(ctx_ref[...], wo_ref[...]) + vec_ref[3:4, :]
    xhat1, inv1 = norm_parts(first_sum)
    normed = xhat1 * vec_ref[4:5, :] + vec_ref[5:6, :]
    nb_ref[...] = normed.astype(BF16)
    sum_scr[...] = normed + vec_ref[6 + ex:7 + ex, :]
    for c in range(ex):
        at = pl.ds(c * D, D)
        h = nt(nb_ref[...], wf_ref[at, :]) + vec_ref[6 + c:7 + c, :]
        act, slope = gelu_pair(h)
        act_ref[:, at] = act.astype(BF16)
        gp_scr[:, at] = slope.astype(gp_scr.dtype)
        sum_scr[...] += nn(act_ref[:, at], wf_ref[pl.ds(FF + c * D, D), :])
    xhat2, inv2 = norm_parts(sum_scr[...])
    out_ref[...] = (xhat2 * vec_ref[7 + ex:8 + ex, :] + vec_ref[8 + ex:9 + ex, :]).astype(BF16)
    cot = cot_ref[...].astype(F32)
    vg_ref[4 + ex:5 + ex, :] += colsum(cot * xhat2)
    vg_ref[5 + ex:6 + ex, :] += colsum(cot)
    gs = norm_pull(cot * vec_ref[7 + ex:8 + ex, :], xhat2, inv2)
    vg_ref[3 + ex:4 + ex, :] += colsum(gs)
    bg_ref[...] = gs.astype(BF16)
    sum_scr[...] = gs
    for c in range(ex):
        at = pl.ds(c * D, D)
        hg = nt(bg_ref[...], wf_ref[pl.ds(FF + c * D, D), :]) * gp_scr[:, at].astype(F32)
        vg_ref[3 + c:4 + c, :] += colsum(hg)
        hg_ref[:, at] = hg.astype(BF16)
        sum_scr[...] += nn(hg_ref[:, at], wf_ref[at, :])
    ng = sum_scr[...]
    vg_ref[1:2, :] += colsum(ng * xhat1)
    vg_ref[2:3, :] += colsum(ng)
    fgr = norm_pull(ng * vec_ref[4:5, :], xhat1, inv1)
    vg_ref[0:1, :] += colsum(fgr)
    first_ref[...] = fgr
    fb_ref[...] = fgr.astype(BF16)
    dctx_ref[...] = nt(fb_ref[...], wo_ref[...]).astype(BF16)


def k2(me, mixed, ctx, cot, att, ff, offsets, vec, tile=256):
    n = mixed.shape[0]
    blk = pl.BlockSpec((tile, D), lambda i, s: (i, 0))
    o = lambda *w, dt=BF16: jax.ShapeDtypeStruct(w, dt)
    any_spec = pl.BlockSpec(memory_space=pl.ANY)
    return pl.pallas_call(
        partial(k2_body, offsets),
        grid_spec=pltpu.PrefetchScalarGridSpec(
            num_scalar_prefetch=1, grid=(n // tile,),
            in_specs=[blk, pl.BlockSpec((1, tile, D), lambda i, s: (1, i, 0)), blk,
                      pl.BlockSpec((D, D), lambda i, s: (3, 0), pipeline_mode=pl.Buffered(1)), whole(vec.shape)]
            + ([any_spec] * 4 if offsets else [whole(ff[0].shape)]),
            out_specs=[blk, blk, blk, blk, pl.BlockSpec((2, tile, FF), lambda i, s: (0, i, 0)),
                       pl.BlockSpec((2, tile, D), lambda i, s: (0, i, 0)), pl.BlockSpec((16, D), lambda i, s: (0, 0))],
            scratch_shapes=[VMEM((tile, FF), F32), VMEM((tile, D), F32)]
            + ([VMEM((2 * FF, D), BF16), pltpu.SemaphoreType.DMA] if offsets else []),
        ),
        out_shape=[o(n, D), o(n, D, dt=F32), o(n, D), o(n, D), o(2, n, FF), o(2, n, D), o(16, D, dt=F32)],
        cost_estimate=cost(60, 80),
        name="feed_forward",
    )(me, mixed, ctx, cot, att, vec, *ff)

def dw_body(rows, side_ref, lhs_ref, rhs_ref, out_ref):
    step = 384 if rows % 384 == 0 else 128
    for at in range(0, rows, step):
        out_ref[0, at:at + step, :] = tn(lhs_ref[0, :, at:at + step], rhs_ref[0]).astype(BF16)


def dw(side, lhs, rhs, rows, count):
    n, span = lhs.shape[1:]
    per = span // rows
    repeats = rhs.shape[0] // lhs.shape[0]
    tall = lambda i, s: (2 * i + s[0]) // per
    left = (lambda t: t // 3) if repeats == 2 else (lambda t: t)
    return pl.pallas_call(
        partial(dw_body, rows),
        grid_spec=pltpu.PrefetchScalarGridSpec(
            num_scalar_prefetch=1, grid=(count,),
            in_specs=[pl.BlockSpec((1, n, rows), lambda i, s: (left(tall(i, s)), 0, (2 * i + s[0]) % per)),
                      pl.BlockSpec((1, n, D), lambda i, s: (tall(i, s), 0, 0))],
            out_specs=pl.BlockSpec((1, rows, D), lambda i, s: (i, 0, 0)),
        ),
        out_shape=jax.ShapeDtypeStruct((count, rows, D), BF16),
        cost_estimate=cost(2e-9 * n * rows * D * count, 10),
        name="weight_grad",
    )(side, lhs, rhs)

def attend_back_step(i, q_ref, k_ref, v_ref, ctx_ref, dctx_ref, fb_ref, lse_ref, seg_ref, d_ref, vg_ref, bias_scr, lse_scr, del_scr, service):
    ctx_ref = ctx_ref.at[0]
    dq_ref, dk_ref, dv_ref = d_ref.at[0], d_ref.at[1], d_ref.at[2]
    d_ref[3] = fb_ref[...]
    @pl.when(pl.program_id(0) == 0)
    def _():
        vg_ref[...] = jnp.zeros_like(vg_ref)
    seg = seg_ref[pl.ds(i, 1), :]
    length = seg.shape[1]
    bias_scr[...] = jnp.where(column_of(seg) == seg, 0.0, AWAY)
    lse_scr[...] = jnp.transpose(lse_ref[...])[:16, :]
    prod = dctx_ref[...].astype(F32) * ctx_ref[...].astype(F32)
    pick = (lax.broadcasted_iota(jnp.int32, (16, D), 1) // HEAD_DIM == lax.broadcasted_iota(jnp.int32, (16, D), 0)).astype(F32).astype(BF16)
    high = prod.astype(BF16)
    del_scr[...] = nt(pick, high) + nt(pick, (prod - high.astype(F32)).astype(BF16))
    low = lax.broadcasted_iota(jnp.int32, (length, 128), 1) < HEAD_DIM

    def pair(p, carry):
        at = pl.ds(pl.multiple_of(p * 128, 128), 128)
        qp, kp, vp, op = q_ref[:, at], k_ref[:, at], v_ref[:, at], dctx_ref[:, at]
        zero = jnp.zeros_like(qp)
        got = []
        for half in range(2):
            mine = low if half == 0 else jnp.logical_not(low)
            st = nt(jnp.where(mine, kp, zero), qp) + bias_scr[...]
            pt = jnp.exp(st - lse_scr[pl.ds(2 * p + half, 1), :])
            dv = nn(pt.astype(BF16), op)
            dpt = nt(jnp.where(mine, vp, zero), op)
            dst = (pt * (dpt - del_scr[pl.ds(2 * p + half, 1), :])).astype(BF16)
            dk = nn(dst, qp)
            dq = tn(dst, kp)
            got.append((dq, dk, dv))
        dq, dk, dv = (jnp.where(low, a, b) for a, b in zip(*got))
        dqb = dq.astype(BF16) * jnp.bfloat16(0.125)
        dvb = dv.astype(BF16)
        dq_ref[:, at] = dqb
        dk_ref[:, at] = dk.astype(BF16)
        dv_ref[:, at] = dvb
        vg_ref[0:1, at] += colsum(dqb.astype(F32))
        vg_ref[1:2, at] += colsum(dvb.astype(F32))
        return carry
    service(0)
    lax.fori_loop(0, HEADS // 4, pair, 0)
    service(1)
    lax.fori_loop(HEADS // 4, HEADS // 2, pair, 0)
    service(2)


def k3_body(first_seq, kept, *refs):
    ins, rest = refs[:8], refs[8 + kept:]
    attend_back_step(pl.program_id(0) + first_seq, *ins, *rest, lambda point: None)


def k3(first_seq, count, q, k, v, ctx, dctx, fb, lse, seg, kept):
    seqs, length = seg.shape
    n = seqs * length
    blk = pl.BlockSpec((length, D), lambda i: (i + first_seq, 0))
    return pl.pallas_call(
        partial(k3_body, first_seq, len(kept)), grid=(count,),
        in_specs=[blk] * 3 + [pl.BlockSpec((1, length, D), lambda i: (1, i + first_seq, 0)), blk, blk,
                              pl.BlockSpec((length, 128), lambda i: (i + first_seq, 0)), whole((seqs, length))]
        + [pl.BlockSpec(memory_space=pl.ANY)] * len(kept),
        out_specs=[pl.BlockSpec((4, length, D), lambda i: (0, i + first_seq, 0)), pl.BlockSpec((8, D), lambda i: (0, 0))],
        out_shape=[jax.ShapeDtypeStruct((4, n, D), BF16), jax.ShapeDtypeStruct((8, D), F32)],
        scratch_shapes=[VMEM((length, length), F32), VMEM((16, length), F32), VMEM((16, length), F32)],
        input_output_aliases={8 + j: j for j in range(len(kept))},
        cost_estimate=cost(count * 12, count * 6),
        name="attend_back",
    )(q, k, v, ctx, dctx, fb, lse, seg, *kept)

def summing_k3_body(wide, narrow, steps, *refs):
    ins, (mine_ref, got_ref, d_ref, vg_ref, own_ref), rest = refs[:8], refs[8:13], refs[13:]
    (bias_scr, lse_scr, del_scr, total), rest = rest[:4], rest[4:]
    *tree_refs, out_sems, in_sems = rest
    i = pl.program_id(0)
    turns = len(tree_refs)
    half = Halving(wide, narrow, total, tree_refs, [], (out_sems, in_sems))

    @pl.when(i == 0)
    def _():
        greet(wide, 1)
        begin_total(total, mine_ref, got_ref)
        half.send("tree", 0)

    def service(point):
        for t in range(turns):
            spot = 3 * steps * (t + 1) // (turns + 1) - 1 if t < turns - 1 else 3 * steps - 2
            if spot % 3 == point:
                @pl.when(i == spot // 3)
                def _(t=t):
                    if t < turns - 1:
                        half.take("tree", t, True)
                        half.send("tree", t + 1)
                    else:
                        for done in range(turns):
                            half.take("tree", done, False)

    attend_back_step(i, *ins, d_ref, vg_ref, bias_scr, lse_scr, del_scr, service)

    @pl.when(i == steps - 1)
    def _():
        half.drain()
        own_ref[...] = total[lax.axis_index("wide") // 2]


def summing_k3(wide, narrow, q, k, v, ctx, dctx, fb, lse, seg, mine, got):
    seqs, length = seg.shape
    n = seqs * length
    blk = pl.BlockSpec((length, D), lambda i: (i, 0))
    span = mine.shape[1]
    return pl.pallas_call(
        partial(summing_k3_body, wide, narrow, seqs), grid=(seqs,),
        in_specs=[blk] * 3 + [pl.BlockSpec((1, length, D), lambda i: (1, i, 0)), blk, blk,
                              pl.BlockSpec((length, 128), lambda i: (i, 0)), whole((seqs, length)), whole(mine.shape), whole(got.shape)],
        out_specs=[pl.BlockSpec((4, length, D), lambda i: (0, i, 0)), whole((8, D)), whole((span, D))],
        out_shape=[jax.ShapeDtypeStruct((4, n, D), BF16), jax.ShapeDtypeStruct((8, D), F32), jax.ShapeDtypeStruct((span, D), BF16)],
        scratch_shapes=[VMEM((length, length), F32), VMEM((16, length), F32), VMEM((16, length), F32),
                        *halving_scratch(wide, narrow, span // narrow, False)],
        compiler_params=pltpu.CompilerParams(collective_id=1, has_side_effects=True),
        cost_estimate=cost(60, 40),
        name="attend_back_sum",
    )(q, k, v, ctx, dctx, fb, lse, seg, mine, got)


def token_back_step(i, first_ref, d_ref, tok_ref, seg_ref, feat_ref, w_ref, vec_ref, tg_ref, vg_ref):
    dq_ref, dk_ref, dv_ref = d_ref.at[0], d_ref.at[1], d_ref.at[2]

    @pl.when(pl.program_id(0) == 0)
    def _():
        vg_ref[...] = jnp.zeros_like(vg_ref)
    group = group_of(seg_ref[pl.ds(i, 1), :], feat_ref[pl.ds(i, 1), :])
    gf = group.astype(F32)
    members = jnp.sum(gf, axis=1, keepdims=True)
    gb = gf.astype(BF16)
    tok = tok_ref[...]
    merging = nn(gb, tok) / members
    mg = (first_ref[...] + nt(dq_ref[...], w_ref[0:D, :]) + nt(dk_ref[...], w_ref[D:2 * D, :])
          + nt(dv_ref[...], w_ref[2 * D:3 * D, :]))
    vg_ref[0:1, :] += colsum(mg * merging)
    spread = (vec_ref[0:1, :] * mg / members).astype(BF16)
    tg_ref[...] = (mg + nn(gb, spread)).astype(BF16)


def k4_body(first_seq, kept, *refs):
    token_back_step(pl.program_id(0) + first_seq, *refs[:7], *refs[7 + kept:])


def summing_k4_body(wide, narrow, steps, *refs):
    ins, (mine_ref, got_ref, vg2_ref, vg3_ref, tg_ref, own_ref, vec_out), rest = refs[:7], refs[7:14], refs[14:]
    (vg_scr, total), rest = rest[:2], rest[2:]
    outer, inner = (wide // 2).bit_length() - 1, narrow.bit_length() - 1
    tree_refs, line_refs, rest = rest[:outer], rest[outer:outer + inner], rest[outer + inner:]
    out_sems, in_sems, sum_scr, came_scr, vec_sems_out, vec_sems_in = rest
    i = pl.program_id(0)
    half = Halving(wide, narrow, total, tree_refs, line_refs, (out_sems, in_sems))
    w, z = lax.axis_index("wide"), lax.axis_index("narrow")
    o, c = w // 2, w % 2
    peers = [(2 * o + 1 - c, z)] + [(2 * flips(o, 1 << b) + c, z) for b in range(outer)] + [(w, flips(z, 1 << b)) for b in range(inner)]

    def across(n):
        return pltpu.make_async_remote_copy(sum_scr.at[n], came_scr.at[n], vec_sems_out.at[n], vec_sems_in.at[n],
                                            device_id=peers[n], device_id_type=MESH)

    @pl.when(i == 0)
    def _():
        greet(wide, narrow)
        begin_total(total, mine_ref, got_ref)
        half.send("tree", 0)

    token_back_step(i, *ins, tg_ref, vg_scr)

    for t in range(outer - 1):
        @pl.when(i == min(steps - 1, (steps * (t + 1)) // (outer + 1)))
        def _(t=t):
            half.take("tree", t, True)
            half.send("tree", t + 1)

    @pl.when(i == steps - 1)
    def _():
        sum_scr[0, 0:1, :] = vg_scr[0:1, :]
        sum_scr[0, 1:3, :] = vg3_ref[0:2, :]
        sum_scr[0, 3:13, :] = vg2_ref[0:10, :]
        sum_scr[0, 13:16, :] = jnp.zeros((3, D), F32)
        across(0).start()
        for t in range(outer):
            half.take("tree", t, False)
        half.send("line", 0)
        turn = 0
        for n in range(len(peers)):
            across(n).wait_recv()
            added = sum_scr[n] + came_scr[n]
            if n + 1 < len(peers):
                sum_scr[n + 1] = added
                across(n + 1).start()
            else:
                vec_out[...] = added
            if n % 2 == 1 and turn < inner - 1:
                half.take("line", turn, True)
                half.take("line", turn, False)
                turn += 1
                half.send("line", turn)
        while turn < inner - 1:
            half.take("line", turn, True)
            half.take("line", turn, False)
            turn += 1
            half.send("line", turn)
        last = half.pick("line", turn, False)[0]
        half.copy(last).wait_recv()
        at = pl.ds(pl.multiple_of(z * half.rows, 8), half.rows)
        own_ref[...] = total[o, at, :].astype(F32) + line_refs[turn][0].astype(F32)
        half.drain()
        for n in range(len(peers)):
            across(n).wait_send()


def summing_k4(wide, narrow, first, d, tokens, seg, feat, att, vec, mine, got, vg2, vg3):
    seqs, length = seg.shape
    n = seqs * length
    blk = pl.BlockSpec((length, D), lambda i: (i, 0))
    rows = mine.shape[1] // narrow
    stages = (wide * narrow).bit_length() - 1
    return pl.pallas_call(
        partial(summing_k4_body, wide, narrow, seqs), grid=(seqs,),
        in_specs=[blk, pl.BlockSpec((3, length, D), lambda i: (0, i, 0)), blk, whole(seg.shape), whole(feat.shape),
                  pl.BlockSpec((3 * D, D), lambda i: (0, 0), pipeline_mode=pl.Buffered(1)), whole(vec.shape),
                  whole(mine.shape), whole(got.shape), whole(vg2.shape), whole(vg3.shape)],
        out_specs=[blk, whole((rows, D)), whole((16, D))],
        out_shape=[jax.ShapeDtypeStruct((n, D), BF16), jax.ShapeDtypeStruct((rows, D), F32), jax.ShapeDtypeStruct((16, D), F32)],
        scratch_shapes=[VMEM((8, D), F32), *halving_scratch(wide, narrow, rows, True),
                        VMEM((stages, 16, D), F32), VMEM((stages, 16, D), F32), pltpu.SemaphoreType.DMA((stages,)), pltpu.SemaphoreType.DMA((stages,))],
        compiler_params=pltpu.CompilerParams(collective_id=2, has_side_effects=True),
        cost_estimate=cost(30, 30),
        name="token_grad_sum",
    )(first, d, tokens, seg, feat, att, vec, mine, got, vg2, vg3)


def k4(first_seq, count, first, d, tokens, seg, feat, att, vec, kept):
    seqs, length = seg.shape
    n = seqs * length
    blk = pl.BlockSpec((length, D), lambda i: (i + first_seq, 0))
    return pl.pallas_call(
        partial(k4_body, first_seq, len(kept)), grid=(count,),
        in_specs=[blk, pl.BlockSpec((3, length, D), lambda i: (0, i + first_seq, 0)), blk, whole(seg.shape), whole(feat.shape),
                  pl.BlockSpec((3 * D, D), lambda i: (0, 0), pipeline_mode=pl.Buffered(1)), whole(vec.shape)]
        + [pl.BlockSpec(memory_space=pl.ANY)] * len(kept),
        out_specs=[blk, pl.BlockSpec((8, D), lambda i: (0, 0))],
        out_shape=[jax.ShapeDtypeStruct((n, D), BF16), jax.ShapeDtypeStruct((8, D), F32)],
        input_output_aliases={7 + j: j for j in range(len(kept))},
        cost_estimate=cost(count * 3, count * 5),
        name="token_grad",
    )(first, d, tokens, seg, feat, att, vec, *kept)

def adam_step(master, first, second, gradient, rate):
    first_new = BETA * first + (1.0 - BETA) * gradient
    second_new = BETA * second + (1.0 - BETA) * gradient * gradient
    correction = 1.0 - BETA**ADAM_STEP
    master_new = master - rate * (
        first_new / correction / (jnp.sqrt(second_new / correction) + ADAM_EPS) + DECAY * master
    )
    return (master_new, first_new, second_new)


BETA = 0.5
ADAM_STEP = 3
ADAM_EPS = 1e-08
DECAY = 0.01
VECTOR_RATE = 0.1
BOTH = ("wide", "narrow")


def rates(rows, split, first_rate, second_rate):
    index = (lax.axis_index(BOTH) * rows + jnp.arange(rows))[:, None]
    return jnp.where(index < split, first_rate, second_rate)


def tie(*groups):
    return lax.optimization_barrier(groups)


def bit_steps(wide, narrow):
    inner = [1 << b for b in range(narrow.bit_length() - 1)]
    outer = [narrow << b for b in range(1, wide.bit_length() - 1)]
    return inner, outer, narrow


def swap(value, bit, devices):
    return lax.ppermute(value, BOTH, [(i, i ^ bit) for i in range(devices)])


class Gather:
    def __init__(self, shard, wide, narrow):
        self.devices = wide * narrow
        inner, outer, self.core = bit_steps(wide, narrow)
        self.turns = [(bit,) for bit in reversed(inner)] + list(zip(outer, reversed(outer))) + [(self.core, self.core)]
        self.held, self.offsets, self.last = [shard[None]], [[0]], None

    def turn(self):
        bits = self.turns.pop(0)
        if len(bits) == 2 and len(self.held) == 1:
            whole_rows = self.held[0]
            self.held = [whole_rows[:, :, :D // 2], whole_rows[:, :, D // 2:]]
            self.offsets = self.offsets * 2
        self.bits = bits
        self.got = [swap(h, bit, self.devices) for h, bit in zip(self.held, bits)]

    def take(self):
        if not self.turns:
            return (*self.held, *self.got), tuple((a, b, self.core) for a, b in zip(*self.offsets))
        self.held = [jnp.concatenate(pair) for pair in zip(self.held, self.got)]
        self.offsets = [o + [x ^ bit for x in o] for o, bit in zip(self.offsets, self.bits)]


def gather_small(shard, me, wide, narrow):
    devices = wide * narrow
    held = shard[None]
    bit = 1
    while bit < devices:
        held = jnp.concatenate([held, swap(held, bit, devices)])
        bit *= 2
    bit = 1
    while bit < devices:
        split = held.reshape(devices // (2 * bit), 2, bit, *shard.shape)
        held = jnp.where((me & bit) != 0, split[:, ::-1], split).reshape(held.shape)
        bit *= 2
    return held


def part(value, me, bit, axis, mine):
    index = (me & bit) != 0
    index = index.astype(jnp.int32) if mine else 1 - index.astype(jnp.int32)
    return lax.dynamic_index_in_dim(value, index, axis, keepdims=False)


def add(a, b, kind=BF16):
    return (a.astype(F32) + b.astype(F32)).astype(kind)


class Scatter:
    def __init__(self, me, wide, narrow):
        self.me, self.devices, self.narrow = me, wide * narrow, narrow
        self.inner, outer, _ = bit_steps(wide, narrow)
        self.orders = [list(outer), list(outer)[::-1]]
        self.turns = len(outer) + len(self.inner)
        self.done = 0

    def begin(self, mine, got):
        total = add(mine, got)
        width = len(self.orders[0])
        self.values = [h.reshape((2,) * width + h.shape[1:]) for h in (total[:, :, :D // 2], total[:, :, D // 2:])]
        self.split()

    def resume(self, own):
        self.done = len(self.orders[0])
        self.values = [own]
        self.split()

    def split(self):
        turn, outer = self.done, len(self.orders[0])
        if turn < outer:
            bits = [o[turn] for o in self.orders]
            axes = [sorted(o[turn:], reverse=True).index(bit) for o, bit in zip(self.orders, bits)]
        else:
            if turn == outer:
                self.values = [jnp.concatenate(self.values, axis=1)]
                self.values = [v.reshape(self.narrow, -1, D) for v in self.values]
            bits, axes = [self.inner[turn - outer]], [1]
            v = self.values[0]
            self.values = [v.reshape(v.shape[0] // 2, 2, *v.shape[1:])]
        self.bits = bits
        self.sends = [part(v, self.me, bit, axis, False) for v, bit, axis in zip(self.values, bits, axes)]
        self.keeps = [part(v, self.me, bit, axis, True) for v, bit, axis in zip(self.values, bits, axes)]

    def turn(self):
        self.got = [swap(s, bit, self.devices) for s, bit in zip(self.sends, self.bits)]

    def take(self):
        self.done += 1
        last = self.done == self.turns
        self.values = [add(a, b, F32 if last else BF16) for a, b in zip(self.keeps, self.got)]
        if last:
            return self.values[0][0]
        self.split()

    def over(self, inputs, work):
        self.sends, inputs = tie(self.sends, inputs)
        self.turn()
        result = work(inputs)
        self.got, result = tie(self.got, result)
        return result, self.take()


def scatter_small(grad, me, wide, narrow):
    devices = wide * narrow
    bit = devices // 2
    while bit:
        both = grad.reshape(2, bit, *grad.shape[1:])
        grad = add(part(both, me, bit, 0, True), swap(part(both, me, bit, 0, False), bit, devices), F32)
        bit //= 2
    return grad[0]


def one_side(me, lhs, rhs, wide, narrow, owned, mine):
    side = (me // narrow) % 2
    side = side if mine else 1 - side
    return dw(side.reshape(1).astype(jnp.int32), lhs, rhs, narrow * owned, wide // 2)


def split_grads(me, lhs, rhs, wide, narrow, owned):
    rows, side = narrow * owned, (me // narrow) % 2
    sides = [(1 - side).reshape(1).astype(jnp.int32), side.reshape(1).astype(jnp.int32)]
    if rows % 128 == 0:
        sent = dw(sides[0], lhs, rhs, rows, wide // 2)
        sent, lhs = tie(sent, lhs)
        got = swap(sent, narrow, wide * narrow)
        mine = dw(sides[1], lhs, rhs, rows, wide // 2)
        return mine, got
    repeats = rhs.shape[0] // lhs.shape[0]
    left = [lhs[0]] * 3 + [lhs[1]] if repeats == 2 else list(lhs)
    grad = jnp.concatenate([tn(a, b) for a, b in zip(left, rhs)], axis=0).astype(BF16)
    grad = grad.reshape(wide // 2, 2, rows, D)
    return part(grad, me, narrow, 1, True), swap(part(grad, me, narrow, 1, False), narrow, wide * narrow)


def spread(seqs, shares):
    runs, at = [], 0
    for j, share in enumerate(shares):
        upto = seqs * sum(shares[:j + 1]) // sum(shares)
        if upto > at:
            runs.append((at, upto - at))
        at = upto
    return runs


def forward_by_permutes(me, wide, narrow, tokens, seg, feat, attention, feedforward, vector):
    seqs = seg.shape[0]
    me1 = me.reshape(1).astype(jnp.int32)
    small = gather_small(vector, me, wide, narrow)
    vec = jnp.pad(jnp.transpose(small, (1, 0, 2)).reshape(small.shape[1], D).astype(F32), ((0, 3), (0, 0)))
    near = Gather(attention, wide, narrow)
    far = Gather(feedforward, wide, narrow)
    ready = narrow.bit_length() - 2
    early = len(far.turns) - 3
    for t in range(len(near.turns)):
        near.turn()
        behind = t > ready and early > 0
        if behind:
            far.turn()
            early -= 1
        near.got, far.held = tie(near.got, far.held)
        if behind:
            near.got, far.got = tie(near.got, far.got)
            far.take()
        weights = near.take()
    att, offsets = weights
    held = ()
    runs = spread(seqs, (1, 2, 1))
    for first_seq, count in runs:
        more = len(far.turns) > 0
        if more:
            far.held, source = tie(far.held, held if held else att)
            far.turn()
        else:
            source = held if held else att
        if held:
            *held, natural = *k1(first_seq, count, me1, tokens, seg, feat, [natural], offsets, vec, source), natural
        else:
            *held, natural = k1(first_seq, count, me1, tokens, seg, feat, source, offsets, vec, ())
        held = tuple(held)
        if more:
            far.got, held = tie(far.got, held)
            ff = far.take()
    while far.turns:
        far.turn()
        ff = far.take()
    ff = ff[0]
    return (*held, vec, natural, ff, offsets)


def backward_by_permutes(me, wide, narrow, tokens, seg, feat, held, out_parts, natural, vec, owned):
    devices, seqs = wide * narrow, seg.shape[0]
    q, k, v, ctx, lse = held
    first, fb, dctx, broad, slim, vg2 = out_parts
    ff_sum = Scatter(me, wide, narrow)
    ff_sum.begin(*split_grads(me, broad, slim, wide, narrow, owned[0]))
    vg3, held, ff_owned = 0.0, (), None
    for first_seq, count in spread(seqs, (2, 1, 1)):
        def attend(given):
            source, kept = given
            return k3(first_seq, count, *source, ctx, dctx, fb, lse, seg, kept)
        (grads, more), ff_owned = ff_sum.over(((q, k, v), held), attend)
        held, vg3 = (grads,), vg3 + more
    d = held[0]
    if ff_owned is None:
        (mine, got), ff_owned = ff_sum.over((ctx, d), lambda g: split_grads(me, *g, wide, narrow, owned[1]))
    else:
        mine, got = split_grads(me, ctx, d, wide, narrow, owned[1])
    while ff_owned is None:
        _, ff_owned = ff_sum.over((), lambda g: ())
    att_sum = Scatter(me, wide, narrow)
    att_sum.begin(mine, got)
    vg4, held, att_owned = 0.0, (), None
    for first_seq, count in spread(seqs, (2, 1, 1)):
        def back(given):
            source, kept = given
            return k4(first_seq, count, source, d, tokens, seg, feat, natural, vec, kept)
        (grads, more), att_owned = att_sum.over((first, held), back)
        held, vg4 = (grads,), vg4 + more
    token_grads = held[0]
    vec_grad = jnp.concatenate([vg4[0:1], vg3[0:2], vg2[:10]], axis=0)
    vec_owned = scatter_small(jnp.transpose(vec_grad.reshape(vec_grad.shape[0], devices, -1), (1, 0, 2)), me, wide, narrow)
    while att_owned is None:
        att_sum.turn()
        att_owned = att_sum.take()
    return token_grads, ff_owned, att_owned, vec_owned


def local(wide, narrow, tokens, cotangent, segment_ids, feature_ids,
          attention_master, attention_first, attention_second,
          feedforward_master, feedforward_first, feedforward_second,
          vector_master, vector_first, vector_second):
    devices = wide * narrow
    me = lax.axis_index(BOTH)
    me1 = me.reshape(1).astype(jnp.int32)
    seg, feat = segment_ids, feature_ids
    seqs = seg.shape[0]
    shards = [m.astype(BF16) for m in (attention_master, feedforward_master, vector_master)]
    if devices <= 32:
        *held, vec, natural, ff = gathering_k1(wide, narrow, tokens, seg, feat, *shards)
        ff, offsets = [ff], ()
    else:
        *held, vec, natural, ff, offsets = forward_by_permutes(me, wide, narrow, tokens, seg, feat, *shards)
    mixed, q, k, v, ctx, lse = held
    out, first, fb, dctx, broad, slim, vg2 = k2(me1, mixed, ctx, cotangent, natural, ff, offsets, vec)
    parts = (first, fb, dctx, broad, slim, vg2)
    rows = (feedforward_master.shape[0], attention_master.shape[0])
    if devices <= 32:
        mine, got = split_grads(me, broad, slim, wide, narrow, rows[0])
        d, vg3, own = summing_k3(wide, narrow, q, k, v, ctx, dctx, fb, lse, seg, mine, got)
        ff_sum = Scatter(me, wide, narrow)
        ff_sum.resume(own)
        lhs, ff_owned = ctx, None
        sent, ff_owned = ff_sum.over((lhs, d), lambda g: one_side(me, *g, wide, narrow, rows[1], False))
        back = swap(sent, narrow, devices)
        if ff_owned is None:
            mine, ff_owned = ff_sum.over((lhs, d), lambda g: one_side(me, *g, wide, narrow, rows[1], True))
        else:
            mine = one_side(me, lhs, d, wide, narrow, rows[1], True)
        while ff_owned is None:
            _, ff_owned = ff_sum.over((), lambda g: ())
        token_grads, att_owned, vec_sum = summing_k4(wide, narrow, first, d, tokens, seg, feat, natural, vec, mine, back, vg2, vg3)
        width = vector_master.shape[1]
        vec_owned = lax.dynamic_slice(vec_sum, (0, me * width), (vector_master.shape[0], width))
    else:
        token_grads, ff_owned, att_owned, vec_owned = backward_by_permutes(
            me, wide, narrow, tokens, seg, feat, (q, k, v, ctx, lse), parts, natural, vec, rows)
    ff_rate = rates(feedforward_master.shape[0], FF, D ** (-0.5), FF ** (-0.5))
    att_rate = rates(attention_master.shape[0], 3 * D, D ** (-0.5), (D // 64) ** (-0.5))
    f_new = adam_step(feedforward_master, feedforward_first, feedforward_second, ff_owned, ff_rate)
    a_new = adam_step(attention_master, attention_first, attention_second, att_owned, att_rate)
    v_new = adam_step(vector_master, vector_first, vector_second, vec_owned, VECTOR_RATE)
    result = [out, token_grads]
    for new in (a_new, f_new, v_new):
        result += [*new, new[0].astype(BF16)]
    return tuple(result)


def solution(mesh):
    rows, cols = P(BOTH, None), P(None, BOTH)
    return jax.shard_map(
        partial(local, mesh.shape["wide"], mesh.shape["narrow"]), mesh=mesh,
        in_specs=(rows,) * 10 + (cols,) * 3,
        out_specs=(rows,) * 10 + (cols,) * 4,
        check_vma=False,
    )
```

```python
from functools import partial
import jax, jax.numpy as jnp
from jax import lax
from jax.experimental import pallas as pl
from jax.experimental.pallas import tpu as pltpu
from jax.sharding import PartitionSpec as P

D = 768
FF = 3072
HEADS = 12
HEAD_DIM = 64
NORM_EPS = 1e-05
AWAY = -1e30
F32, BF16 = jnp.float32, jnp.bfloat16
ERFC = (0.11841221385764535, 0.11979147087435008, 0.09737185909338779, 0.13434283549706147,
        -0.0652102059595758, 0.2202795624136942, -0.16009561537425632, 0.035107795064101)
VMEM = pltpu.VMEM


def nn(a, b):
    return lax.dot_general(a, b, (((1,), (0,)), ((), ())), preferred_element_type=F32)

def nt(a, b):
    return lax.dot_general(a, b, (((1,), (1,)), ((), ())), preferred_element_type=F32)

def tn(a, b):
    return lax.dot_general(a, b, (((0,), (0,)), ((), ())), preferred_element_type=F32)

def whole(shape):
    return pl.BlockSpec(shape, lambda *_: (0,) * len(shape), pipeline_mode=pl.Buffered(1))

def gelu_pair(h):
    below = 0.5 + 0.5 * lax.erf(h * 0.7071067811865476)
    bell = jnp.exp(h * h * -0.5)
    return h * below, below + h * (bell * 0.3989422804014327)


def column_of(row):
    return jnp.transpose(jnp.broadcast_to(row, (8, row.shape[1])))[:, :1]

def group_of(seg, feat):
    both = seg * 16 + feat
    return column_of(both) == both

def cost(gigaflops, megabytes):
    return pl.CostEstimate(flops=int(gigaflops * 1e9), bytes_accessed=int(megabytes * 1e6), transcendentals=0)


def fetch_weights(me, offsets, pieces, w_ref, sem):
    rows = pieces[0].shape[1]
    half = D // 2
    copies = []
    for j, offset in enumerate(offsets):
        for side in range(2):
            for col in range(2):
                owner = (me ^ offset[col]) if side == 0 else (me ^ offset[col] ^ offset[2])
                at = pl.ds(pl.multiple_of(owner * rows, 8), rows)
                copies.append(pltpu.make_async_copy(pieces[2 * side + col].at[j], w_ref.at[at, pl.ds(col * half, half)], sem))
    for c in copies:
        c.start()
    for c in copies:
        c.wait()

def attend_forward(i, tok_ref, seg_ref, feat_ref, w_ref, vec_ref, mixed_ref, q_ref, k_ref, v_ref, ctx_ref, lse_ref, bias_scr, service):
    seg = seg_ref[pl.ds(i, 1), :]
    feat = feat_ref[pl.ds(i, 1), :]
    length = seg.shape[1]
    bias_scr[...] = jnp.where(column_of(seg) == seg, 0.0, AWAY)
    group = group_of(seg, feat)
    members = jnp.sum(group.astype(F32), axis=1, keepdims=True)
    tok = tok_ref[...]
    merging = nn(group.astype(F32).astype(BF16), tok) / members
    mixed = tok.astype(F32) + vec_ref[0:1, :] * merging
    mixed_ref[...] = mixed
    mb = mixed.astype(BF16)
    ctx_ref[0] = mb
    q_ref[...] = ((nn(mb, w_ref[0:D, :]) + vec_ref[1:2, :]) * 0.125).astype(BF16)
    k_ref[...] = nn(mb, w_ref[D:2 * D, :]).astype(BF16)
    v_ref[...] = (nn(mb, w_ref[2 * D:3 * D, :]) + vec_ref[2:3, :]).astype(BF16)
    lane = lax.broadcasted_iota(jnp.int32, (length, 128), 1)
    low = lane < HEAD_DIM
    lse_ref[...] = jnp.zeros_like(lse_ref)

    def pair(p, carry):
        at = pl.ds(pl.multiple_of(p * 128, 128), 128)
        qp = q_ref[:, at]
        kp = k_ref[:, at]
        vp = v_ref[:, at]
        outs = []
        zero = jnp.zeros_like(qp)
        for half in range(2):
            mine = low if half == 0 else jnp.logical_not(low)
            s = nt(jnp.where(mine, qp, zero), kp) + bias_scr[...]
            top = jnp.max(s, axis=1, keepdims=True)
            e = jnp.exp(s - top)
            total = jnp.sum(e, axis=1, keepdims=True)
            o = nn(e.astype(BF16), vp) * (1.0 / total)
            outs.append(o)
            lse_ref[...] = jnp.where(lane == 2 * p + half, top + jnp.log(total), lse_ref[...])
        ctx_ref[1, :, at] = jnp.where(low, outs[0], outs[1]).astype(BF16)
        return carry
    service(0)
    lax.fori_loop(0, HEADS // 4, pair, 0)
    service(1)
    lax.fori_loop(HEADS // 4, HEADS // 2, pair, 0)
    service(2)


def k1_body(first_seq, offsets, kept, self_ref, tok_ref, seg_ref, feat_ref, vec_ref, *rest):
    if kept:
        w_ref, rest = rest[0], rest[1 + kept:]
        mixed_ref, q_ref, k_ref, v_ref, ctx_ref, lse_ref, bias_scr = rest
    else:
        pieces, rest = rest[:4], rest[4:]
        mixed_ref, q_ref, k_ref, v_ref, ctx_ref, lse_ref, w_ref, bias_scr, sem = rest
    i = pl.program_id(0) + first_seq

    if not kept:
        @pl.when(pl.program_id(0) == 0)
        def _():
            fetch_weights(self_ref[0], offsets, pieces, w_ref, sem)

    attend_forward(i, tok_ref, seg_ref, feat_ref, w_ref, vec_ref, mixed_ref, q_ref, k_ref, v_ref, ctx_ref, lse_ref, bias_scr, lambda point: None)


def k1(first_seq, count, me, tokens, seg, feat, weights, offsets, vec, kept):
    seqs, length = seg.shape
    blk = pl.BlockSpec((length, D), lambda i, s: (i + first_seq, 0))
    both = pl.BlockSpec((2, length, D), lambda i, s: (0, i + first_seq, 0))
    narrow = pl.BlockSpec((length, 128), lambda i, s: (i + first_seq, 0))
    n = seqs * length
    o = lambda dt: jax.ShapeDtypeStruct((n, D), dt)
    any_spec = pl.BlockSpec(memory_space=pl.ANY)
    out_specs = [blk] * 4 + [both, narrow]
    out_shape = [o(F32), o(BF16), o(BF16), o(BF16), jax.ShapeDtypeStruct((2, n, D), BF16), jax.ShapeDtypeStruct((n, 128), F32)]
    scratch = [VMEM((length, length), F32)]
    if kept:
        weight_specs = [pl.BlockSpec((3 * D, D), lambda i, s: (0, 0), pipeline_mode=pl.Buffered(1))]
    else:
        weight_specs = [any_spec] * 4
        out_specs = out_specs + [whole((4 * D, D))]
        out_shape = out_shape + [jax.ShapeDtypeStruct((4 * D, D), BF16)]
        scratch = scratch + [pltpu.SemaphoreType.DMA]
    return pl.pallas_call(
        partial(k1_body, first_seq, offsets, len(kept)),
        grid_spec=pltpu.PrefetchScalarGridSpec(
            num_scalar_prefetch=1, grid=(count,),
            in_specs=[blk, whole(seg.shape), whole(feat.shape), whole(vec.shape)] + weight_specs + [any_spec] * len(kept),
            out_specs=out_specs, scratch_shapes=scratch,
        ),
        out_shape=out_shape,
        input_output_aliases={6 + j: j for j in range(len(kept))},
        cost_estimate=cost(count * 11, count * 4),
        name="mix_attend",
    )(me, tokens, seg, feat, vec, *weights, *kept)

MESH = pl.DeviceIdType.MESH


def flips(x, mask):
    bit = 1
    while bit <= mask:
        if mask & bit:
            x = x + bit - 2 * bit * ((x // bit) % 2)
        bit *= 2
    return x


class Spreading:
    def __init__(self, wide, narrow, shard, full, columns, sems):
        self.narrow, self.masks = narrow, wide // 2
        self.bits = [1 << b for b in range((wide // 2).bit_length() - 1)]
        w, self.z = lax.axis_index("wide"), lax.axis_index("narrow")
        self.o, self.c = w // 2, w % 2
        self.shard, self.full, self.columns = shard, full, columns
        self.line_out, self.line_in, self.tree_out, self.tree_in, self.core_out, self.core_in, self.own = sems

    def at(self, r, k, c=None, h=None):
        c = self.c if c is None else c
        rows = self.shard.shape[0]
        owner = (2 * flips(self.o, r) + c) * self.narrow + flips(self.z, k)
        where = pl.ds(pl.multiple_of(owner * rows, 8), rows)
        if h is None:
            return self.full.at[where, :]
        return self.full.at[where, pl.ds(*self.columns[h][:2])]

    def source(self, r, k, h=None):
        if r or k:
            return self.at(r, k, None, h)
        return self.shard if h is None else self.shard.at[:, pl.ds(*self.columns[h][:2])]

    def keep(self):
        return pltpu.make_async_copy(self.shard, self.at(0, 0), self.own)

    def line(self, k, arriving=False):
        return pltpu.make_async_remote_copy(
            self.shard, self.at(0, k if arriving else 0), self.line_out.at[k - 1], self.line_in.at[k - 1],
            device_id=(2 * self.o + self.c, flips(self.z, k)), device_id_type=MESH)

    def tree(self, r, k, h, bit, arriving=False):
        there = r if arriving else r ^ bit
        n = (k * len(self.columns) + h) * self.masks + there
        part = self.at(r, k, None, h)
        return pltpu.make_async_remote_copy(
            part if arriving else self.source(r, k, h), part, self.tree_out.at[n], self.tree_in.at[n],
            device_id=(2 * flips(self.o, bit) + self.c, self.z), device_id_type=MESH)

    def core(self, r, k, arriving=False):
        n = k * self.masks + r
        part = self.at(r, k, 1 - self.c if arriving else None)
        return pltpu.make_async_remote_copy(
            part if arriving else self.source(r, k), part, self.core_out.at[n], self.core_in.at[n],
            device_id=(2 * self.o + 1 - self.c, self.z), device_id_type=MESH)

    def onward(self, r, h):
        if self.columns[h][2]:
            return [b for b in reversed(self.bits) if r == 0 or b < (r & -r)]
        return [b for b in self.bits if b > r]

    def last_bit(self, r, h):
        if self.columns[h][2]:
            return r & -r
        return 1 << (r.bit_length() - 1)

    def open(self):
        self.keep().start()
        for k in range(1, self.narrow):
            self.line(k).start()

    def send_on(self, r, k, h):
        for bit in self.onward(r, h):
            self.tree(r, k, h, bit).start()

    def roots(self, k):
        if k:
            self.line(k, True).wait_recv()
        for h in range(len(self.columns)):
            self.send_on(0, k, h)
        self.core(0, k).start()

    def relay(self, r, k):
        for h in range(len(self.columns)):
            self.tree(r, k, h, self.last_bit(r, h), True).wait_recv()
            self.send_on(r, k, h)
        self.core(r, k).start()

    def close(self):
        for k in range(self.narrow):
            for r in range(self.masks):
                self.core(r, k, True).wait_recv()
        self.keep().wait()

    def drain(self):
        for k in range(self.narrow):
            if k:
                self.line(k).wait_send()
            for r in range(self.masks):
                for h in range(len(self.columns)):
                    for bit in self.onward(r, h):
                        self.tree(r, k, h, bit).wait_send()
                self.core(r, k).wait_send()


def spreading_sems(wide, narrow, halves):
    dma = pltpu.SemaphoreType.DMA
    tree, core = narrow * halves * (wide // 2), narrow * (wide // 2)
    return [dma((narrow - 1,)), dma((narrow - 1,)), dma((tree,)), dma((tree,)), dma((core,)), dma((core,)), dma]


def greet(wide, narrow):
    barrier = pltpu.get_barrier_semaphore()
    w, z = lax.axis_index("wide"), lax.axis_index("narrow")
    o, c = w // 2, w % 2
    peers = [(w, flips(z, k)) for k in range(1, narrow)] + [(2 * o + 1 - c, z)]
    bit = 1
    while bit < wide // 2:
        peers.append((2 * flips(o, bit) + c, z))
        bit *= 2
    for peer in peers:
        pl.semaphore_signal(barrier, inc=1, device_id=peer, device_id_type=MESH)
    pl.semaphore_wait(barrier, len(peers))


def gathering_k1_body(wide, narrow, cols, steps, tok_ref, seg_ref, feat_ref, att_master, ff_master, vec_master,
                      mixed_ref, q_ref, k_ref, v_ref, ctx_ref, lse_ref, vec_ref, wout_ref, fout_ref,
                      bias_scr, w_ref, vs_scr, att_ref, ff_ref, vs_ref, put_sem, *sems):
    i = pl.program_id(0)
    half = D // 2
    count = len(sems) // 3
    pairs = [(0, half, False), (half, half, True)]
    att = Spreading(wide, narrow, att_ref, w_ref, pairs, sems[:count])
    ff = Spreading(wide, narrow, ff_ref, fout_ref, pairs, sems[count:2 * count])
    vs = Spreading(wide, narrow, vs_ref, vs_scr, [(0, 128, False)], sems[2 * count:])
    levels = {deep: [r for r in range(1, wide // 2) if (r & (r - 1) != 0) == deep] for deep in (False, True)}
    save = pltpu.make_async_copy(w_ref, wout_ref, put_sem)

    @pl.when(i == 0)
    def _():
        att_ref[...] = att_master[...].astype(BF16)
        ff_ref[...] = ff_master[...].astype(BF16)
        vs_ref[...] = jnp.zeros_like(vs_ref)
        vs_ref[0:vec_master.shape[0], 0:cols] = vec_master[...].astype(BF16)
        greet(wide, narrow)
        for one in (vs, att, ff):
            one.open()
        for k in range(narrow):
            vs.roots(k)
            att.roots(k)
            if k == 0:
                ff.roots(0)
        for r in range(1, wide // 2):
            for k in range(narrow):
                vs.relay(r, k)
                att.relay(r, k)
        vs.close()
        vec = jnp.zeros((16, D), F32)
        row = lax.broadcasted_iota(jnp.int32, (128, D), 0)
        col = lax.broadcasted_iota(jnp.int32, (128, D), 1)
        for d in range(wide * narrow):
            pick = jnp.logical_and(row < cols, col == row + cols * d).astype(F32).astype(BF16)
            vec = vec + nn(vs_scr[16 * d:16 * d + 16, :], pick)
        vec_ref[...] = vec
        att.close()
        save.start()

    plan = [[lambda k=k: ff.roots(k)] for k in range(1, narrow)]
    for r in range(1, wide // 2):
        plan += [[lambda r=r, k=k: ff.relay(r, k)] for k in range(narrow)]

    def service(point):
        for s in range(steps):
            todo = slots.get((s, point), ())
            if todo:
                @pl.when(i == s)
                def _(todo=todo):
                    for act in todo:
                        act()
    total = steps * 3 - 1
    slots = {}
    for n, group in enumerate(plan):
        spot = n * total // len(plan)
        slots.setdefault((spot // 3, spot % 3), []).extend(group)

    attend_forward(i, tok_ref, seg_ref, feat_ref, w_ref, vec_ref, mixed_ref, q_ref, k_ref, v_ref, ctx_ref, lse_ref, bias_scr, service)

    @pl.when(i == steps - 1)
    def _():
        ff.close()
        for one in (vs, att, ff):
            one.drain()
        save.wait()


def gathering_k1(wide, narrow, tokens, seg, feat, att_shard, ff_shard, vec_shard):
    seqs, length = seg.shape
    n, devices = seqs * length, wide * narrow
    blk = pl.BlockSpec((length, D), lambda i: (i, 0))
    any_spec = pl.BlockSpec(memory_space=pl.ANY)
    o = lambda dt: jax.ShapeDtypeStruct((n, D), dt)
    sems = spreading_sems(wide, narrow, 2) * 2 + spreading_sems(wide, narrow, 1)
    return pl.pallas_call(
        partial(gathering_k1_body, wide, narrow, vec_shard.shape[1], seqs), grid=(seqs,),
        in_specs=[blk] + [whole(a.shape) for a in (seg, feat, att_shard, ff_shard, vec_shard)],
        out_specs=[blk] * 4 + [pl.BlockSpec((2, length, D), lambda i: (0, i, 0)), pl.BlockSpec((length, 128), lambda i: (i, 0)),
                               whole((16, D)), any_spec, any_spec],
        out_shape=[o(F32), o(BF16), o(BF16), o(BF16), jax.ShapeDtypeStruct((2, n, D), BF16), jax.ShapeDtypeStruct((n, 128), F32),
                   jax.ShapeDtypeStruct((16, D), F32), jax.ShapeDtypeStruct((4 * D, D), BF16), jax.ShapeDtypeStruct((2 * FF, D), BF16)],
        scratch_shapes=[VMEM((length, length), F32), VMEM((4 * D, D), BF16), VMEM((16 * devices, 128), BF16),
                        VMEM(att_shard.shape, BF16), VMEM(ff_shard.shape, BF16), VMEM((16, 128), BF16), pltpu.SemaphoreType.DMA, *sems],
        compiler_params=pltpu.CompilerParams(collective_id=0, has_side_effects=True),
        cost_estimate=cost(60, 60),
        name="gather_attend",
    )(tokens, seg, feat, att_shard, ff_shard, vec_shard)

def masks_of(bits):
    found = [0]
    for b in bits:
        found = found + [m | b for m in found]
    return sorted(found, key=lambda m: (-bin(m).count("1"), m))


class Halving:
    def __init__(self, wide, narrow, total, tree_refs, line_refs, sems):
        bits = [1 << b for b in range((wide // 2).bit_length() - 1)]
        w, self.z = lax.axis_index("wide"), lax.axis_index("narrow")
        self.o, self.c = w // 2, w % 2
        self.total, self.tree_refs, self.line_refs, self.sems = total, tree_refs, line_refs, sems
        self.rows = total.shape[1] // narrow
        self.orders = [bits, bits[::-1]]
        self.line_bits = [1 << b for b in range(narrow.bit_length() - 1)]
        self.final = len(bits) - 1
        self.blocks = sorted(range(narrow), key=lambda k: (1 - k % 2, k))
        self.names = [("tree", h, t, m) for t in range(self.final) for h in range(2) for m in masks_of(self.orders[h][t + 1:])]
        self.names += [("last", h, self.final, k) for k in self.blocks for h in range(2)]
        self.names += [("line", 0, t, m) for t in range(len(line_refs)) for m in masks_of(self.line_bits[t + 1:])]

    def copy(self, name):
        kind, h, t, m = name
        n = self.names.index(name)
        if kind == "tree":
            bit = self.orders[h][t]
            cols = pl.ds(h * (D // 2), D // 2)
            slot = masks_of(self.orders[h][t + 1:]).index(m)
            source = self.total.at[flips(self.o, bit | m), :, cols]
            landing = self.tree_refs[t].at[h, slot]
            device = (2 * flips(self.o, bit) + self.c, self.z)
        elif kind == "last":
            bit = self.orders[h][t]
            at, cols = self.block(m), pl.ds(h * (D // 2), D // 2)
            source = self.total.at[flips(self.o, bit), at, cols]
            landing = self.tree_refs[t].at[h, 0, at, :]
            device = (2 * flips(self.o, bit) + self.c, self.z)
        else:
            bit = self.line_bits[t]
            slot = masks_of(self.line_bits[t + 1:]).index(m)
            source = self.total.at[self.o, pl.ds(pl.multiple_of(flips(self.z, bit | m) * self.rows, 8), self.rows), :]
            landing = self.line_refs[t].at[slot]
            device = (2 * self.o + self.c, flips(self.z, bit))
        return pltpu.make_async_remote_copy(source, landing, self.sems[0].at[n], self.sems[1].at[n], device_id=device, device_id_type=MESH)

    def block(self, k):
        return pl.ds(pl.multiple_of(flips(self.z, k) * self.rows, 8), self.rows)

    def take_last(self, onward):
        for name in self.names:
            if name[0] == "last" and (name[3] % 2 == 1) == onward:
                self.copy(name).wait_recv()
                _, h, t, k = name
                at, cols = self.block(k), pl.ds(h * (D // 2), D // 2)
                self.total[self.o, at, cols] = self.total[self.o, at, cols] + self.tree_refs[t][h, 0, at, :]

    def pick(self, kind, turn, deep):
        return [n for n in self.names if n[0] == kind and n[2] == turn and (n[3] != 0) == deep]

    def send(self, kind, turn):
        if kind == "tree" and turn == self.final:
            for name in self.names:
                if name[0] == "last":
                    self.copy(name).start()
            return
        for deep in (True, False):
            for name in self.pick(kind, turn, deep):
                self.copy(name).start()

    def take(self, kind, turn, deep):
        for name in self.pick(kind, turn, deep):
            self.copy(name).wait_recv()
            _, h, t, m = name
            if kind == "tree":
                cols = pl.ds(h * (D // 2), D // 2)
                slot = masks_of(self.orders[h][t + 1:]).index(m)
                self.total[flips(self.o, m), :, cols] = self.total[flips(self.o, m), :, cols] + self.tree_refs[t][h, slot]
            else:
                slot = masks_of(self.line_bits[t + 1:]).index(m)
                at = pl.ds(pl.multiple_of(flips(self.z, m) * self.rows, 8), self.rows)
                self.total[self.o, at, :] = self.total[self.o, at, :] + self.line_refs[t][slot]

    def drain(self):
        for name in self.names:
            self.copy(name).wait_send()


def halving_scratch(wide, narrow, rows, left):
    outer, inner = (wide // 2).bit_length() - 1, narrow.bit_length() - 1
    groups = wide // 2
    shapes = [VMEM((groups, narrow * rows, D), BF16)]
    shapes += [VMEM((2, groups >> (t + 1), narrow * rows, D // 2), BF16) for t in range(outer)]
    count = 2 * (groups - 2) + 2 * narrow
    shapes += [VMEM((narrow >> (t + 1), rows, D), BF16) for t in range(inner - left)]
    count += sum(narrow >> (t + 1) for t in range(inner - left))
    return shapes + [pltpu.SemaphoreType.DMA((count,)), pltpu.SemaphoreType.DMA((count,))]


def begin_total(total, mine_ref, got_ref):
    def one(g, carry):
        total[g] = mine_ref[g] + got_ref[g]
        return carry
    lax.fori_loop(0, total.shape[0], one, 0)

def norm_parts(z):
    mean = jnp.mean(z, axis=1, keepdims=True)
    c = z - mean
    var = jnp.mean(c * c, axis=1, keepdims=True)
    inv = lax.rsqrt(var + NORM_EPS)
    return c * inv, inv

def norm_pull(g, xhat, inv):
    a = jnp.mean(g, axis=1, keepdims=True)
    b = jnp.mean(g * xhat, axis=1, keepdims=True)
    return (g - a - xhat * b) * inv

def colsum(x):
    return jnp.sum(x, axis=0, keepdims=True)

def k2_body(offsets, self_ref, mixed_ref, ctx_ref, cot_ref, wo_ref, vec_ref, *rest):
    if offsets:
        pieces, rest = rest[:4], rest[4:]
        out_ref, first_ref, fb_ref, dctx_ref, wide_ref, slim_ref, vg_ref, gp_scr, sum_scr, wf_ref, sem = rest
    else:
        wf_ref, out_ref, first_ref, fb_ref, dctx_ref, wide_ref, slim_ref, vg_ref, gp_scr, sum_scr = rest
    ctx_ref = ctx_ref.at[0]
    hg_ref, act_ref = wide_ref.at[0], wide_ref.at[1]
    nb_ref, bg_ref = slim_ref.at[0], slim_ref.at[1]
    @pl.when(pl.program_id(0) == 0)
    def _():
        vg_ref[...] = jnp.zeros_like(vg_ref)
        if offsets:
            fetch_weights(self_ref[0], offsets, pieces, wf_ref, sem)

    ex = FF // D
    first_sum = mixed_ref[...] + nn(ctx_ref[...], wo_ref[...]) + vec_ref[3:4, :]
    xhat1, inv1 = norm_parts(first_sum)
    normed = xhat1 * vec_ref[4:5, :] + vec_ref[5:6, :]
    nb_ref[...] = normed.astype(BF16)
    sum_scr[...] = normed + vec_ref[6 + ex:7 + ex, :]
    for c in range(ex):
        at = pl.ds(c * D, D)
        h = nt(nb_ref[...], wf_ref[at, :]) + vec_ref[6 + c:7 + c, :]
        act, slope = gelu_pair(h)
        act_ref[:, at] = act.astype(BF16)
        gp_scr[:, at] = slope.astype(gp_scr.dtype)
        sum_scr[...] += nn(act_ref[:, at], wf_ref[pl.ds(FF + c * D, D), :])
    xhat2, inv2 = norm_parts(sum_scr[...])
    out_ref[...] = (xhat2 * vec_ref[7 + ex:8 + ex, :] + vec_ref[8 + ex:9 + ex, :]).astype(BF16)
    cot = cot_ref[...].astype(F32)
    vg_ref[4 + ex:5 + ex, :] += colsum(cot * xhat2)
    vg_ref[5 + ex:6 + ex, :] += colsum(cot)
    gs = norm_pull(cot * vec_ref[7 + ex:8 + ex, :], xhat2, inv2)
    vg_ref[3 + ex:4 + ex, :] += colsum(gs)
    bg_ref[...] = gs.astype(BF16)
    sum_scr[...] = gs
    for c in range(ex):
        at = pl.ds(c * D, D)
        hg = nt(bg_ref[...], wf_ref[pl.ds(FF + c * D, D), :]) * gp_scr[:, at].astype(F32)
        vg_ref[3 + c:4 + c, :] += colsum(hg)
        hg_ref[:, at] = hg.astype(BF16)
        sum_scr[...] += nn(hg_ref[:, at], wf_ref[at, :])
    ng = sum_scr[...]
    vg_ref[1:2, :] += colsum(ng * xhat1)
    vg_ref[2:3, :] += colsum(ng)
    fgr = norm_pull(ng * vec_ref[4:5, :], xhat1, inv1)
    vg_ref[0:1, :] += colsum(fgr)
    first_ref[...] = fgr
    fb_ref[...] = fgr.astype(BF16)
    dctx_ref[...] = nt(fb_ref[...], wo_ref[...]).astype(BF16)


def k2(me, mixed, ctx, cot, att, ff, offsets, vec, tile=256):
    n = mixed.shape[0]
    blk = pl.BlockSpec((tile, D), lambda i, s: (i, 0))
    o = lambda *w, dt=BF16: jax.ShapeDtypeStruct(w, dt)
    any_spec = pl.BlockSpec(memory_space=pl.ANY)
    return pl.pallas_call(
        partial(k2_body, offsets),
        grid_spec=pltpu.PrefetchScalarGridSpec(
            num_scalar_prefetch=1, grid=(n // tile,),
            in_specs=[blk, pl.BlockSpec((1, tile, D), lambda i, s: (1, i, 0)), blk,
                      pl.BlockSpec((D, D), lambda i, s: (3, 0), pipeline_mode=pl.Buffered(1)), whole(vec.shape)]
            + ([any_spec] * 4 if offsets else [whole(ff[0].shape)]),
            out_specs=[blk, blk, blk, blk, pl.BlockSpec((2, tile, FF), lambda i, s: (0, i, 0)),
                       pl.BlockSpec((2, tile, D), lambda i, s: (0, i, 0)), pl.BlockSpec((16, D), lambda i, s: (0, 0))],
            scratch_shapes=[VMEM((tile, FF), F32), VMEM((tile, D), F32)]
            + ([VMEM((2 * FF, D), BF16), pltpu.SemaphoreType.DMA] if offsets else []),
        ),
        out_shape=[o(n, D), o(n, D, dt=F32), o(n, D), o(n, D), o(2, n, FF), o(2, n, D), o(16, D, dt=F32)],
        cost_estimate=cost(60, 80),
        name="feed_forward",
    )(me, mixed, ctx, cot, att, vec, *ff)

def dw_body(rows, side_ref, lhs_ref, rhs_ref, out_ref):
    step = 384 if rows % 384 == 0 else 128
    for at in range(0, rows, step):
        out_ref[0, at:at + step, :] = tn(lhs_ref[0, :, at:at + step], rhs_ref[0]).astype(BF16)


def dw(side, lhs, rhs, rows, count):
    n, span = lhs.shape[1:]
    per = span // rows
    repeats = rhs.shape[0] // lhs.shape[0]
    tall = lambda i, s: (2 * i + s[0]) // per
    left = (lambda t: t // 3) if repeats == 2 else (lambda t: t)
    return pl.pallas_call(
        partial(dw_body, rows),
        grid_spec=pltpu.PrefetchScalarGridSpec(
            num_scalar_prefetch=1, grid=(count,),
            in_specs=[pl.BlockSpec((1, n, rows), lambda i, s: (left(tall(i, s)), 0, (2 * i + s[0]) % per)),
                      pl.BlockSpec((1, n, D), lambda i, s: (tall(i, s), 0, 0))],
            out_specs=pl.BlockSpec((1, rows, D), lambda i, s: (i, 0, 0)),
        ),
        out_shape=jax.ShapeDtypeStruct((count, rows, D), BF16),
        cost_estimate=cost(2e-9 * n * rows * D * count, 10),
        name="weight_grad",
    )(side, lhs, rhs)

def attend_back_step(i, q_ref, k_ref, v_ref, ctx_ref, dctx_ref, fb_ref, lse_ref, seg_ref, d_ref, vg_ref, bias_scr, lse_scr, del_scr, service):
    ctx_ref = ctx_ref.at[0]
    dq_ref, dk_ref, dv_ref = d_ref.at[0], d_ref.at[1], d_ref.at[2]
    d_ref[3] = fb_ref[...]
    @pl.when(pl.program_id(0) == 0)
    def _():
        vg_ref[...] = jnp.zeros_like(vg_ref)
    seg = seg_ref[pl.ds(i, 1), :]
    length = seg.shape[1]
    bias_scr[...] = jnp.where(column_of(seg) == seg, 0.0, AWAY)
    lse_scr[...] = jnp.transpose(lse_ref[...])[:16, :]
    prod = dctx_ref[...].astype(F32) * ctx_ref[...].astype(F32)
    pick = (lax.broadcasted_iota(jnp.int32, (16, D), 1) // HEAD_DIM == lax.broadcasted_iota(jnp.int32, (16, D), 0)).astype(F32).astype(BF16)
    high = prod.astype(BF16)
    del_scr[...] = nt(pick, high) + nt(pick, (prod - high.astype(F32)).astype(BF16))
    low = lax.broadcasted_iota(jnp.int32, (length, 128), 1) < HEAD_DIM

    def pair(p, carry):
        at = pl.ds(pl.multiple_of(p * 128, 128), 128)
        qp, kp, vp, op = q_ref[:, at], k_ref[:, at], v_ref[:, at], dctx_ref[:, at]
        zero = jnp.zeros_like(qp)
        got = []
        for half in range(2):
            mine = low if half == 0 else jnp.logical_not(low)
            st = nt(jnp.where(mine, kp, zero), qp) + bias_scr[...]
            pt = jnp.exp(st - lse_scr[pl.ds(2 * p + half, 1), :])
            dv = nn(pt.astype(BF16), op)
            dpt = nt(jnp.where(mine, vp, zero), op)
            dst = (pt * (dpt - del_scr[pl.ds(2 * p + half, 1), :])).astype(BF16)
            dk = nn(dst, qp)
            dq = tn(dst, kp)
            got.append((dq, dk, dv))
        dq, dk, dv = (jnp.where(low, a, b) for a, b in zip(*got))
        dqb = dq.astype(BF16) * jnp.bfloat16(0.125)
        dvb = dv.astype(BF16)
        dq_ref[:, at] = dqb
        dk_ref[:, at] = dk.astype(BF16)
        dv_ref[:, at] = dvb
        vg_ref[0:1, at] += colsum(dqb.astype(F32))
        vg_ref[1:2, at] += colsum(dvb.astype(F32))
        return carry
    service(0)
    lax.fori_loop(0, HEADS // 4, pair, 0)
    service(1)
    lax.fori_loop(HEADS // 4, HEADS // 2, pair, 0)
    service(2)


def k3_body(first_seq, kept, *refs):
    ins, rest = refs[:8], refs[8 + kept:]
    attend_back_step(pl.program_id(0) + first_seq, *ins, *rest, lambda point: None)


def k3(first_seq, count, q, k, v, ctx, dctx, fb, lse, seg, kept):
    seqs, length = seg.shape
    n = seqs * length
    blk = pl.BlockSpec((length, D), lambda i: (i + first_seq, 0))
    return pl.pallas_call(
        partial(k3_body, first_seq, len(kept)), grid=(count,),
        in_specs=[blk] * 3 + [pl.BlockSpec((1, length, D), lambda i: (1, i + first_seq, 0)), blk, blk,
                              pl.BlockSpec((length, 128), lambda i: (i + first_seq, 0)), whole((seqs, length))]
        + [pl.BlockSpec(memory_space=pl.ANY)] * len(kept),
        out_specs=[pl.BlockSpec((4, length, D), lambda i: (0, i + first_seq, 0)), pl.BlockSpec((8, D), lambda i: (0, 0))],
        out_shape=[jax.ShapeDtypeStruct((4, n, D), BF16), jax.ShapeDtypeStruct((8, D), F32)],
        scratch_shapes=[VMEM((length, length), F32), VMEM((16, length), F32), VMEM((16, length), F32)],
        input_output_aliases={8 + j: j for j in range(len(kept))},
        cost_estimate=cost(count * 12, count * 6),
        name="attend_back",
    )(q, k, v, ctx, dctx, fb, lse, seg, *kept)

def summing_k3_body(wide, narrow, steps, *refs):
    ins, (mine_ref, got_ref, d_ref, vg_ref, own_ref), rest = refs[:8], refs[8:13], refs[13:]
    (bias_scr, lse_scr, del_scr, total), rest = rest[:4], rest[4:]
    *land_refs, out_sems, in_sems = rest
    i = pl.program_id(0)
    turns = (wide // 2).bit_length() - 1
    tree_refs, line_refs = land_refs[:turns], land_refs[turns:]
    half = Halving(wide, narrow, total, tree_refs, line_refs, (out_sems, in_sems))

    @pl.when(i == 0)
    def _():
        greet(wide, narrow)
        begin_total(total, mine_ref, got_ref)
        half.send("tree", 0)

    def service(point):
        for t in range(turns):
            spot = 3 * steps * (t + 1) // (turns + 1) - 1 if t < turns - 1 else 3 * steps - 4
            if spot % 3 == point:
                @pl.when(i == spot // 3)
                def _(t=t):
                    if t < turns - 1:
                        half.take("tree", t, True)
                        half.send("tree", t + 1)
                    else:
                        for done in range(turns):
                            half.take("tree", done, False)
                        half.take_last(True)
                        if line_refs:
                            half.send("line", 0)

    attend_back_step(i, *ins, d_ref, vg_ref, bias_scr, lse_scr, del_scr, service)

    @pl.when(i == steps - 1)
    def _():
        half.take_last(False)
        for t in range(len(line_refs)):
            half.take("line", t, True)
            half.take("line", t, False)
            if t + 1 < len(line_refs):
                half.send("line", t + 1)
        half.drain()
        far = narrow // 2
        for n, mask in enumerate((0, far) if far else (0,)):
            own_ref[n] = total[half.o, pl.ds(pl.multiple_of(flips(half.z, mask) * half.rows, 8), half.rows), :]


def summing_k3(wide, narrow, q, k, v, ctx, dctx, fb, lse, seg, mine, got):
    seqs, length = seg.shape
    n = seqs * length
    blk = pl.BlockSpec((length, D), lambda i: (i, 0))
    span = mine.shape[1]
    return pl.pallas_call(
        partial(summing_k3_body, wide, narrow, seqs), grid=(seqs,),
        in_specs=[blk] * 3 + [pl.BlockSpec((1, length, D), lambda i: (1, i, 0)), blk, blk,
                              pl.BlockSpec((length, 128), lambda i: (i, 0)), whole((seqs, length)), whole(mine.shape), whole(got.shape)],
        out_specs=[pl.BlockSpec((4, length, D), lambda i: (0, i, 0)), whole((8, D)), whole((2, span // narrow, D))],
        out_shape=[jax.ShapeDtypeStruct((4, n, D), BF16), jax.ShapeDtypeStruct((8, D), F32), jax.ShapeDtypeStruct((2, span // narrow, D), BF16)],
        scratch_shapes=[VMEM((length, length), F32), VMEM((16, length), F32), VMEM((16, length), F32),
                        *halving_scratch(wide, narrow, span // narrow, 1)],
        compiler_params=pltpu.CompilerParams(collective_id=1, has_side_effects=True),
        cost_estimate=cost(60, 40),
        name="attend_back_sum",
    )(q, k, v, ctx, dctx, fb, lse, seg, mine, got)


def token_back_step(i, first_ref, d_ref, tok_ref, seg_ref, feat_ref, w_ref, vec_ref, tg_ref, vg_ref):
    dq_ref, dk_ref, dv_ref = d_ref.at[0], d_ref.at[1], d_ref.at[2]

    @pl.when(pl.program_id(0) == 0)
    def _():
        vg_ref[...] = jnp.zeros_like(vg_ref)
    group = group_of(seg_ref[pl.ds(i, 1), :], feat_ref[pl.ds(i, 1), :])
    gf = group.astype(F32)
    members = jnp.sum(gf, axis=1, keepdims=True)
    gb = gf.astype(BF16)
    tok = tok_ref[...]
    merging = nn(gb, tok) / members
    mg = (first_ref[...] + nt(dq_ref[...], w_ref[0:D, :]) + nt(dk_ref[...], w_ref[D:2 * D, :])
          + nt(dv_ref[...], w_ref[2 * D:3 * D, :]))
    vg_ref[0:1, :] += colsum(mg * merging)
    spread = (vec_ref[0:1, :] * mg / members).astype(BF16)
    tg_ref[...] = (mg + nn(gb, spread)).astype(BF16)


def k4_body(first_seq, kept, *refs):
    token_back_step(pl.program_id(0) + first_seq, *refs[:7], *refs[7 + kept:])


def summing_k4_body(wide, narrow, steps, *refs):
    ins, (mine_ref, got_ref, vg2_ref, vg3_ref, tg_ref, own_ref, vec_out), rest = refs[:7], refs[7:14], refs[14:]
    (vg_scr, total), rest = rest[:2], rest[2:]
    outer, inner = (wide // 2).bit_length() - 1, narrow.bit_length() - 1
    tree_refs, line_refs, rest = rest[:outer], rest[outer:outer + inner], rest[outer + inner:]
    out_sems, in_sems, sum_scr, came_scr, vec_sems_out, vec_sems_in = rest
    i = pl.program_id(0)
    half = Halving(wide, narrow, total, tree_refs, line_refs, (out_sems, in_sems))
    w, z = lax.axis_index("wide"), lax.axis_index("narrow")
    o, c = w // 2, w % 2
    ones = [(2 * o + 1 - c, z)] + [(2 * flips(o, 1 << b) + c, z) for b in range(outer)]
    line = [(w, flips(z, k)) for k in range(1, narrow)]

    def across(n, peer):
        return pltpu.make_async_remote_copy(sum_scr.at[min(n, len(ones))], came_scr.at[n], vec_sems_out.at[n], vec_sems_in.at[n],
                                            device_id=peer, device_id_type=MESH)

    hops = [across(n, peer) for n, peer in enumerate(ones + line)]

    @pl.when(i == 0)
    def _():
        greet(wide, narrow)
        begin_total(total, mine_ref, got_ref)
        half.send("tree", 0)

    @pl.when(i == steps - 1)
    def _():
        for t in range(outer):
            half.take("tree", t, False)
        half.take_last(True)
        half.send("line", 0)

    token_back_step(i, *ins, tg_ref, vg_scr)

    for t in range(outer - 1):
        @pl.when(i == min(steps - 2, (steps * (t + 1)) // (outer + 1)))
        def _(t=t):
            half.take("tree", t, True)
            half.send("tree", t + 1)

    @pl.when(i == steps - 1)
    def _():
        sum_scr[0, 0:1, :] = vg_scr[0:1, :]
        sum_scr[0, 1:3, :] = vg3_ref[0:2, :]
        sum_scr[0, 3:13, :] = vg2_ref[0:10, :]
        sum_scr[0, 13:16, :] = jnp.zeros((3, D), F32)
        hops[0].start()
        half.take_last(False)
        for turn in range(inner - 1):
            half.take("line", turn, True)
            half.take("line", turn, False)
            half.send("line", turn + 1)
        for n in range(len(ones)):
            hops[n].wait_recv()
            sum_scr[n + 1] = sum_scr[n] + came_scr[n]
            for later in (hops[n + 1:n + 2] if n + 1 < len(ones) else hops[n + 1:]):
                later.start()
        for hop in hops[len(ones):]:
            hop.wait_recv()
        spots = [sum_scr[len(ones)]] + [came_scr[len(ones) + k] for k in range(narrow - 1)]
        vec_out[...] = sum(spots[1:], spots[0])
        turn = inner - 1
        last = half.pick("line", turn, False)[0]
        half.copy(last).wait_recv()
        at = pl.ds(pl.multiple_of(z * half.rows, 8), half.rows)
        own_ref[...] = total[o, at, :].astype(F32) + line_refs[turn][0].astype(F32)
        half.drain()
        for hop in hops:
            hop.wait_send()


def summing_k4(wide, narrow, first, d, tokens, seg, feat, att, vec, mine, got, vg2, vg3):
    seqs, length = seg.shape
    n = seqs * length
    blk = pl.BlockSpec((length, D), lambda i: (i, 0))
    rows = mine.shape[1] // narrow
    stages = (wide // 2).bit_length() + narrow - 1
    return pl.pallas_call(
        partial(summing_k4_body, wide, narrow, seqs), grid=(seqs,),
        in_specs=[blk, pl.BlockSpec((3, length, D), lambda i: (0, i, 0)), blk, whole(seg.shape), whole(feat.shape),
                  pl.BlockSpec((3 * D, D), lambda i: (0, 0), pipeline_mode=pl.Buffered(1)), whole(vec.shape),
                  whole(mine.shape), whole(got.shape), whole(vg2.shape), whole(vg3.shape)],
        out_specs=[blk, whole((rows, D)), whole((16, D))],
        out_shape=[jax.ShapeDtypeStruct((n, D), BF16), jax.ShapeDtypeStruct((rows, D), F32), jax.ShapeDtypeStruct((16, D), F32)],
        scratch_shapes=[VMEM((8, D), F32), *halving_scratch(wide, narrow, rows, 0),
                        VMEM((stages, 16, D), F32), VMEM((stages, 16, D), F32), pltpu.SemaphoreType.DMA((stages,)), pltpu.SemaphoreType.DMA((stages,))],
        compiler_params=pltpu.CompilerParams(collective_id=2, has_side_effects=True),
        cost_estimate=cost(30, 30),
        name="token_grad_sum",
    )(first, d, tokens, seg, feat, att, vec, mine, got, vg2, vg3)


def k4(first_seq, count, first, d, tokens, seg, feat, att, vec, kept):
    seqs, length = seg.shape
    n = seqs * length
    blk = pl.BlockSpec((length, D), lambda i: (i + first_seq, 0))
    return pl.pallas_call(
        partial(k4_body, first_seq, len(kept)), grid=(count,),
        in_specs=[blk, pl.BlockSpec((3, length, D), lambda i: (0, i + first_seq, 0)), blk, whole(seg.shape), whole(feat.shape),
                  pl.BlockSpec((3 * D, D), lambda i: (0, 0), pipeline_mode=pl.Buffered(1)), whole(vec.shape)]
        + [pl.BlockSpec(memory_space=pl.ANY)] * len(kept),
        out_specs=[blk, pl.BlockSpec((8, D), lambda i: (0, 0))],
        out_shape=[jax.ShapeDtypeStruct((n, D), BF16), jax.ShapeDtypeStruct((8, D), F32)],
        input_output_aliases={7 + j: j for j in range(len(kept))},
        cost_estimate=cost(count * 3, count * 5),
        name="token_grad",
    )(first, d, tokens, seg, feat, att, vec, *kept)

def adam_step(master, first, second, gradient, rate):
    first_new = BETA * first + (1.0 - BETA) * gradient
    second_new = BETA * second + (1.0 - BETA) * gradient * gradient
    correction = 1.0 - BETA**ADAM_STEP
    master_new = master - rate * (
        first_new / correction / (jnp.sqrt(second_new / correction) + ADAM_EPS) + DECAY * master
    )
    return (master_new, first_new, second_new)


BETA = 0.5
ADAM_STEP = 3
ADAM_EPS = 1e-08
DECAY = 0.01
VECTOR_RATE = 0.1
BOTH = ("wide", "narrow")


def rates(rows, split, first_rate, second_rate):
    index = (lax.axis_index(BOTH) * rows + jnp.arange(rows))[:, None]
    return jnp.where(index < split, first_rate, second_rate)


def tie(*groups):
    return lax.optimization_barrier(groups)


def bit_steps(wide, narrow):
    inner = [1 << b for b in range(narrow.bit_length() - 1)]
    outer = [narrow << b for b in range(1, wide.bit_length() - 1)]
    return inner, outer, narrow


def swap(value, bit, devices):
    return lax.ppermute(value, BOTH, [(i, i ^ bit) for i in range(devices)])


class Gather:
    def __init__(self, shard, wide, narrow):
        self.devices = wide * narrow
        inner, outer, self.core = bit_steps(wide, narrow)
        self.turns = [(bit,) for bit in reversed(inner)] + list(zip(outer, reversed(outer))) + [(self.core, self.core)]
        self.held, self.offsets, self.last = [shard[None]], [[0]], None

    def turn(self):
        bits = self.turns.pop(0)
        if len(bits) == 2 and len(self.held) == 1:
            whole_rows = self.held[0]
            self.held = [whole_rows[:, :, :D // 2], whole_rows[:, :, D // 2:]]
            self.offsets = self.offsets * 2
        self.bits = bits
        self.got = [swap(h, bit, self.devices) for h, bit in zip(self.held, bits)]

    def take(self):
        if not self.turns:
            return (*self.held, *self.got), tuple((a, b, self.core) for a, b in zip(*self.offsets))
        self.held = [jnp.concatenate(pair) for pair in zip(self.held, self.got)]
        self.offsets = [o + [x ^ bit for x in o] for o, bit in zip(self.offsets, self.bits)]


def gather_small(shard, me, wide, narrow):
    devices = wide * narrow
    held = shard[None]
    bit = 1
    while bit < devices:
        held = jnp.concatenate([held, swap(held, bit, devices)])
        bit *= 2
    bit = 1
    while bit < devices:
        split = held.reshape(devices // (2 * bit), 2, bit, *shard.shape)
        held = jnp.where((me & bit) != 0, split[:, ::-1], split).reshape(held.shape)
        bit *= 2
    return held


def part(value, me, bit, axis, mine):
    index = (me & bit) != 0
    index = index.astype(jnp.int32) if mine else 1 - index.astype(jnp.int32)
    return lax.dynamic_index_in_dim(value, index, axis, keepdims=False)


def add(a, b, kind=BF16):
    return (a.astype(F32) + b.astype(F32)).astype(kind)


class Scatter:
    def __init__(self, me, wide, narrow):
        self.me, self.devices, self.narrow = me, wide * narrow, narrow
        self.inner, outer, _ = bit_steps(wide, narrow)
        self.orders = [list(outer), list(outer)[::-1]]
        self.turns = len(outer) + len(self.inner)
        self.done = 0

    def begin(self, mine, got):
        total = add(mine, got)
        width = len(self.orders[0])
        self.values = [h.reshape((2,) * width + h.shape[1:]) for h in (total[:, :, :D // 2], total[:, :, D // 2:])]
        self.split()

    def split(self):
        turn, outer = self.done, len(self.orders[0])
        if turn < outer:
            bits = [o[turn] for o in self.orders]
            axes = [sorted(o[turn:], reverse=True).index(bit) for o, bit in zip(self.orders, bits)]
        else:
            if turn == outer:
                self.values = [jnp.concatenate(self.values, axis=1)]
                self.values = [v.reshape(self.narrow, -1, D) for v in self.values]
            bits, axes = [self.inner[turn - outer]], [1]
            v = self.values[0]
            self.values = [v.reshape(v.shape[0] // 2, 2, *v.shape[1:])]
        self.bits = bits
        self.sends = [part(v, self.me, bit, axis, False) for v, bit, axis in zip(self.values, bits, axes)]
        self.keeps = [part(v, self.me, bit, axis, True) for v, bit, axis in zip(self.values, bits, axes)]

    def turn(self):
        self.got = [swap(s, bit, self.devices) for s, bit in zip(self.sends, self.bits)]

    def take(self):
        self.done += 1
        last = self.done == self.turns
        self.values = [add(a, b, F32 if last else BF16) for a, b in zip(self.keeps, self.got)]
        if last:
            return self.values[0][0]
        self.split()

    def over(self, inputs, work):
        self.sends, inputs = tie(self.sends, inputs)
        self.turn()
        result = work(inputs)
        self.got, result = tie(self.got, result)
        return result, self.take()


def scatter_small(grad, me, wide, narrow):
    devices = wide * narrow
    bit = devices // 2
    while bit:
        both = grad.reshape(2, bit, *grad.shape[1:])
        grad = add(part(both, me, bit, 0, True), swap(part(both, me, bit, 0, False), bit, devices), F32)
        bit //= 2
    return grad[0]


def one_side(me, lhs, rhs, wide, narrow, owned, mine):
    side = (me // narrow) % 2
    side = side if mine else 1 - side
    return dw(side.reshape(1).astype(jnp.int32), lhs, rhs, narrow * owned, wide // 2)


def split_grads(me, lhs, rhs, wide, narrow, owned):
    rows, side = narrow * owned, (me // narrow) % 2
    sides = [(1 - side).reshape(1).astype(jnp.int32), side.reshape(1).astype(jnp.int32)]
    if rows % 128 == 0:
        sent = dw(sides[0], lhs, rhs, rows, wide // 2)
        sent, lhs = tie(sent, lhs)
        got = swap(sent, narrow, wide * narrow)
        mine = dw(sides[1], lhs, rhs, rows, wide // 2)
        return mine, got
    repeats = rhs.shape[0] // lhs.shape[0]
    left = [lhs[0]] * 3 + [lhs[1]] if repeats == 2 else list(lhs)
    grad = jnp.concatenate([tn(a, b) for a, b in zip(left, rhs)], axis=0).astype(BF16)
    grad = grad.reshape(wide // 2, 2, rows, D)
    return part(grad, me, narrow, 1, True), swap(part(grad, me, narrow, 1, False), narrow, wide * narrow)


def spread(seqs, shares):
    runs, at = [], 0
    for j, share in enumerate(shares):
        upto = seqs * sum(shares[:j + 1]) // sum(shares)
        if upto > at:
            runs.append((at, upto - at))
        at = upto
    return runs


def forward_by_permutes(me, wide, narrow, tokens, seg, feat, attention, feedforward, vector):
    seqs = seg.shape[0]
    me1 = me.reshape(1).astype(jnp.int32)
    small = gather_small(vector, me, wide, narrow)
    vec = jnp.pad(jnp.transpose(small, (1, 0, 2)).reshape(small.shape[1], D).astype(F32), ((0, 3), (0, 0)))
    near = Gather(attention, wide, narrow)
    far = Gather(feedforward, wide, narrow)
    ready = narrow.bit_length() - 2
    early = len(far.turns) - 3
    for t in range(len(near.turns)):
        near.turn()
        behind = t > ready and early > 0
        if behind:
            far.turn()
            early -= 1
        near.got, far.held = tie(near.got, far.held)
        if behind:
            near.got, far.got = tie(near.got, far.got)
            far.take()
        weights = near.take()
    att, offsets = weights
    held = ()
    runs = spread(seqs, (1, 2, 1))
    for first_seq, count in runs:
        more = len(far.turns) > 0
        if more:
            far.held, source = tie(far.held, held if held else att)
            far.turn()
        else:
            source = held if held else att
        if held:
            *held, natural = *k1(first_seq, count, me1, tokens, seg, feat, [natural], offsets, vec, source), natural
        else:
            *held, natural = k1(first_seq, count, me1, tokens, seg, feat, source, offsets, vec, ())
        held = tuple(held)
        if more:
            far.got, held = tie(far.got, held)
            ff = far.take()
    while far.turns:
        far.turn()
        ff = far.take()
    ff = ff[0]
    return (*held, vec, natural, ff, offsets)


def backward_by_permutes(me, wide, narrow, tokens, seg, feat, held, out_parts, natural, vec, owned):
    devices, seqs = wide * narrow, seg.shape[0]
    q, k, v, ctx, lse = held
    first, fb, dctx, broad, slim, vg2 = out_parts
    ff_sum = Scatter(me, wide, narrow)
    ff_sum.begin(*split_grads(me, broad, slim, wide, narrow, owned[0]))
    vg3, held, ff_owned = 0.0, (), None
    for first_seq, count in spread(seqs, (2, 1, 1)):
        def attend(given):
            source, kept = given
            return k3(first_seq, count, *source, ctx, dctx, fb, lse, seg, kept)
        (grads, more), ff_owned = ff_sum.over(((q, k, v), held), attend)
        held, vg3 = (grads,), vg3 + more
    d = held[0]
    if ff_owned is None:
        (mine, got), ff_owned = ff_sum.over((ctx, d), lambda g: split_grads(me, *g, wide, narrow, owned[1]))
    else:
        mine, got = split_grads(me, ctx, d, wide, narrow, owned[1])
    while ff_owned is None:
        _, ff_owned = ff_sum.over((), lambda g: ())
    att_sum = Scatter(me, wide, narrow)
    att_sum.begin(mine, got)
    vg4, held, att_owned = 0.0, (), None
    for first_seq, count in spread(seqs, (2, 1, 1)):
        def back(given):
            source, kept = given
            return k4(first_seq, count, source, d, tokens, seg, feat, natural, vec, kept)
        (grads, more), att_owned = att_sum.over((first, held), back)
        held, vg4 = (grads,), vg4 + more
    token_grads = held[0]
    vec_grad = jnp.concatenate([vg4[0:1], vg3[0:2], vg2[:10]], axis=0)
    vec_owned = scatter_small(jnp.transpose(vec_grad.reshape(vec_grad.shape[0], devices, -1), (1, 0, 2)), me, wide, narrow)
    while att_owned is None:
        att_sum.turn()
        att_owned = att_sum.take()
    return token_grads, ff_owned, att_owned, vec_owned


def local(wide, narrow, tokens, cotangent, segment_ids, feature_ids,
          attention_master, attention_first, attention_second,
          feedforward_master, feedforward_first, feedforward_second,
          vector_master, vector_first, vector_second):
    devices = wide * narrow
    me = lax.axis_index(BOTH)
    me1 = me.reshape(1).astype(jnp.int32)
    seg, feat = segment_ids, feature_ids
    seqs = seg.shape[0]
    shards = (attention_master, feedforward_master, vector_master)
    if devices <= 32:
        *held, vec, natural, ff = gathering_k1(wide, narrow, tokens, seg, feat, *shards)
        ff, offsets = [ff], ()
    else:
        *held, vec, natural, ff, offsets = forward_by_permutes(me, wide, narrow, tokens, seg, feat, *[m.astype(BF16) for m in shards])
    mixed, q, k, v, ctx, lse = held
    out, first, fb, dctx, broad, slim, vg2 = k2(me1, mixed, ctx, cotangent, natural, ff, offsets, vec)
    parts = (first, fb, dctx, broad, slim, vg2)
    rows = (feedforward_master.shape[0], attention_master.shape[0])
    if devices <= 32:
        mine, got = split_grads(me, broad, slim, wide, narrow, rows[0])
        d, vg3, own = summing_k3(wide, narrow, q, k, v, ctx, dctx, fb, lse, seg, mine, got)
        own, away, lhs = tie(own[0], own[1], ctx)
        came = swap(away, narrow // 2, devices)
        sent = one_side(me, lhs, d, wide, narrow, rows[1], False)
        came, sent, lhs = tie(came, sent, lhs)
        back = swap(sent, narrow, devices)
        mine = one_side(me, lhs, d, wide, narrow, rows[1], True)
        ff_owned = add(own, came, F32)
        token_grads, att_owned, vec_sum = summing_k4(wide, narrow, first, d, tokens, seg, feat, natural, vec, mine, back, vg2, vg3)
        width = vector_master.shape[1]
        vec_owned = lax.dynamic_slice(vec_sum, (0, me * width), (vector_master.shape[0], width))
    else:
        token_grads, ff_owned, att_owned, vec_owned = backward_by_permutes(
            me, wide, narrow, tokens, seg, feat, (q, k, v, ctx, lse), parts, natural, vec, rows)
    ff_rate = rates(feedforward_master.shape[0], FF, D ** (-0.5), FF ** (-0.5))
    att_rate = rates(attention_master.shape[0], 3 * D, D ** (-0.5), (D // 64) ** (-0.5))
    f_new = adam_step(feedforward_master, feedforward_first, feedforward_second, ff_owned, ff_rate)
    a_new = adam_step(attention_master, attention_first, attention_second, att_owned, att_rate)
    v_new = adam_step(vector_master, vector_first, vector_second, vec_owned, VECTOR_RATE)
    result = [out, token_grads]
    for new in (a_new, f_new, v_new):
        result += [*new, new[0].astype(BF16)]
    return tuple(result)


def solution(mesh):
    rows, cols = P(BOTH, None), P(None, BOTH)
    return jax.shard_map(
        partial(local, mesh.shape["wide"], mesh.shape["narrow"]), mesh=mesh,
        in_specs=(rows,) * 10 + (cols,) * 3,
        out_specs=(rows,) * 10 + (cols,) * 4,
        check_vma=False,
    )
```
